32 devices in a mesh: grp: 2 (over y), ka: 4 (over z), orb: 2 (over x), band: 2 (over core).
Axes of the slice: x: 2, y: 2, z: 4, core: 2. Of those that a mesh axis runs over, the one named last changes fastest.
Arguments:
- eigvecs: bfloat16 [8, 2, 8192, 256], P(('grp', 'ka'), None, 'orb', 'band'), parts along dimension 0, may hold values from -0.03515625 to 0.03515625
- band_rank: int32 [8, 256], P(('grp', 'ka'), 'band'), parts along dimension 0, may hold values from 0 to 255, each once within a row
- occ_count: int32 [2], P('grp'), parts along dimension 0, may hold values from 128 to 256
- wrap_shift: int32 [2], P('grp'), parts along dimension 0, may hold values from 1 to 4095
- orbital_site: int32 [16384], P(('grp', 'orb')), parts along dimension 0, may hold values from 0 to 63
Outputs:
- wilson: float32 [8, 256, 2, 256], P(('grp', 'ka'), 'orb', None, 'band'), parts along dimension 0
The draws below stay inside these ranges and needn't reach their ends.
There are 2 independent parts, one for each index of `grp`. The reference program is written for one: setup_inputs(seed, part) draws one part's arguments, and reference() takes and returns one part's arrays. A program takes and returns all parts, laid end to end along the dimension named above; each array names one. Nothing has to cross between parts.
All inputs are finite; a program needn't handle non-finite values.
Results may differ from the reference program's by a relative error of at most 0.025.
Values may be sent and summed in bfloat16 or wider, within the bound.
A program may use at most 64 MiB of HBM per device.

```python
import math
import jax
import jax.numpy as jnp
from jax import lax

ORBS = 8192
BANDS = 256
NS_STEPS = 8
SITES = 64
KPTS = 4


def draw_eigvecs(key, part):
    entry_scale = (2.0 * ORBS) ** (-0.5)
    full_shape = (KPTS, 2, ORBS, BANDS)
    base_key = jax.random.fold_in(key, 101)
    noise_key = jax.random.fold_in(key, 202)
    mix_key = jax.random.fold_in(key, 303)
    common = jax.random.normal(base_key, (2, ORBS, BANDS), jnp.float32)
    fresh_noise = jax.random.normal(noise_key, full_shape, jnp.float32)
    mixing = jax.random.uniform(mix_key, (KPTS, 1, 1, 1), jnp.float32, 0.3, 0.55)
    values = mixing * common[None] + jnp.sqrt(1.0 - mixing * mixing) * fresh_noise
    return (jnp.clip(values, -4.4, 4.4) * entry_scale).astype(jnp.bfloat16)


def set_ends(array, key, smallest, largest):
    spot = [jax.random.randint(jax.random.fold_in(key, axis), (), 0, length) for axis, length in enumerate(array.shape)]
    main_axis = array.shape.index(max(array.shape))
    next_to = spot[:main_axis] + [(spot[main_axis] + 1) % array.shape[main_axis]] + spot[main_axis + 1:]
    return array.at[tuple(spot)].set(smallest).at[tuple(next_to)].set(largest)


def setup_inputs(seed: int = 0, part: int = 0) -> dict:
    streams_of = jax.random.split(jax.random.key(seed), 6)
    part_splits = jax.random.split(jax.random.fold_in(streams_of[5], part), 6)
    eigvecs = draw_eigvecs(jax.random.fold_in(jax.random.fold_in(streams_of[5], part), 71), part)
    band_rank = jax.vmap(lambda own: jax.random.permutation(own, BANDS))(jax.random.split(part_splits[1], KPTS)).reshape((KPTS, BANDS)).astype(jnp.int32)
    occ_count = jax.random.randint(part_splits[2], (1,), BANDS // 2, BANDS + 1).astype(jnp.int32)
    wrap_shift = jax.random.randint(part_splits[3], (1,), 1, 4096).astype(jnp.int32)
    orbital_site = set_ends(jax.random.randint(part_splits[4], (ORBS,), 0, SITES), jax.random.fold_in(part_splits[4], 1), 0, SITES - 1).astype(jnp.int32)
    return dict(eigvecs=eigvecs, band_rank=band_rank, occ_count=occ_count, wrap_shift=wrap_shift, orbital_site=orbital_site)


ns_gain = 0.7
eps_mean = 1e-06

def complex_block(matrix):
    order_size = matrix.shape[0]
    real_part = matrix[:, :order_size]
    imag_part = matrix[:, order_size:]
    upper_half = jnp.concatenate([real_part, imag_part], axis=1)
    lower_half = jnp.concatenate([-imag_part, real_part], axis=1)
    return jnp.concatenate([upper_half, lower_half], axis=0)

def complex_product(left_side, right_side):
    return jnp.dot(left_side, complex_block(right_side), precision=lax.Precision.HIGHEST, preferred_element_type=jnp.float32)

def polar_step(iterate):
    order_size = iterate.shape[1]
    rounded = iterate.astype(jnp.bfloat16)
    widened = rounded.astype(jnp.float32)
    gram_matrix = jnp.einsum('kri,krj->kij', widened, widened, precision=lax.Precision.HIGHEST)
    gram_real = gram_matrix[:, :order_size, :order_size] + gram_matrix[:, order_size:, order_size:]
    gram_imag = gram_matrix[:, :order_size, order_size:] - gram_matrix[:, order_size:, :order_size]
    upper_half = jnp.concatenate([gram_real, gram_imag], axis=2)
    lower_half = jnp.concatenate([-gram_imag, gram_real], axis=2)
    gram_block = jnp.concatenate([upper_half, lower_half], axis=1).astype(jnp.bfloat16).astype(jnp.float32)
    product = jnp.einsum('kri,kij->krj', widened, gram_block, precision=lax.Precision.HIGHEST)
    return 1.5 * iterate - 0.5 * product

def margin_pair(block_pair):
    left_block, right_block = block_pair
    stacked = jnp.concatenate([left_block[0], left_block[1]], axis=0)
    real_side = jnp.concatenate([right_block[0], right_block[1]], axis=0)
    imag_side = jnp.concatenate([right_block[1], -right_block[0]], axis=0)
    paired = jnp.concatenate([real_side, imag_side], axis=1)
    return jnp.dot(stacked.T, paired, preferred_element_type=jnp.float32)

def reference(eigvecs, band_rank, occ_count, wrap_shift, orbital_site):
    occupied = band_rank < occ_count[0]
    masked = jnp.where(occupied[:, None, None, :], eigvecs, jnp.zeros((), jnp.bfloat16))
    phase_angle = (wrap_shift[0] * orbital_site % SITES).astype(jnp.float32) * (2.0 * math.pi / SITES)
    cosine = jnp.cos(phase_angle)[:, None]
    sine_factor = jnp.sin(phase_angle)[:, None]
    first_real = masked[0, 0].astype(jnp.float32)
    first_imag = masked[0, 1].astype(jnp.float32)
    wrapped = jnp.stack([cosine * first_real + sine_factor * first_imag, cosine * first_imag - sine_factor * first_real]).astype(jnp.bfloat16)
    right_blocks = jnp.concatenate([masked[1:], wrapped[None]], axis=0)
    margins = lax.map(margin_pair, (masked, right_blocks))
    occupied_total = occ_count[0].astype(jnp.float32)
    squares = lax.optimization_barrier(jnp.sum(margins * margins, axis=(1, 2)))
    iterate = margins * (ns_gain * lax.rsqrt(squares / occupied_total + eps_mean))[:, None, None]
    for sweep_index in range(NS_STEPS):
        iterate = polar_step(iterate)
    identity = jnp.concatenate([jnp.eye(BANDS, dtype=jnp.float32), jnp.zeros((BANDS, BANDS), jnp.float32)], axis=1)

    def link(running, factor):
        following = complex_product(running, factor)
        return (following, following)
    final_loop, prefix = lax.scan(link, identity, iterate)
    return prefix.reshape(KPTS, BANDS, 2, BANDS) * math.sqrt(BANDS)
```

```python
import functools
import math

import jax
import jax.numpy as jnp
from jax import lax
from jax.experimental import pallas as pl
from jax.experimental.pallas import tpu as pltpu
from jax.sharding import PartitionSpec as P

NS_STEPS = 8
SITES = 64
CHUNKS = 12
BLOCKS = 8

ns_gain = 0.7
eps_mean = 1e-06

MESH = pl.DeviceIdType.MESH
BF16 = jnp.bfloat16
F32 = jnp.float32


def levels_of(count):
    return max(1, (count - 1).bit_length())


def remote(src, dst, send_sem, recv_sem, device):
    return pltpu.make_async_remote_copy(
        src_ref=src,
        dst_ref=dst,
        send_sem=send_sem,
        recv_sem=recv_sem,
        device_id=device,
        device_id_type=MESH,
    )


def across(left, right, contract):
    return lax.dot_general(left, right, (contract, ((), ())), preferred_element_type=F32)


def column_of(row, width):
    return jnp.transpose(jnp.broadcast_to(row, (width, row.shape[1])))


def polar_step(iterate):
    half = iterate.shape[1] // 2
    rounded = iterate.astype(BF16)
    real, imag = rounded[:, :half], rounded[:, half:]
    tall = jnp.concatenate(
        [rounded, jnp.concatenate([imag, -real], axis=1)], axis=0
    )
    gram = across(tall, rounded, ((1,), (1,))).astype(BF16)
    rows = iterate.shape[0]
    wide = jnp.concatenate([gram[:rows], gram[rows:]], axis=1)
    block = jnp.concatenate(
        [rounded, jnp.concatenate([-imag, real], axis=1)], axis=0
    )
    product = across(wide, block, ((1,), (0,)))
    return 1.5 * iterate - 0.5 * product


def merge(pieces, factor):
    cols = factor.shape[1] // 2
    left = jnp.concatenate(
        [piece[:, :cols] for piece in pieces] + [piece[:, cols:] for piece in pieces], axis=1
    )
    lower = jnp.concatenate([-factor[:, cols:], factor[:, :cols]], axis=1)
    return across(left, jnp.concatenate([factor, lower], axis=0), ((1,), (0,)))


def kernel(
    nka, norb, nband,
    eig, rank, occ_at, shift_at, site_at,
    out,
    lefts, rights, stage, tail, cosine, sine, angle_cos, angle_sin, tail_cos, tail_sin,
    occ, shift, site, rank_band, rank_next, acc, mask, parts, full, cur, pfx, got,
    ready,
    sem_own, sem_arg, sem_left, sem_rank, sem_next, sem_right, sem_tail, sem_part, sem_pre, sem_fwd,
):
    ka, orb, band = lax.axis_index("ka"), lax.axis_index("orb"), lax.axis_index("band")
    rows, cols = eig.shape[1], eig.shape[2]
    bands = nband * cols
    depth = tail.shape[2]
    body = rows - depth
    step = body // CHUNKS
    width = cols // BLOCKS
    before = lax.rem(ka + nka - 1, nka)
    lanes = site.shape[1]

    barrier = pltpu.get_barrier_semaphore()
    for d in range(norb):
        for e in range(nband):
            if d + e > 0:
                to = {"orb": lax.rem(orb + d, norb), "band": lax.rem(band + e, nband)}
                pl.semaphore_signal(barrier, inc=1, device_id=to, device_id_type=MESH)
    for t in range(1, nka):
        @pl.when(ka + t < nka)
        def _(t=t):
            pl.semaphore_signal(
                barrier, inc=1, device_id={"ka": lax.rem(ka + t, nka)}, device_id_type=MESH
            )
    pl.semaphore_wait(barrier, norb * nband - 1 + ka)
    for t in range(1, nka):
        @pl.when(ka >= t)
        def _(t=t):
            pl.semaphore_signal(
                ready, inc=1, device_id={"ka": lax.rem(ka + nka - t, nka)}, device_id_type=MESH
            )

    def chunk(c):
        return pl.ds(pl.multiple_of(c * step, step), step)

    def right_copy(c):
        return remote(
            eig.at[:, chunk(c)], rights.at[:, chunk(c)],
            sem_right.at[0, c], sem_right.at[1, c], {"ka": before},
        )

    def part_of(b):
        return pl.ds(b * width, width)

    def tail_copy(b):
        return remote(
            stage.at[:, part_of(b)], tail.at[:, part_of(b)],
            sem_tail.at[0, b], sem_tail.at[1, b], {"ka": before},
        )

    next_rank = remote(rank, rank_next, sem_next.at[0], sem_next.at[1], {"ka": before})

    def start_right():
        next_rank.start()
        for c in range(CHUNKS):
            right_copy(c).start()

    @pl.when(ka > 0)
    def _():
        start_right()

    own = pltpu.make_async_copy(eig, lefts.at[:, band], sem_own)
    own.start()
    arguments = [
        pltpu.make_async_copy(src, dst, sem_arg.at[i])
        for i, (src, dst) in enumerate(
            ((occ_at, occ), (shift_at, shift), (site_at, site), (rank, rank_band.at[band]))
        )
    ]
    for copy in arguments:
        copy.start()
    band_sends = []
    for d in range(1, nband):
        to = {"band": lax.rem(band + d, nband)}
        copy = remote(eig, lefts.at[:, band], sem_left.at[0, d], sem_left.at[1, d], to)
        copy.start()
        band_sends.append(copy)
        copy = remote(rank, rank_band.at[band], sem_rank.at[0, d], sem_rank.at[1, d], to)
        copy.start()
        band_sends.append(copy)

    @pl.when(ka < nka - 1)
    def _():
        pl.semaphore_wait(ready, nka - 1 - ka)

    @pl.when(ka == 0)
    def _():
        start_right()

    for copy in arguments:
        copy.wait()

    at_end, at_start = ka == nka - 1, ka == 0
    angle = ((shift[0] * site[...]) & (SITES - 1)).astype(F32) * (2.0 * math.pi / SITES)
    turned, lifted = jnp.cos(angle), jnp.sin(angle)
    angle_cos[...] = jnp.where(at_end, turned, 1.0)
    angle_sin[...] = jnp.where(at_end, lifted, 0.0)
    tail_cos[...] = jnp.where(at_start, turned, 1.0)
    tail_sin[...] = jnp.where(at_start, lifted, 0.0)

    own.wait()

    @pl.loop(0, depth // lanes)
    def _(i):
        from_rows = pl.ds(pl.multiple_of(body + i * lanes, lanes), lanes)
        to_lanes = pl.ds(pl.multiple_of(i * lanes, lanes), lanes)
        real = jnp.transpose(lefts[0, band, from_rows, :].astype(F32))
        imag = jnp.transpose(lefts[1, band, from_rows, :].astype(F32))
        turn = tail_cos[pl.ds(body // lanes + i, 1), :]
        lift = tail_sin[pl.ds(body // lanes + i, 1), :]
        stage[0, :, to_lanes] = (turn * real + lift * imag).astype(BF16)
        stage[1, :, to_lanes] = (turn * imag - lift * real).astype(BF16)

    @pl.loop(0, body // lanes)
    def _(i):
        place = pl.ds(pl.multiple_of(i * lanes, lanes), lanes)
        cosine[place, :] = column_of(angle_cos[pl.ds(i, 1), :], cols)
        sine[place, :] = column_of(angle_sin[pl.ds(i, 1), :], cols)

    for b in range(BLOCKS):
        tail_copy(b).start()

    for d in range(1, nband):
        came = lax.rem(band + nband - d, nband)
        to = {"band": lax.rem(band + d, nband)}
        remote(eig, lefts.at[:, came], sem_left.at[0, d], sem_left.at[1, d], to).wait_recv()
        remote(rank, rank_band.at[came], sem_rank.at[0, d], sem_rank.at[1, d], to).wait_recv()
    next_rank.wait_recv()

    count = occ[0]
    row_mask = jnp.concatenate(
        [(rank_band[j] < count).astype(F32) for j in range(nband)], axis=1
    )
    col_mask = column_of((rank_next[...] < count).astype(F32), cols)
    col_mask = jnp.concatenate([col_mask] * nband, axis=1)
    mask[...] = row_mask * col_mask

    acc[...] = jnp.zeros_like(acc)

    def lefts_of(p, place):
        return jnp.concatenate([lefts[p, j, place, :] for j in range(nband)], axis=1)

    @pl.loop(0, CHUNKS)
    def _(c):
        right_copy(c).wait_recv()
        place = chunk(c)
        real, imag = rights[0, place, :].astype(F32), rights[1, place, :].astype(F32)
        turn, lift = cosine[place, :], sine[place, :]
        new_real = (turn * real + lift * imag).astype(BF16)
        new_imag = (turn * imag - lift * real).astype(BF16)
        paired = jnp.concatenate(
            [
                jnp.concatenate([new_real, new_imag], axis=1),
                jnp.concatenate([new_imag, -new_real], axis=1),
            ],
            axis=0,
        )
        stacked = jnp.concatenate([lefts_of(p, place) for p in range(2)], axis=0)
        acc[...] += across(paired, stacked, ((0,), (0,)))

    def share(b, d, e, slot):
        block = parts.at[slot, 0, :, part_of(b)]
        return remote(
            block, parts.at[slot, d, :, part_of(b)],
            sem_part.at[0, b, d, e], sem_part.at[1, b, d, e],
            {"orb": lax.rem(orb + d, norb), "band": lax.rem(band + e, nband)},
        )

    peers = [(d, e) for d in range(norb) for e in range(nband) if d + e > 0]
    peers = sorted(peers, key=lambda peer: -peer[0])
    rest = pl.ds(body, depth)
    for b in range(BLOCKS):
        tail_copy(b).wait_recv()
        real, imag = tail[0, part_of(b), :], tail[1, part_of(b), :]
        block = jnp.concatenate(
            [
                jnp.concatenate([real, imag], axis=1),
                jnp.concatenate([imag, -real], axis=1),
            ],
            axis=0,
        )
        whole = jnp.concatenate([lefts_of(p, rest) for p in range(2)], axis=0)
        term = across(block, whole, ((1,), (0,)))
        for p in range(2):
            total = acc[pl.ds(p * cols + b * width, width), :] + term[p * width : (p + 1) * width]
            parts[band, 0, p, part_of(b), :] = (total * mask[part_of(b), :]).astype(BF16)
        for d, e in peers:
            share(b, d, e, band).start()
    for b in range(BLOCKS):
        for d, e in peers:
            share(b, d, e, lax.rem(band + nband - e, nband)).wait_recv()

    halves = []
    for p in range(2):
        pieces = []
        for j in range(nband):
            total = parts[j, 0, p].astype(F32)
            for d in range(1, norb):
                total += parts[j, d, p].astype(F32)
            pieces.append(total)
        halves.append(jnp.transpose(jnp.concatenate(pieces, axis=0)))
    margins = jnp.concatenate(halves, axis=1)
    squares = jnp.sum(margins * margins, keepdims=True)
    iterate = margins * (ns_gain * lax.rsqrt(squares / count.astype(F32) + eps_mean))
    for _ in range(NS_STEPS):
        iterate = polar_step(iterate)

    def columns(j):
        at = [iterate[:, p * bands + j * cols : p * bands + (j + 1) * cols] for p in range(2)]
        return jnp.concatenate(at, axis=1)

    mine = columns(0)
    for j in range(1, nband):
        mine = jnp.where(band == j, columns(j), mine)
    cur[...] = mine.astype(BF16)
    height_of = bands // norb
    my_rows = pl.ds(pl.multiple_of(orb * height_of, height_of), height_of)
    scale = math.sqrt(bands)

    @pl.when(ka == 0)
    def _():
        full[...] = mine
        out[...] = full[my_rows, :] * scale
        pfx[...] = cur[my_rows, :]

    for level in range(levels_of(nka) if nka > 1 else 0):
        half = 1 << level
        first = ka < 2 * half
        for is_first in (True, False):
            if not is_first and 2 * half >= nka:
                continue
            height = height_of if is_first else bands
            source = pfx if is_first else cur
            here = first if is_first else jnp.logical_not(first)
            sending = jnp.logical_and(here, lax.rem(ka, 2 * half) == half - 1)
            taking = jnp.logical_and(here, lax.rem(ka // half, 2) == 1)

            def push(t, level=level, height=height, source=source):
                return remote(
                    source, got.at[level, band, pl.ds(0, height)],
                    sem_pre.at[0, level, t], sem_pre.at[1, level, 0],
                    {"ka": lax.rem(ka + t, nka)},
                )

            def pass_on(d, level=level, height=height):
                block = got.at[level, band, pl.ds(0, height)]
                return remote(
                    block, block, sem_fwd.at[0, level, d], sem_fwd.at[1, level, d],
                    {"band": lax.rem(band + d, nband)},
                )

            for t in range(half, 0, -1):
                @pl.when(jnp.logical_and(sending, ka + t < nka))
                def _(t=t, push=push):
                    push(t).start()

            for t in range(half, 0, -1):
                @pl.when(jnp.logical_and(sending, ka + t < nka))
                def _(t=t, push=push):
                    push(t).wait_send()

            @pl.when(taking)
            def _(level=level, height=height, is_first=is_first, push=push, pass_on=pass_on):
                push(1).wait_recv()
                for d in range(1, nband):
                    pass_on(d).start()
                for d in range(1, nband):
                    came = lax.rem(band + nband - d, nband)
                    block = got.at[level, came, pl.ds(0, height)]
                    remote(
                        block, block, sem_fwd.at[0, level, d], sem_fwd.at[1, level, d],
                        {"band": lax.rem(band + d, nband)},
                    ).wait_recv()
                pieces = [got[level, j, :height, :] for j in range(nband)]
                joined = merge(pieces, cur[...])
                if is_first:
                    out[...] = joined * scale
                    pfx[...] = joined.astype(BF16)
                else:
                    cur[...] = joined.astype(BF16)
                for d in range(1, nband):
                    pass_on(d).wait_send()

    for copy in band_sends + [next_rank]:
        copy.wait_send()

    @pl.loop(0, CHUNKS)
    def _(c):
        right_copy(c).wait_send()

    for b in range(BLOCKS):
        tail_copy(b).wait_send()
        for d, e in peers:
            share(b, d, e, band).wait_send()


def solution(mesh):
    nka, norb, nband = mesh.shape["ka"], mesh.shape["orb"], mesh.shape["band"]
    depth = levels_of(nka)

    def body(eigvecs, band_rank, occ_count, wrap_shift, orbital_site):
        rows, cols = eigvecs.shape[2], eigvecs.shape[3]
        bands = cols * nband
        share = bands // norb
        depth_of = rows // 4
        hbm = pl.BlockSpec(memory_space=pltpu.HBM)
        dma = pltpu.SemaphoreType.DMA
        result = pl.pallas_call(
            functools.partial(kernel, nka, norb, nband),
            out_shape=jax.ShapeDtypeStruct((share, 2 * cols), F32),
            in_specs=[hbm] * 5,
            out_specs=pl.BlockSpec(memory_space=pltpu.VMEM),
            scratch_shapes=[
                pltpu.VMEM((2, nband, rows, cols), BF16),
                pltpu.VMEM((2, rows - depth_of, cols), BF16),
                pltpu.VMEM((2, cols, depth_of), BF16),
                pltpu.VMEM((2, cols, depth_of), BF16),
                pltpu.VMEM((rows - depth_of, cols), F32),
                pltpu.VMEM((rows - depth_of, cols), F32),
                pltpu.VMEM((rows // 128, 128), F32),
                pltpu.VMEM((rows // 128, 128), F32),
                pltpu.VMEM((rows // 128, 128), F32),
                pltpu.VMEM((rows // 128, 128), F32),
                pltpu.SMEM((1,), jnp.int32),
                pltpu.SMEM((1,), jnp.int32),
                pltpu.VMEM((rows // 128, 128), jnp.int32),
                pltpu.VMEM((nband, 1, cols), jnp.int32),
                pltpu.VMEM((1, cols), jnp.int32),
                pltpu.VMEM((2 * cols, bands), F32),
                pltpu.VMEM((cols, bands), F32),
                pltpu.VMEM((nband, norb, 2, cols, bands), BF16),
                pltpu.VMEM((bands, 2 * cols), F32),
                pltpu.VMEM((bands, 2 * cols), BF16),
                pltpu.VMEM((share, 2 * cols), BF16),
                pltpu.VMEM((depth, nband, bands, 2 * cols), BF16),
                pltpu.SemaphoreType.REGULAR,
                dma,
                dma((4,)),
                dma((2, nband)),
                dma((2, nband)),
                dma((2,)),
                dma((2, CHUNKS)),
                dma((2, BLOCKS)),
                dma((2, BLOCKS, norb, nband)),
                dma((2, depth, max(2, 1 << (depth - 1)) + 1)),
                dma((2, depth, nband)),
            ],
            compiler_params=pltpu.CompilerParams(
                collective_id=0, has_side_effects=True,
                vmem_limit_bytes=67043328
            ),
            name="wilson",
        )(
            eigvecs.reshape(2, rows, cols), band_rank, occ_count, wrap_shift,
            orbital_site.reshape(rows // 128, 128),
        )
        return result.reshape(1, share, 2, cols)

    return jax.shard_map(
        body,
        mesh=mesh,
        in_specs=(
            P(("grp", "ka"), None, "orb", "band"),
            P(("grp", "ka"), "band"),
            P("grp"),
            P("grp"),
            P(("grp", "orb")),
        ),
        out_specs=P(("grp", "ka"), "orb", None, "band"),
        check_vma=False,
    )
```

```python
import functools
import math

import jax
import jax.numpy as jnp
from jax import lax
from jax.experimental import pallas as pl
from jax.experimental.pallas import tpu as pltpu
from jax.sharding import PartitionSpec as P

NS_STEPS = 8
SITES = 64
CHUNKS = 12
BLOCKS = 8
PIECES = 2

ns_gain = 0.7
eps_mean = 1e-06

MESH = pl.DeviceIdType.MESH
BF16 = jnp.bfloat16
F32 = jnp.float32


def levels_of(count):
    return max(1, (count - 1).bit_length())


def remote(src, dst, send_sem, recv_sem, device):
    return pltpu.make_async_remote_copy(
        src_ref=src,
        dst_ref=dst,
        send_sem=send_sem,
        recv_sem=recv_sem,
        device_id=device,
        device_id_type=MESH,
    )


def across(left, right, contract):
    return lax.dot_general(left, right, (contract, ((), ())), preferred_element_type=F32)


def column_of(row, width):
    return jnp.transpose(jnp.broadcast_to(row, (width, row.shape[1])))


def polar_step(iterate):
    half = iterate.shape[1] // 2
    rounded = iterate.astype(BF16)
    real, imag = rounded[:, :half], rounded[:, half:]
    tall = jnp.concatenate(
        [rounded, jnp.concatenate([imag, -real], axis=1)], axis=0
    )
    gram = across(tall, rounded, ((1,), (1,))).astype(BF16)
    rows = iterate.shape[0]
    wide = jnp.concatenate([gram[:rows], gram[rows:]], axis=1)
    block = jnp.concatenate(
        [rounded, jnp.concatenate([-imag, real], axis=1)], axis=0
    )
    product = across(wide, block, ((1,), (0,)))
    return 1.5 * iterate - 0.5 * product


def kernel(
    nka, norb, nband,
    eig, rank, occ_at, shift_at, site_at,
    out,
    lefts, rights, stage, tail, cosine, sine, angle_cos, angle_sin, tail_cos, tail_sin,
    occ, shift, site, rank_band, rank_next, acc, mask, parts, full, cur, pfx, got, sides, given, taken,
    ready,
    sem_own, sem_arg, sem_left, sem_rank, sem_next, sem_right, sem_tail, sem_part, sem_pre, sem_side, sem_fwd, sem_swap,
):
    ka, orb, band = lax.axis_index("ka"), lax.axis_index("orb"), lax.axis_index("band")
    rows, cols = eig.shape[1], eig.shape[2]
    bands = nband * cols
    depth = tail.shape[2]
    body = rows - depth
    step = body // CHUNKS
    width = cols // BLOCKS
    before = lax.rem(ka + nka - 1, nka)
    lanes = site.shape[1]

    barrier = pltpu.get_barrier_semaphore()
    for d in range(norb):
        for e in range(nband):
            if d + e > 0:
                to = {"orb": lax.rem(orb + d, norb), "band": lax.rem(band + e, nband)}
                pl.semaphore_signal(barrier, inc=1, device_id=to, device_id_type=MESH)
    for t in range(1, nka):
        @pl.when(ka + t < nka)
        def _(t=t):
            pl.semaphore_signal(
                barrier, inc=1, device_id={"ka": lax.rem(ka + t, nka)}, device_id_type=MESH
            )
    pl.semaphore_wait(barrier, norb * nband - 1 + ka)
    for t in range(1, nka):
        @pl.when(ka >= t)
        def _(t=t):
            pl.semaphore_signal(
                ready, inc=1, device_id={"ka": lax.rem(ka + nka - t, nka)}, device_id_type=MESH
            )

    def chunk(c):
        return pl.ds(pl.multiple_of(c * step, step), step)

    def right_copy(c):
        return remote(
            eig.at[:, chunk(c)], rights.at[:, chunk(c)],
            sem_right.at[0, c], sem_right.at[1, c], {"ka": before},
        )

    def part_of(b):
        return pl.ds(b * width, width)

    def tail_copy(b):
        return remote(
            stage.at[:, part_of(b)], tail.at[:, part_of(b)],
            sem_tail.at[0, b], sem_tail.at[1, b], {"ka": before},
        )

    next_rank = remote(rank, rank_next, sem_next.at[0], sem_next.at[1], {"ka": before})

    def start_right():
        next_rank.start()
        for c in range(CHUNKS):
            right_copy(c).start()

    @pl.when(ka > 0)
    def _():
        start_right()

    own = pltpu.make_async_copy(eig, lefts.at[:, band], sem_own)
    own.start()
    arguments = [
        pltpu.make_async_copy(src, dst, sem_arg.at[i])
        for i, (src, dst) in enumerate(
            ((occ_at, occ), (shift_at, shift), (site_at, site), (rank, rank_band.at[band]))
        )
    ]
    for copy in arguments:
        copy.start()
    band_sends = []
    for d in range(1, nband):
        to = {"band": lax.rem(band + d, nband)}
        copy = remote(eig, lefts.at[:, band], sem_left.at[0, d], sem_left.at[1, d], to)
        copy.start()
        band_sends.append(copy)
        copy = remote(rank, rank_band.at[band], sem_rank.at[0, d], sem_rank.at[1, d], to)
        copy.start()
        band_sends.append(copy)

    @pl.when(ka < nka - 1)
    def _():
        pl.semaphore_wait(ready, nka - 1 - ka)

    @pl.when(ka == 0)
    def _():
        start_right()

    for copy in arguments:
        copy.wait()

    at_end, at_start = ka == nka - 1, ka == 0
    angle = ((shift[0] * site[...]) & (SITES - 1)).astype(F32) * (2.0 * math.pi / SITES)
    turned, lifted = jnp.cos(angle), jnp.sin(angle)
    angle_cos[...] = jnp.where(at_end, turned, 1.0)
    angle_sin[...] = jnp.where(at_end, lifted, 0.0)
    tail_cos[...] = jnp.where(at_start, turned, 1.0)
    tail_sin[...] = jnp.where(at_start, lifted, 0.0)

    own.wait()

    @pl.loop(0, depth // lanes)
    def _(i):
        from_rows = pl.ds(pl.multiple_of(body + i * lanes, lanes), lanes)
        to_lanes = pl.ds(pl.multiple_of(i * lanes, lanes), lanes)
        real = jnp.transpose(lefts[0, band, from_rows, :].astype(F32))
        imag = jnp.transpose(lefts[1, band, from_rows, :].astype(F32))
        turn = tail_cos[pl.ds(body // lanes + i, 1), :]
        lift = tail_sin[pl.ds(body // lanes + i, 1), :]
        stage[0, :, to_lanes] = (turn * real + lift * imag).astype(BF16)
        stage[1, :, to_lanes] = (turn * imag - lift * real).astype(BF16)

    @pl.loop(0, body // lanes)
    def _(i):
        place = pl.ds(pl.multiple_of(i * lanes, lanes), lanes)
        cosine[place, :] = column_of(angle_cos[pl.ds(i, 1), :], cols)
        sine[place, :] = column_of(angle_sin[pl.ds(i, 1), :], cols)

    for b in range(BLOCKS):
        tail_copy(b).start()

    for d in range(1, nband):
        came = lax.rem(band + nband - d, nband)
        to = {"band": lax.rem(band + d, nband)}
        remote(eig, lefts.at[:, came], sem_left.at[0, d], sem_left.at[1, d], to).wait_recv()
        remote(rank, rank_band.at[came], sem_rank.at[0, d], sem_rank.at[1, d], to).wait_recv()
    next_rank.wait_recv()

    count = occ[0]
    row_mask = jnp.concatenate(
        [(rank_band[j] < count).astype(F32) for j in range(nband)], axis=1
    )
    col_mask = column_of((rank_next[...] < count).astype(F32), cols)
    col_mask = jnp.concatenate([col_mask] * nband, axis=1)
    mask[...] = row_mask * col_mask

    acc[...] = jnp.zeros_like(acc)

    def lefts_of(p, place):
        return jnp.concatenate([lefts[p, j, place, :] for j in range(nband)], axis=1)

    @pl.loop(0, CHUNKS)
    def _(c):
        right_copy(c).wait_recv()
        place = chunk(c)
        real, imag = rights[0, place, :].astype(F32), rights[1, place, :].astype(F32)
        turn, lift = cosine[place, :], sine[place, :]
        new_real = (turn * real + lift * imag).astype(BF16)
        new_imag = (turn * imag - lift * real).astype(BF16)
        paired = jnp.concatenate(
            [
                jnp.concatenate([new_real, new_imag], axis=1),
                jnp.concatenate([new_imag, -new_real], axis=1),
            ],
            axis=0,
        )
        stacked = jnp.concatenate([lefts_of(p, place) for p in range(2)], axis=0)
        acc[...] += across(paired, stacked, ((0,), (0,)))

    def share(b, d, e, slot):
        block = parts.at[slot, 0, :, part_of(b)]
        return remote(
            block, parts.at[slot, d, :, part_of(b)],
            sem_part.at[0, b, d, e], sem_part.at[1, b, d, e],
            {"orb": lax.rem(orb + d, norb), "band": lax.rem(band + e, nband)},
        )

    peers = [(d, e) for d in range(norb) for e in range(nband) if d + e > 0]
    peers = sorted(peers, key=lambda peer: -peer[0])
    rest = pl.ds(body, depth)
    for b in range(BLOCKS):
        tail_copy(b).wait_recv()
        real, imag = tail[0, part_of(b), :], tail[1, part_of(b), :]
        block = jnp.concatenate(
            [
                jnp.concatenate([real, imag], axis=1),
                jnp.concatenate([imag, -real], axis=1),
            ],
            axis=0,
        )
        whole = jnp.concatenate([lefts_of(p, rest) for p in range(2)], axis=0)
        term = across(block, whole, ((1,), (0,)))
        for p in range(2):
            total = acc[pl.ds(p * cols + b * width, width), :] + term[p * width : (p + 1) * width]
            parts[band, 0, p, part_of(b), :] = (total * mask[part_of(b), :]).astype(BF16)
        for d, e in peers:
            share(b, d, e, band).start()
    for b in range(BLOCKS):
        for d, e in peers:
            share(b, d, e, lax.rem(band + nband - e, nband)).wait_recv()

    halves = []
    for p in range(2):
        pieces = []
        for j in range(nband):
            total = parts[j, 0, p].astype(F32)
            for d in range(1, norb):
                total += parts[j, d, p].astype(F32)
            pieces.append(total)
        halves.append(jnp.transpose(jnp.concatenate(pieces, axis=0)))
    margins = jnp.concatenate(halves, axis=1)
    squares = jnp.sum(margins * margins, keepdims=True)
    iterate = margins * (ns_gain * lax.rsqrt(squares / count.astype(F32) + eps_mean))
    for _ in range(NS_STEPS):
        iterate = polar_step(iterate)

    real, imag = iterate[:, :bands].astype(BF16), iterate[:, bands:].astype(BF16)
    cur[:bands, :bands] = real
    cur[:bands, bands:] = imag
    cur[bands:, :bands] = -imag
    cur[bands:, bands:] = real
    levels = levels_of(nka) if nka > 1 else 0
    height = bands // (norb * nband)
    piece = height // PIECES
    side = bands // nband
    quarter = (orb * nband + band) * height
    scale = math.sqrt(bands)

    def rows_of(i):
        return pl.ds(i * piece, piece)

    def push(level, t, i):
        return remote(
            pfx.at[rows_of(i)], got.at[level, rows_of(i)],
            sem_pre.at[0, level, t, i], sem_pre.at[1, level, 0, i],
            {"ka": lax.rem(ka + t, nka)},
        )

    def push_side(level, t):
        mine = pl.ds(pl.multiple_of(band * side, side), side)
        return remote(
            cur.at[mine], sides.at[level, mine],
            sem_side.at[0, level, t], sem_side.at[1, level, 0],
            {"ka": lax.rem(ka + t, nka)},
        )

    def pass_on(level, d, slot):
        block = sides.at[level, pl.ds(pl.multiple_of(slot * side, side), side)]
        return remote(
            block, block, sem_fwd.at[0, level, d], sem_fwd.at[1, level, d],
            {"band": lax.rem(band + d, nband)},
        )

    def side_sent(level):
        half = 1 << level
        sending = jnp.logical_and(ka >= 2 * half, lax.rem(ka, 2 * half) == half - 1)
        for t in range(1, half + 1):
            @pl.when(jnp.logical_and(sending, ka + t < nka))
            def _(t=t):
                push_side(level, t).wait_send()

    def swap(i, d):
        return remote(
            given.at[lax.rem(band + d, nband), rows_of(i)], taken.at[band, rows_of(i)],
            sem_swap.at[0, i, d], sem_swap.at[1, i, d], {"band": lax.rem(band + d, nband)},
        )

    def each_push(level, i, act):
        for t in range(1, (1 << level) + 1):
            @pl.when(ka + t < nka)
            def _(t=t):
                act(push(level, t, i))

    @pl.when(ka == 0)
    def _():
        pfx[...] = cur[pl.ds(pl.multiple_of(quarter, height), height), :]
        for i in range(PIECES):
            if levels:
                each_push(0, i, lambda copy: copy.start())
        full[...] = iterate * scale
        share_of = bands // norb
        my_rows = pl.ds(pl.multiple_of(orb * share_of, share_of), share_of)
        for p in range(2):
            from_cols = pl.ds(pl.multiple_of(p * bands + band * cols, cols), cols)
            out[:, p * cols : (p + 1) * cols] = full[my_rows, from_cols]

    for level in range(levels):
        half = 1 << level
        later = ka >= 2 * half
        sending = jnp.logical_and(later, lax.rem(ka, 2 * half) == half - 1)
        taking = jnp.logical_and(later, lax.rem(ka // half, 2) == 1)
        if 2 * half < nka:
            if level:
                side_sent(level - 1)
            for t in range(1, half + 1):
                @pl.when(jnp.logical_and(sending, ka + t < nka))
                def _(t=t):
                    push_side(level, t).start()

            @pl.when(taking)
            def _(level=level):
                push_side(level, 1).wait_recv()
                for d in range(1, nband):
                    pass_on(level, d, band).start()
                for d in range(1, nband):
                    pass_on(level, d, lax.rem(band + nband - d, nband)).wait_recv()
                joined = across(sides[level], cur[...], ((1,), (0,))).astype(BF16)
                real, imag = joined[:, :bands], joined[:, bands:]
                cur[:bands, :bands] = real
                cur[:bands, bands:] = imag
                cur[bands:, :bands] = -imag
                cur[bands:, bands:] = real

        @pl.when(jnp.logical_and(ka >= half, ka < 2 * half))
        def _(level=level, half=half):
            for i in range(PIECES):
                push(level, 1, i).wait_recv()
                joined = across(got[level, rows_of(i), :], cur[...], ((1,), (0,)))
                if level + 1 < levels:
                    pfx[rows_of(i), :] = joined.astype(BF16)

                    @pl.when(ka == 2 * half - 1)
                    def _(i=i):
                        each_push(level + 1, i, lambda copy: copy.start())
                joined = joined * scale
                for j in range(nband):
                    for p in range(2):
                        at = p * bands + j * cols
                        given[j, rows_of(i), p * cols : (p + 1) * cols] = joined[:, at : at + cols]
                for d in range(1, nband):
                    swap(i, d).start()

    @pl.when(ka > 0)
    def _():
        def place_of(j):
            return pl.ds(pl.multiple_of(j * height, height), height)

        out[place_of(band), :] = given[band]
        for d in range(1, nband):
            came = lax.rem(band + nband - d, nband)
            for i in range(PIECES):
                swap(i, d).wait_recv()
            out[place_of(came), :] = taken[came]
        for d in range(1, nband):
            for i in range(PIECES):
                swap(i, d).wait_send()

    for level in range(levels):
        half = 1 << level
        later = ka >= 2 * half

        @pl.when(ka == half - 1)
        def _(level=level):
            for i in range(PIECES):
                each_push(level, i, lambda copy: copy.wait_send())

        if 2 * half < nka <= 4 * half:
            side_sent(level)
        if 2 * half < nka:
            @pl.when(jnp.logical_and(later, lax.rem(ka // half, 2) == 1))
            def _(level=level):
                for d in range(1, nband):
                    pass_on(level, d, band).wait_send()

    for copy in band_sends + [next_rank]:
        copy.wait_send()

    @pl.loop(0, CHUNKS)
    def _(c):
        right_copy(c).wait_send()

    for b in range(BLOCKS):
        tail_copy(b).wait_send()
        for d, e in peers:
            share(b, d, e, band).wait_send()


def solution(mesh):
    nka, norb, nband = mesh.shape["ka"], mesh.shape["orb"], mesh.shape["band"]
    depth = levels_of(nka)

    def body(eigvecs, band_rank, occ_count, wrap_shift, orbital_site):
        rows, cols = eigvecs.shape[2], eigvecs.shape[3]
        bands = cols * nband
        share = bands // norb
        depth_of = rows // 4
        height = share // nband
        hbm = pl.BlockSpec(memory_space=pltpu.HBM)
        dma = pltpu.SemaphoreType.DMA
        result = pl.pallas_call(
            functools.partial(kernel, nka, norb, nband),
            out_shape=jax.ShapeDtypeStruct((share, 2 * cols), F32),
            in_specs=[hbm] * 5,
            out_specs=pl.BlockSpec(memory_space=pltpu.VMEM),
            scratch_shapes=[
                pltpu.VMEM((2, nband, rows, cols), BF16),
                pltpu.VMEM((2, rows - depth_of, cols), BF16),
                pltpu.VMEM((2, cols, depth_of), BF16),
                pltpu.VMEM((2, cols, depth_of), BF16),
                pltpu.VMEM((rows - depth_of, cols), F32),
                pltpu.VMEM((rows - depth_of, cols), F32),
                pltpu.VMEM((rows // 128, 128), F32),
                pltpu.VMEM((rows // 128, 128), F32),
                pltpu.VMEM((rows // 128, 128), F32),
                pltpu.VMEM((rows // 128, 128), F32),
                pltpu.SMEM((1,), jnp.int32),
                pltpu.SMEM((1,), jnp.int32),
                pltpu.VMEM((rows // 128, 128), jnp.int32),
                pltpu.VMEM((nband, 1, cols), jnp.int32),
                pltpu.VMEM((1, cols), jnp.int32),
                pltpu.VMEM((2 * cols, bands), F32),
                pltpu.VMEM((cols, bands), F32),
                pltpu.VMEM((nband, norb, 2, cols, bands), BF16),
                pltpu.VMEM((bands, 2 * bands), F32),
                pltpu.VMEM((2 * bands, 2 * bands), BF16),
                pltpu.VMEM((height, 2 * bands), BF16),
                pltpu.VMEM((depth, height, 2 * bands), BF16),
                pltpu.VMEM((depth, bands, 2 * bands), BF16),
                pltpu.VMEM((nband, height, 2 * cols), F32),
                pltpu.VMEM((nband, height, 2 * cols), F32),
                pltpu.SemaphoreType.REGULAR,
                dma,
                dma((4,)),
                dma((2, nband)),
                dma((2, nband)),
                dma((2,)),
                dma((2, CHUNKS)),
                dma((2, BLOCKS)),
                dma((2, BLOCKS, norb, nband)),
                dma((2, depth, (1 << (depth - 1)) + 1, PIECES)),
                dma((2, depth, (1 << (depth - 1)) + 1)),
                dma((2, depth, nband)),
                dma((2, PIECES, nband)),
            ],
            compiler_params=pltpu.CompilerParams(
                collective_id=0, has_side_effects=True,
                vmem_limit_bytes=67043328
            ),
            name="wilson",
        )(
            eigvecs.reshape(2, rows, cols), band_rank, occ_count, wrap_shift,
            orbital_site.reshape(rows // 128, 128),
        )
        return result.reshape(1, share, 2, cols)

    return jax.shard_map(
        body,
        mesh=mesh,
        in_specs=(
            P(("grp", "ka"), None, "orb", "band"),
            P(("grp", "ka"), "band"),
            P("grp"),
            P("grp"),
            P(("grp", "orb")),
        ),
        out_specs=P(("grp", "ka"), "orb", None, "band"),
        check_vma=False,
    )
```

```python
import functools
import math

import jax
import jax.numpy as jnp
from jax import lax
from jax.experimental import pallas as pl
from jax.experimental.pallas import tpu as pltpu
from jax.sharding import PartitionSpec as P

NS_STEPS = 8
SITES = 64
CHUNKS = 12
BLOCKS = 8
PIECES = 2

ns_gain = 0.7
eps_mean = 1e-06

MESH = pl.DeviceIdType.MESH
BF16 = jnp.bfloat16
F32 = jnp.float32


def levels_of(count):
    return max(1, (count - 1).bit_length())


def remote(src, dst, send_sem, recv_sem, device):
    return pltpu.make_async_remote_copy(
        src_ref=src,
        dst_ref=dst,
        send_sem=send_sem,
        recv_sem=recv_sem,
        device_id=device,
        device_id_type=MESH,
    )


def across(left, right, contract):
    return lax.dot_general(left, right, (contract, ((), ())), preferred_element_type=F32)


def column_of(row, width):
    return jnp.transpose(jnp.broadcast_to(row, (width, row.shape[1])))


def polar_step(iterate):
    half = iterate.shape[1] // 2
    rounded = iterate.astype(BF16)
    real, imag = rounded[:, :half], rounded[:, half:]
    tall = jnp.concatenate(
        [rounded, jnp.concatenate([imag, -real], axis=1)], axis=0
    )
    gram = across(tall, rounded, ((1,), (1,))).astype(BF16)
    rows = iterate.shape[0]
    wide = jnp.concatenate([gram[:rows], gram[rows:]], axis=1)
    block = jnp.concatenate(
        [rounded, jnp.concatenate([-imag, real], axis=1)], axis=0
    )
    product = across(wide, block, ((1,), (0,)))
    return 1.5 * iterate - 0.5 * product


def kernel(
    nka, norb, nband,
    eig, rank, occ_at, shift_at, site_at,
    out,
    lefts, rights, stage, tail, cosine, sine, angle_cos, angle_sin, tail_cos, tail_sin,
    occ, shift, site, rank_band, rank_next, acc, mask, parts, full, cur, pfx, got, sides, given, taken,
    ready,
    sem_own, sem_arg, sem_left, sem_rank, sem_next, sem_right, sem_tail, sem_part, sem_pre, sem_side, sem_swap,
):
    ka, orb, band = lax.axis_index("ka"), lax.axis_index("orb"), lax.axis_index("band")
    rows, cols = eig.shape[1], eig.shape[2]
    bands = nband * cols
    depth = tail.shape[2]
    body = rows - depth
    step = body // CHUNKS
    width = cols // BLOCKS
    before = lax.rem(ka + nka - 1, nka)
    lanes = site.shape[1]

    barrier = pltpu.get_barrier_semaphore()
    for d in range(norb):
        for e in range(nband):
            if d + e > 0:
                to = {"orb": lax.rem(orb + d, norb), "band": lax.rem(band + e, nband)}
                pl.semaphore_signal(barrier, inc=1, device_id=to, device_id_type=MESH)
    for t in range(1, nka):
        @pl.when(ka + t < nka)
        def _(t=t):
            pl.semaphore_signal(
                barrier, inc=1, device_id={"ka": lax.rem(ka + t, nka)}, device_id_type=MESH
            )
    pl.semaphore_wait(barrier, norb * nband - 1 + ka)
    for t in range(1, nka):
        @pl.when(ka >= t)
        def _(t=t):
            pl.semaphore_signal(
                ready, inc=1, device_id={"ka": lax.rem(ka + nka - t, nka)}, device_id_type=MESH
            )

    def chunk(c):
        return pl.ds(pl.multiple_of(c * step, step), step)

    def right_copy(c):
        return remote(
            eig.at[:, chunk(c)], rights.at[:, chunk(c)],
            sem_right.at[0, c], sem_right.at[1, c], {"ka": before},
        )

    def part_of(b):
        return pl.ds(b * width, width)

    def tail_copy(b):
        return remote(
            stage.at[:, part_of(b)], tail.at[:, part_of(b)],
            sem_tail.at[0, b], sem_tail.at[1, b], {"ka": before},
        )

    next_rank = remote(rank, rank_next, sem_next.at[0], sem_next.at[1], {"ka": before})

    def start_right():
        next_rank.start()
        for c in range(CHUNKS):
            right_copy(c).start()

    @pl.when(ka > 0)
    def _():
        start_right()

    own = pltpu.make_async_copy(eig, lefts.at[:, band], sem_own)
    own.start()
    arguments = [
        pltpu.make_async_copy(src, dst, sem_arg.at[i])
        for i, (src, dst) in enumerate(
            ((occ_at, occ), (shift_at, shift), (site_at, site), (rank, rank_band.at[band]))
        )
    ]
    for copy in arguments:
        copy.start()
    band_sends = []
    for d in range(1, nband):
        to = {"band": lax.rem(band + d, nband)}
        copy = remote(eig, lefts.at[:, band], sem_left.at[0, d], sem_left.at[1, d], to)
        copy.start()
        band_sends.append(copy)
        copy = remote(rank, rank_band.at[band], sem_rank.at[0, d], sem_rank.at[1, d], to)
        copy.start()
        band_sends.append(copy)

    @pl.when(ka < nka - 1)
    def _():
        pl.semaphore_wait(ready, nka - 1 - ka)

    @pl.when(ka == 0)
    def _():
        start_right()

    for copy in arguments:
        copy.wait()

    at_end, at_start = ka == nka - 1, ka == 0
    angle = ((shift[0] * site[...]) & (SITES - 1)).astype(F32) * (2.0 * math.pi / SITES)
    turned, lifted = jnp.cos(angle), jnp.sin(angle)
    angle_cos[...] = jnp.where(at_end, turned, 1.0)
    angle_sin[...] = jnp.where(at_end, lifted, 0.0)
    tail_cos[...] = jnp.where(at_start, turned, 1.0)
    tail_sin[...] = jnp.where(at_start, lifted, 0.0)

    own.wait()

    @pl.loop(0, depth // lanes)
    def _(i):
        from_rows = pl.ds(pl.multiple_of(body + i * lanes, lanes), lanes)
        to_lanes = pl.ds(pl.multiple_of(i * lanes, lanes), lanes)
        real = jnp.transpose(lefts[0, band, from_rows, :].astype(F32))
        imag = jnp.transpose(lefts[1, band, from_rows, :].astype(F32))
        turn = tail_cos[pl.ds(body // lanes + i, 1), :]
        lift = tail_sin[pl.ds(body // lanes + i, 1), :]
        stage[0, :, to_lanes] = (turn * real + lift * imag).astype(BF16)
        stage[1, :, to_lanes] = (turn * imag - lift * real).astype(BF16)

    @pl.loop(0, body // lanes)
    def _(i):
        place = pl.ds(pl.multiple_of(i * lanes, lanes), lanes)
        cosine[place, :] = column_of(angle_cos[pl.ds(i, 1), :], cols)
        sine[place, :] = column_of(angle_sin[pl.ds(i, 1), :], cols)

    for b in range(BLOCKS):
        tail_copy(b).start()

    for d in range(1, nband):
        came = lax.rem(band + nband - d, nband)
        to = {"band": lax.rem(band + d, nband)}
        remote(eig, lefts.at[:, came], sem_left.at[0, d], sem_left.at[1, d], to).wait_recv()
        remote(rank, rank_band.at[came], sem_rank.at[0, d], sem_rank.at[1, d], to).wait_recv()
    next_rank.wait_recv()

    count = occ[0]
    row_mask = jnp.concatenate(
        [(rank_band[j] < count).astype(F32) for j in range(nband)], axis=1
    )
    col_mask = column_of((rank_next[...] < count).astype(F32), cols)
    col_mask = jnp.concatenate([col_mask] * nband, axis=1)
    mask[...] = row_mask * col_mask

    acc[...] = jnp.zeros_like(acc)

    def lefts_of(p, place):
        return jnp.concatenate([lefts[p, j, place, :] for j in range(nband)], axis=1)

    @pl.loop(0, CHUNKS)
    def _(c):
        right_copy(c).wait_recv()
        place = chunk(c)
        real, imag = rights[0, place, :].astype(F32), rights[1, place, :].astype(F32)
        turn, lift = cosine[place, :], sine[place, :]
        new_real = (turn * real + lift * imag).astype(BF16)
        new_imag = (turn * imag - lift * real).astype(BF16)
        paired = jnp.concatenate(
            [
                jnp.concatenate([new_real, new_imag], axis=1),
                jnp.concatenate([new_imag, -new_real], axis=1),
            ],
            axis=0,
        )
        stacked = jnp.concatenate([lefts_of(p, place) for p in range(2)], axis=0)
        acc[...] += across(paired, stacked, ((0,), (0,)))

    lead = nband - 1
    leads = band == lead

    def share(b, d, slot):
        return remote(
            parts.at[slot, 0, :, part_of(b)], parts.at[slot, d, :, part_of(b)],
            sem_part.at[0, b, d, slot], sem_part.at[1, b, d, slot],
            {"orb": lax.rem(orb + d, norb), "band": lead},
        )

    def each_share(b, act):
        for d in range(norb - 1, 0, -1):
            act(share(b, d, band))

        @pl.when(jnp.logical_not(leads))
        def _():
            act(share(b, 0, band))

    rest = pl.ds(body, depth)
    for b in range(BLOCKS):
        tail_copy(b).wait_recv()
        real, imag = tail[0, part_of(b), :], tail[1, part_of(b), :]
        block = jnp.concatenate(
            [
                jnp.concatenate([real, imag], axis=1),
                jnp.concatenate([imag, -real], axis=1),
            ],
            axis=0,
        )
        whole = jnp.concatenate([lefts_of(p, rest) for p in range(2)], axis=0)
        term = across(block, whole, ((1,), (0,)))
        for p in range(2):
            total = acc[pl.ds(p * cols + b * width, width), :] + term[p * width : (p + 1) * width]
            parts[band, 0, p, part_of(b), :] = (total * mask[part_of(b), :]).astype(BF16)
        each_share(b, lambda copy: copy.start())
    levels = levels_of(nka) if nka > 1 else 0
    height = bands // norb
    piece = height // PIECES
    scale = math.sqrt(bands)

    def rows_of(i):
        return pl.ds(i * piece, piece)

    def swap(i, j):
        return remote(
            given.at[j, rows_of(i)], taken.at[rows_of(i)],
            sem_swap.at[0, i, j], sem_swap.at[1, i, 0], {"band": j},
        )

    def push(level, t, i):
        return remote(
            pfx.at[rows_of(i)], got.at[level, rows_of(i)],
            sem_pre.at[0, level, t, i], sem_pre.at[1, level, 0, i],
            {"ka": lax.rem(ka + t, nka)},
        )

    def each_push(level, i, act):
        for t in range(1, (1 << level) + 1):
            @pl.when(ka + t < nka)
            def _(t=t):
                act(push(level, t, i))

    def push_side(level, t):
        return remote(
            cur.at[pl.ds(0, bands)], sides.at[level],
            sem_side.at[0, level, t], sem_side.at[1, level, 0],
            {"ka": lax.rem(ka + t, nka)},
        )

    def side_sent(level):
        half = 1 << level
        sending = jnp.logical_and(ka >= 2 * half, lax.rem(ka, 2 * half) == half - 1)
        for t in range(1, half + 1):
            @pl.when(jnp.logical_and(sending, ka + t < nka))
            def _(t=t):
                push_side(level, t).wait_send()

    def set_cur(matrix):
        real, imag = matrix[:, :bands], matrix[:, bands:]
        cur[:bands, :bands] = real
        cur[:bands, bands:] = imag
        cur[bands:, :bands] = -imag
        cur[bands:, bands:] = real

    def hand_out(i, joined):
        for j in range(nband):
            for p in range(2):
                at = p * bands + j * cols
                given[j, rows_of(i), p * cols : (p + 1) * cols] = joined[:, at : at + cols] * scale
            if j != lead:
                swap(i, j).start()

    @pl.when(leads)
    def _():
        for b in range(BLOCKS):
            for d in range(norb):
                for j in range(nband):
                    if (d, j) != (0, lead):
                        share(b, d, j).wait_recv()
        halves = []
        for p in range(2):
            pieces = []
            for j in range(nband):
                total = parts[j, 0, p].astype(F32)
                for d in range(1, norb):
                    total += parts[j, d, p].astype(F32)
                pieces.append(total)
            halves.append(jnp.transpose(jnp.concatenate(pieces, axis=0)))
        margins = jnp.concatenate(halves, axis=1)
        squares = jnp.sum(margins * margins, keepdims=True)
        iterate = margins * (ns_gain * lax.rsqrt(squares / count.astype(F32) + eps_mean))
        for _ in range(NS_STEPS):
            iterate = polar_step(iterate)
        set_cur(iterate.astype(BF16))
        full[...] = iterate

        @pl.when(ka == 0)
        def _():
            my_rows = pl.ds(pl.multiple_of(orb * height, height), height)
            pfx[...] = cur[my_rows, :]
            for i in range(PIECES):
                if levels:
                    each_push(0, i, lambda copy: copy.start())
            for i in range(PIECES):
                here = pl.ds(pl.multiple_of(orb * height + i * piece, piece), piece)
                hand_out(i, full[here, :])

        for level in range(levels):
            half = 1 << level
            later = ka >= 2 * half
            sending = jnp.logical_and(later, lax.rem(ka, 2 * half) == half - 1)
            taking = jnp.logical_and(later, lax.rem(ka // half, 2) == 1)
            if 2 * half < nka:
                if level:
                    side_sent(level - 1)
                for t in range(1, half + 1):
                    @pl.when(jnp.logical_and(sending, ka + t < nka))
                    def _(t=t):
                        push_side(level, t).start()

                @pl.when(taking)
                def _(level=level):
                    push_side(level, 1).wait_recv()
                    set_cur(across(sides[level], cur[...], ((1,), (0,))).astype(BF16))

            @pl.when(jnp.logical_and(ka >= half, ka < 2 * half))
            def _(level=level, half=half):
                for i in range(PIECES):
                    push(level, 1, i).wait_recv()
                    joined = across(got[level, rows_of(i), :], cur[...], ((1,), (0,)))
                    if level + 1 < levels:
                        pfx[rows_of(i), :] = joined.astype(BF16)

                        @pl.when(ka == 2 * half - 1)
                        def _(i=i):
                            each_push(level + 1, i, lambda copy: copy.start())
                    hand_out(i, joined)

        out[...] = given[lead]
        for i in range(PIECES):
            for j in range(lead):
                swap(i, j).wait_send()
        for level in range(levels):
            half = 1 << level

            @pl.when(ka == half - 1)
            def _(level=level):
                for i in range(PIECES):
                    each_push(level, i, lambda copy: copy.wait_send())

            if 2 * half < nka <= 4 * half:
                side_sent(level)

    @pl.when(jnp.logical_not(leads))
    def _():
        for i in range(PIECES):
            swap(i, band).wait_recv()
        out[...] = taken[...]

    for copy in band_sends + [next_rank]:
        copy.wait_send()

    @pl.loop(0, CHUNKS)
    def _(c):
        right_copy(c).wait_send()

    for b in range(BLOCKS):
        tail_copy(b).wait_send()
        each_share(b, lambda copy: copy.wait_send())


def solution(mesh):
    nka, norb, nband = mesh.shape["ka"], mesh.shape["orb"], mesh.shape["band"]
    depth = levels_of(nka)

    def body(eigvecs, band_rank, occ_count, wrap_shift, orbital_site):
        rows, cols = eigvecs.shape[2], eigvecs.shape[3]
        bands = cols * nband
        share = bands // norb
        depth_of = rows // 4
        hbm = pl.BlockSpec(memory_space=pltpu.HBM)
        dma = pltpu.SemaphoreType.DMA
        result = pl.pallas_call(
            functools.partial(kernel, nka, norb, nband),
            out_shape=jax.ShapeDtypeStruct((share, 2 * cols), F32),
            in_specs=[hbm] * 5,
            out_specs=pl.BlockSpec(memory_space=pltpu.VMEM),
            scratch_shapes=[
                pltpu.VMEM((2, nband, rows, cols), BF16),
                pltpu.VMEM((2, rows - depth_of, cols), BF16),
                pltpu.VMEM((2, cols, depth_of), BF16),
                pltpu.VMEM((2, cols, depth_of), BF16),
                pltpu.VMEM((rows - depth_of, cols), F32),
                pltpu.VMEM((rows - depth_of, cols), F32),
                pltpu.VMEM((rows // 128, 128), F32),
                pltpu.VMEM((rows // 128, 128), F32),
                pltpu.VMEM((rows // 128, 128), F32),
                pltpu.VMEM((rows // 128, 128), F32),
                pltpu.SMEM((1,), jnp.int32),
                pltpu.SMEM((1,), jnp.int32),
                pltpu.VMEM((rows // 128, 128), jnp.int32),
                pltpu.VMEM((nband, 1, cols), jnp.int32),
                pltpu.VMEM((1, cols), jnp.int32),
                pltpu.VMEM((2 * cols, bands), F32),
                pltpu.VMEM((cols, bands), F32),
                pltpu.VMEM((nband, norb, 2, cols, bands), BF16),
                pltpu.VMEM((bands, 2 * bands), F32),
                pltpu.VMEM((2 * bands, 2 * bands), BF16),
                pltpu.VMEM((share, 2 * bands), BF16),
                pltpu.VMEM((depth, share, 2 * bands), BF16),
                pltpu.VMEM((depth, bands, 2 * bands), BF16),
                pltpu.VMEM((nband, share, 2 * cols), F32),
                pltpu.VMEM((share, 2 * cols), F32),
                pltpu.SemaphoreType.REGULAR,
                dma,
                dma((4,)),
                dma((2, nband)),
                dma((2, nband)),
                dma((2,)),
                dma((2, CHUNKS)),
                dma((2, BLOCKS)),
                dma((2, BLOCKS, norb, nband)),
                dma((2, depth, (1 << (depth - 1)) + 1, PIECES)),
                dma((2, depth, (1 << (depth - 1)) + 1)),
                dma((2, PIECES, nband)),
            ],
            compiler_params=pltpu.CompilerParams(
                collective_id=0, has_side_effects=True,
                vmem_limit_bytes=67043328
            ),
            name="wilson",
        )(
            eigvecs.reshape(2, rows, cols), band_rank, occ_count, wrap_shift,
            orbital_site.reshape(rows // 128, 128),
        )
        return result.reshape(1, share, 2, cols)

    return jax.shard_map(
        body,
        mesh=mesh,
        in_specs=(
            P(("grp", "ka"), None, "orb", "band"),
            P(("grp", "ka"), "band"),
            P("grp"),
            P("grp"),
            P(("grp", "orb")),
        ),
        out_specs=P(("grp", "ka"), "orb", None, "band"),
        check_vma=False,
    )
```

```python
import functools
import math

import jax
import jax.numpy as jnp
from jax import lax
from jax.experimental import pallas as pl
from jax.experimental.pallas import tpu as pltpu
from jax.sharding import PartitionSpec as P

NS_STEPS = 8
SITES = 64
CHUNKS = 12
BLOCKS = 8
PIECES = 2

ns_gain = 0.7
eps_mean = 1e-06

MESH = pl.DeviceIdType.MESH
BF16 = jnp.bfloat16
F32 = jnp.float32


def levels_of(count):
    return max(1, (count - 1).bit_length())


def remote(src, dst, send_sem, recv_sem, device):
    return pltpu.make_async_remote_copy(
        src_ref=src,
        dst_ref=dst,
        send_sem=send_sem,
        recv_sem=recv_sem,
        device_id=device,
        device_id_type=MESH,
    )


def across(left, right, contract):
    return lax.dot_general(left, right, (contract, ((), ())), preferred_element_type=F32)


def column_of(row, width):
    return jnp.transpose(jnp.broadcast_to(row, (width, row.shape[1])))


def polar_step(iterate):
    half = iterate.shape[1] // 2
    rounded = iterate.astype(BF16)
    real, imag = rounded[:, :half], rounded[:, half:]
    tall = jnp.concatenate(
        [rounded, jnp.concatenate([imag, -real], axis=1)], axis=0
    )
    gram = across(tall, rounded, ((1,), (1,))).astype(BF16)
    rows = iterate.shape[0]
    wide = jnp.concatenate([gram[:rows], gram[rows:]], axis=1)
    block = jnp.concatenate(
        [rounded, jnp.concatenate([-imag, real], axis=1)], axis=0
    )
    product = across(wide, block, ((1,), (0,)))
    return 1.5 * iterate - 0.5 * product


def kernel(
    nka, norb, nband,
    eig, rank, occ_at, shift_at, site_at,
    out,
    lefts, rights, stage, tail, cosine, sine, angle_cos, angle_sin, tail_cos, tail_sin,
    occ, shift, site, rank_band, rank_next, acc, mask, parts, full, cur, pfx, got, sides, given, taken,
    ready,
    sem_own, sem_arg, sem_left, sem_rank, sem_next, sem_right, sem_tail, sem_part, sem_pre, sem_side, sem_swap,
):
    ka, orb, band = lax.axis_index("ka"), lax.axis_index("orb"), lax.axis_index("band")
    rows, cols = eig.shape[1], eig.shape[2]
    bands = nband * cols
    depth = tail.shape[2]
    body = rows - depth
    step = body // CHUNKS
    width = cols // BLOCKS
    before = lax.rem(ka + nka - 1, nka)
    lanes = site.shape[1]

    barrier = pltpu.get_barrier_semaphore()
    for d in range(norb):
        for e in range(nband):
            if d + e > 0:
                to = {"orb": lax.rem(orb + d, norb), "band": lax.rem(band + e, nband)}
                pl.semaphore_signal(barrier, inc=1, device_id=to, device_id_type=MESH)
    for t in range(1, nka):
        @pl.when(ka + t < nka)
        def _(t=t):
            pl.semaphore_signal(
                barrier, inc=1, device_id={"ka": lax.rem(ka + t, nka)}, device_id_type=MESH
            )
    pl.semaphore_wait(barrier, norb * nband - 1 + ka)
    for t in range(1, nka):
        @pl.when(ka >= t)
        def _(t=t):
            pl.semaphore_signal(
                ready, inc=1, device_id={"ka": lax.rem(ka + nka - t, nka)}, device_id_type=MESH
            )

    def chunk(c):
        return pl.ds(pl.multiple_of(c * step, step), step)

    def right_copy(c):
        return remote(
            eig.at[:, chunk(c)], rights.at[:, chunk(c)],
            sem_right.at[0, c], sem_right.at[1, c], {"ka": before},
        )

    def part_of(b):
        return pl.ds(b * width, width)

    def tail_copy(b):
        return remote(
            stage.at[:, part_of(b)], tail.at[:, part_of(b)],
            sem_tail.at[0, b], sem_tail.at[1, b], {"ka": before},
        )

    next_rank = remote(rank, rank_next, sem_next.at[0], sem_next.at[1], {"ka": before})

    def start_right():
        next_rank.start()
        for c in range(CHUNKS):
            right_copy(c).start()

    @pl.when(ka > 0)
    def _():
        start_right()

    own = pltpu.make_async_copy(eig, lefts.at[:, band], sem_own)
    own.start()
    arguments = [
        pltpu.make_async_copy(src, dst, sem_arg.at[i])
        for i, (src, dst) in enumerate(
            ((occ_at, occ), (shift_at, shift), (site_at, site), (rank, rank_band.at[band]))
        )
    ]
    for copy in arguments:
        copy.start()
    band_sends = []
    for d in range(1, nband):
        to = {"band": lax.rem(band + d, nband)}
        copy = remote(eig, lefts.at[:, band], sem_left.at[0, d], sem_left.at[1, d], to)
        copy.start()
        band_sends.append(copy)
        copy = remote(rank, rank_band.at[band], sem_rank.at[0, d], sem_rank.at[1, d], to)
        copy.start()
        band_sends.append(copy)

    @pl.when(ka < nka - 1)
    def _():
        pl.semaphore_wait(ready, nka - 1 - ka)

    @pl.when(ka == 0)
    def _():
        start_right()

    for copy in arguments:
        copy.wait()

    at_end, at_start = ka == nka - 1, ka == 0
    angle = ((shift[0] * site[...]) & (SITES - 1)).astype(F32) * (2.0 * math.pi / SITES)
    turned, lifted = jnp.cos(angle), jnp.sin(angle)
    angle_cos[...] = jnp.where(at_end, turned, 1.0)
    angle_sin[...] = jnp.where(at_end, lifted, 0.0)
    tail_cos[...] = jnp.where(at_start, turned, 1.0)
    tail_sin[...] = jnp.where(at_start, lifted, 0.0)

    own.wait()

    @pl.loop(0, depth // lanes)
    def _(i):
        from_rows = pl.ds(pl.multiple_of(body + i * lanes, lanes), lanes)
        to_lanes = pl.ds(pl.multiple_of(i * lanes, lanes), lanes)
        real = jnp.transpose(lefts[0, band, from_rows, :].astype(F32))
        imag = jnp.transpose(lefts[1, band, from_rows, :].astype(F32))
        turn = tail_cos[pl.ds(body // lanes + i, 1), :]
        lift = tail_sin[pl.ds(body // lanes + i, 1), :]
        stage[0, :, to_lanes] = (turn * real + lift * imag).astype(BF16)
        stage[1, :, to_lanes] = (turn * imag - lift * real).astype(BF16)

    @pl.loop(0, body // lanes)
    def _(i):
        place = pl.ds(pl.multiple_of(i * lanes, lanes), lanes)
        cosine[place, :] = column_of(angle_cos[pl.ds(i, 1), :], cols)
        sine[place, :] = column_of(angle_sin[pl.ds(i, 1), :], cols)

    for b in range(BLOCKS):
        tail_copy(b).start()

    for d in range(1, nband):
        came = lax.rem(band + nband - d, nband)
        to = {"band": lax.rem(band + d, nband)}
        remote(eig, lefts.at[:, came], sem_left.at[0, d], sem_left.at[1, d], to).wait_recv()
        remote(rank, rank_band.at[came], sem_rank.at[0, d], sem_rank.at[1, d], to).wait_recv()
    next_rank.wait_recv()

    count = occ[0]
    row_mask = jnp.concatenate(
        [(rank_band[j] < count).astype(F32) for j in range(nband)], axis=1
    )
    col_mask = column_of((rank_next[...] < count).astype(F32), cols)
    col_mask = jnp.concatenate([col_mask] * nband, axis=1)
    mask[...] = row_mask * col_mask

    acc[...] = jnp.zeros_like(acc)

    def lefts_of(p, place):
        return jnp.concatenate([lefts[p, j, place, :] for j in range(nband)], axis=1)

    @pl.loop(0, CHUNKS)
    def _(c):
        right_copy(c).wait_recv()
        place = chunk(c)
        real, imag = rights[0, place, :].astype(F32), rights[1, place, :].astype(F32)
        turn, lift = cosine[place, :], sine[place, :]
        new_real = (turn * real + lift * imag).astype(BF16)
        new_imag = (turn * imag - lift * real).astype(BF16)
        paired = jnp.concatenate(
            [
                jnp.concatenate([new_real, new_imag], axis=1),
                jnp.concatenate([new_imag, -new_real], axis=1),
            ],
            axis=0,
        )
        stacked = jnp.concatenate([lefts_of(p, place) for p in range(2)], axis=0)
        acc[...] += across(paired, stacked, ((0,), (0,)))

    lead = nband - 1
    leads = band == lead

    def share(b, d, slot):
        return remote(
            parts.at[slot, 0, :, part_of(b)], parts.at[slot, d, :, part_of(b)],
            sem_part.at[0, b, d, slot], sem_part.at[1, b, d, slot],
            {"orb": lax.rem(orb + d, norb), "band": lead},
        )

    def each_share(b, act):
        for d in range(norb - 1, 0, -1):
            act(share(b, d, band))

        @pl.when(jnp.logical_not(leads))
        def _():
            act(share(b, 0, band))

    rest = pl.ds(body, depth)
    for b in range(BLOCKS):
        tail_copy(b).wait_recv()
        real, imag = tail[0, part_of(b), :], tail[1, part_of(b), :]
        block = jnp.concatenate(
            [
                jnp.concatenate([real, imag], axis=1),
                jnp.concatenate([imag, -real], axis=1),
            ],
            axis=0,
        )
        whole = jnp.concatenate([lefts_of(p, rest) for p in range(2)], axis=0)
        term = across(block, whole, ((1,), (0,)))
        for p in range(2):
            total = acc[pl.ds(p * cols + b * width, width), :] + term[p * width : (p + 1) * width]
            parts[band, 0, p, part_of(b), :] = (total * mask[part_of(b), :]).astype(BF16)
        each_share(b, lambda copy: copy.start())
    levels = levels_of(nka) if nka > 1 else 0
    height = bands // norb
    piece = height // PIECES
    scale = math.sqrt(bands)

    def rows_of(i):
        return pl.ds(i * piece, piece)

    def swap(i, j):
        return remote(
            given.at[j, rows_of(i)], taken.at[rows_of(i)],
            sem_swap.at[0, i, j], sem_swap.at[1, i, 0], {"band": j},
        )

    def push(level, t, i):
        return remote(
            pfx.at[rows_of(i)], got.at[level, rows_of(i)],
            sem_pre.at[0, level, t, i], sem_pre.at[1, level, 0, i],
            {"ka": lax.rem(ka + t, nka)},
        )

    def each_push(level, i, act):
        for t in range(1, (1 << level) + 1):
            @pl.when(ka + t < nka)
            def _(t=t):
                act(push(level, t, i))

    def push_side(level, t):
        return remote(
            cur.at[pl.ds(0, bands)], sides.at[level],
            sem_side.at[0, level, t], sem_side.at[1, level, 0],
            {"ka": lax.rem(ka + t, nka)},
        )

    def side_sent(level):
        half = 1 << level
        sending = jnp.logical_and(ka >= 2 * half, lax.rem(ka, 2 * half) == half - 1)
        for t in range(1, half + 1):
            @pl.when(jnp.logical_and(sending, ka + t < nka))
            def _(t=t):
                push_side(level, t).wait_send()

    def set_cur(matrix):
        real, imag = matrix[:, :bands], matrix[:, bands:]
        cur[:bands, :bands] = real
        cur[:bands, bands:] = imag
        cur[bands:, :bands] = -imag
        cur[bands:, bands:] = real

    def hand_out(i, joined):
        for j in range(nband):
            for p in range(2):
                at = p * bands + j * cols
                given[j, rows_of(i), p * cols : (p + 1) * cols] = joined[:, at : at + cols] * scale
            if j != lead:
                swap(i, j).start()

    @pl.when(leads)
    def _():
        for b in range(BLOCKS):
            for d in range(norb):
                for j in range(nband):
                    if (d, j) != (0, lead):
                        share(b, d, j).wait_recv()
        halves = []
        for p in range(2):
            pieces = []
            for j in range(nband):
                total = parts[j, 0, p].astype(F32)
                for d in range(1, norb):
                    total += parts[j, d, p].astype(F32)
                pieces.append(total)
            halves.append(jnp.transpose(jnp.concatenate(pieces, axis=0)))
        margins = jnp.concatenate(halves, axis=1)
        squares = jnp.sum(margins * margins, keepdims=True)
        iterate = margins * (ns_gain * lax.rsqrt(squares / count.astype(F32) + eps_mean))
        for _ in range(NS_STEPS):
            iterate = polar_step(iterate)
        set_cur(iterate.astype(BF16))
        full[...] = iterate

        @pl.when(ka == 0)
        def _():
            my_rows = pl.ds(pl.multiple_of(orb * height, height), height)
            pfx[...] = cur[my_rows, :]
            for i in range(PIECES):
                if levels:
                    each_push(0, i, lambda copy: copy.start())
            for i in range(PIECES):
                here = pl.ds(pl.multiple_of(orb * height + i * piece, piece), piece)
                hand_out(i, full[here, :])

        for level in range(levels):
            half = 1 << level
            later = ka >= 2 * half
            sending = jnp.logical_and(later, lax.rem(ka, 2 * half) == half - 1)
            taking = jnp.logical_and(later, lax.rem(ka // half, 2) == 1)
            if 2 * half < nka:
                if level:
                    side_sent(level - 1)
                for t in range(1, half + 1):
                    @pl.when(jnp.logical_and(sending, ka + t < nka))
                    def _(t=t):
                        push_side(level, t).start()

                @pl.when(taking)
                def _(level=level):
                    push_side(level, 1).wait_recv()
                    set_cur(across(sides[level], cur[...], ((1,), (0,))).astype(BF16))

            @pl.when(jnp.logical_and(ka >= half, ka < 2 * half))
            def _(level=level, half=half):
                for i in range(PIECES):
                    push(level, 1, i).wait_recv()
                    joined = across(got[level, rows_of(i), :], cur[...], ((1,), (0,)))
                    if level + 1 < levels:
                        pfx[rows_of(i), :] = joined.astype(BF16)

                        @pl.when(ka == 2 * half - 1)
                        def _(i=i):
                            each_push(level + 1, i, lambda copy: copy.start())
                    hand_out(i, joined)

        out[...] = given[lead]
        for i in range(PIECES):
            for j in range(lead):
                swap(i, j).wait_send()
        for level in range(levels):
            half = 1 << level

            @pl.when(ka == half - 1)
            def _(level=level):
                for i in range(PIECES):
                    each_push(level, i, lambda copy: copy.wait_send())

            if 2 * half < nka <= 4 * half:
                side_sent(level)

    @pl.when(jnp.logical_not(leads))
    def _():
        for i in range(PIECES):
            swap(i, band).wait_recv()
        out[...] = taken[...]

    for copy in band_sends + [next_rank]:
        copy.wait_send()

    @pl.loop(0, CHUNKS)
    def _(c):
        right_copy(c).wait_send()

    for b in range(BLOCKS):
        tail_copy(b).wait_send()
        each_share(b, lambda copy: copy.wait_send())


def solution(mesh):
    nka, norb, nband = mesh.shape["ka"], mesh.shape["orb"], mesh.shape["band"]
    depth = levels_of(nka)

    def body(eigvecs, band_rank, occ_count, wrap_shift, orbital_site):
        rows, cols = eigvecs.shape[2], eigvecs.shape[3]
        bands = cols * nband
        share = bands // norb
        depth_of = rows // 4
        hbm = pl.BlockSpec(memory_space=pltpu.HBM)
        dma = pltpu.SemaphoreType.DMA
        result = pl.pallas_call(
            functools.partial(kernel, nka, norb, nband),
            out_shape=pltpu.VMEM((share, 2 * cols), F32),
            in_specs=[hbm] * 5,
            out_specs=pl.BlockSpec(memory_space=pltpu.VMEM),
            scratch_shapes=[
                pltpu.VMEM((2, nband, rows, cols), BF16),
                pltpu.VMEM((2, rows - depth_of, cols), BF16),
                pltpu.VMEM((2, cols, depth_of), BF16),
                pltpu.VMEM((2, cols, depth_of), BF16),
                pltpu.VMEM((rows - depth_of, cols), F32),
                pltpu.VMEM((rows - depth_of, cols), F32),
                pltpu.VMEM((rows // 128, 128), F32),
                pltpu.VMEM((rows // 128, 128), F32),
                pltpu.VMEM((rows // 128, 128), F32),
                pltpu.VMEM((rows // 128, 128), F32),
                pltpu.SMEM((1,), jnp.int32),
                pltpu.SMEM((1,), jnp.int32),
                pltpu.VMEM((rows // 128, 128), jnp.int32),
                pltpu.VMEM((nband, 1, cols), jnp.int32),
                pltpu.VMEM((1, cols), jnp.int32),
                pltpu.VMEM((2 * cols, bands), F32),
                pltpu.VMEM((cols, bands), F32),
                pltpu.VMEM((nband, norb, 2, cols, bands), BF16),
                pltpu.VMEM((bands, 2 * bands), F32),
                pltpu.VMEM((2 * bands, 2 * bands), BF16),
                pltpu.VMEM((share, 2 * bands), BF16),
                pltpu.VMEM((depth, share, 2 * bands), BF16),
                pltpu.VMEM((depth, bands, 2 * bands), BF16),
                pltpu.VMEM((nband, share, 2 * cols), F32),
                pltpu.VMEM((share, 2 * cols), F32),
                pltpu.SemaphoreType.REGULAR,
                dma,
                dma((4,)),
                dma((2, nband)),
                dma((2, nband)),
                dma((2,)),
                dma((2, CHUNKS)),
                dma((2, BLOCKS)),
                dma((2, BLOCKS, norb, nband)),
                dma((2, depth, (1 << (depth - 1)) + 1, PIECES)),
                dma((2, depth, (1 << (depth - 1)) + 1)),
                dma((2, PIECES, nband)),
            ],
            compiler_params=pltpu.CompilerParams(
                collective_id=0, has_side_effects=True,
                vmem_limit_bytes=60000000
            ),
            name="wilson",
        )(
            eigvecs.reshape(2, rows, cols), band_rank, occ_count, wrap_shift,
            orbital_site.reshape(rows // 128, 128),
        )
        return result.reshape(1, share, 2, cols)

    return jax.shard_map(
        body,
        mesh=mesh,
        in_specs=(
            P(("grp", "ka"), None, "orb", "band"),
            P(("grp", "ka"), "band"),
            P("grp"),
            P("grp"),
            P(("grp", "orb")),
        ),
        out_specs=P(("grp", "ka"), "orb", None, "band"),
        check_vma=False,
    )
```

```python
import functools
import math

import jax
import jax.numpy as jnp
from jax import lax
from jax.experimental import pallas as pl
from jax.experimental.pallas import tpu as pltpu
from jax.sharding import PartitionSpec as P

NS_STEPS = 8
SITES = 64
CHUNKS = 6
BLOCKS = 8
PIECES = 2
BEHIND = 2

ns_gain = 0.7
eps_mean = 1e-06

MESH = pl.DeviceIdType.MESH
BF16 = jnp.bfloat16
F32 = jnp.float32


def levels_of(count):
    return max(1, (count - 1).bit_length())


def remote(src, dst, send_sem, recv_sem, device):
    return pltpu.make_async_remote_copy(
        src_ref=src,
        dst_ref=dst,
        send_sem=send_sem,
        recv_sem=recv_sem,
        device_id=device,
        device_id_type=MESH,
    )


def across(left, right, contract):
    return lax.dot_general(left, right, (contract, ((), ())), preferred_element_type=F32)


def column_of(row, width):
    return jnp.transpose(jnp.broadcast_to(row, (width, row.shape[1])))


def polar_step(iterate):
    half = iterate.shape[1] // 2
    rounded = iterate.astype(BF16)
    real, imag = rounded[:, :half], rounded[:, half:]
    tall = jnp.concatenate(
        [rounded, jnp.concatenate([imag, -real], axis=1)], axis=0
    )
    gram = across(tall, rounded, ((1,), (1,))).astype(BF16)
    rows = iterate.shape[0]
    wide = jnp.concatenate([gram[:rows], gram[rows:]], axis=1)
    block = jnp.concatenate(
        [rounded, jnp.concatenate([-imag, real], axis=1)], axis=0
    )
    product = across(wide, block, ((1,), (0,)))
    return 1.5 * iterate - 0.5 * product


def kernel(
    nka, norb, nband,
    eig, rank, occ_at, shift_at, site_at,
    out,
    lefts, rights, stage, tail, cosine, sine, angle_cos, angle_sin, tail_cos, tail_sin,
    occ, shift, site, rank_band, rank_next, accs, mask, parts, sums, full, cur, pfx, got, sides, given, taken,
    ready,
    sem_own, sem_arg, sem_left, sem_rank, sem_next, sem_right, sem_tail, sem_acc, sem_part, sem_pre, sem_side, sem_swap,
):
    ka, orb, band = lax.axis_index("ka"), lax.axis_index("orb"), lax.axis_index("band")
    rows, cols = eig.shape[1], eig.shape[2]
    bands = nband * cols
    depth = stage.shape[2]
    body = rows - depth
    step = body // CHUNKS
    width = cols // BLOCKS
    before = lax.rem(ka + nka - 1, nka)
    lead = nband - 1
    leads = band == lead
    lanes = site.shape[1]

    barrier = pltpu.get_barrier_semaphore()
    for d in range(norb):
        for e in range(nband):
            if d + e > 0:
                to = {"orb": lax.rem(orb + d, norb), "band": lax.rem(band + e, nband)}
                pl.semaphore_signal(barrier, inc=1, device_id=to, device_id_type=MESH)
    for t in range(1, nka):
        @pl.when(ka + t < nka)
        def _(t=t):
            for e in range(nband):
                to = {"ka": lax.rem(ka + t, nka), "band": lax.rem(band + e, nband)}
                pl.semaphore_signal(barrier, inc=1, device_id=to, device_id_type=MESH)
    pl.semaphore_wait(barrier, norb * nband - 1 + ka * nband)
    for t in range(1, nka):
        @pl.when(ka >= t)
        def _(t=t):
            for e in range(nband):
                to = {"ka": lax.rem(ka + nka - t, nka), "band": lax.rem(band + e, nband)}
                pl.semaphore_signal(ready, inc=1, device_id=to, device_id_type=MESH)

    def chunk(c):
        return pl.ds(pl.multiple_of(c * step, step), step)

    def right_copy(c):
        return remote(
            eig.at[:, chunk(c)], rights.at[:, chunk(c)],
            sem_right.at[0, c], sem_right.at[1, c], {"ka": before},
        )

    def part_of(b):
        return pl.ds(b * width, width)

    def tail_copy(b, j):
        return remote(
            stage.at[:, part_of(b)], tail.at[j, :, part_of(b)],
            sem_tail.at[0, b, j], sem_tail.at[1, b, j], {"ka": before, "band": lead},
        )

    def next_rank(j):
        return remote(
            rank, rank_next.at[j], sem_next.at[0, j], sem_next.at[1, j],
            {"ka": before, "band": lead},
        )

    def start_right():
        next_rank(band).start()
        for c in range(CHUNKS):
            right_copy(c).start()

    @pl.when(ka > 0)
    def _():
        start_right()

    own = pltpu.make_async_copy(eig, lefts.at[:, band], sem_own)
    own.start()
    arguments = [
        pltpu.make_async_copy(src, dst, sem_arg.at[i])
        for i, (src, dst) in enumerate(
            ((occ_at, occ), (shift_at, shift), (site_at, site), (rank, rank_band.at[band]))
        )
    ]
    for copy in arguments:
        copy.start()
    band_sends = []
    for d in range(1, nband):
        to = {"band": lax.rem(band + d, nband)}
        copy = remote(eig, lefts.at[:, band], sem_left.at[0, d], sem_left.at[1, d], to)
        copy.start()
        band_sends.append(copy)
        copy = remote(rank, rank_band.at[band], sem_rank.at[0, d], sem_rank.at[1, d], to)
        copy.start()
        band_sends.append(copy)

    @pl.when(ka < nka - 1)
    def _():
        pl.semaphore_wait(ready, (nka - 1 - ka) * nband)

    @pl.when(ka == 0)
    def _():
        start_right()

    for copy in arguments:
        copy.wait()

    at_end, at_start = ka == nka - 1, ka == 0
    angle = ((shift[0] * site[...]) & (SITES - 1)).astype(F32) * (2.0 * math.pi / SITES)
    turned, lifted = jnp.cos(angle), jnp.sin(angle)
    angle_cos[...] = jnp.where(at_end, turned, 1.0)
    angle_sin[...] = jnp.where(at_end, lifted, 0.0)
    tail_cos[...] = jnp.where(at_start, turned, 1.0)
    tail_sin[...] = jnp.where(at_start, lifted, 0.0)

    own.wait()

    @pl.loop(0, depth // lanes)
    def _(i):
        from_rows = pl.ds(pl.multiple_of(body + i * lanes, lanes), lanes)
        to_lanes = pl.ds(pl.multiple_of(i * lanes, lanes), lanes)
        real = jnp.transpose(lefts[0, band, from_rows, :].astype(F32))
        imag = jnp.transpose(lefts[1, band, from_rows, :].astype(F32))
        turn = tail_cos[pl.ds(body // lanes + i, 1), :]
        lift = tail_sin[pl.ds(body // lanes + i, 1), :]
        stage[0, :, to_lanes] = (turn * real + lift * imag).astype(BF16)
        stage[1, :, to_lanes] = (turn * imag - lift * real).astype(BF16)

    @pl.loop(0, body // lanes)
    def _(i):
        place = pl.ds(pl.multiple_of(i * lanes, lanes), lanes)
        cosine[place, :] = column_of(angle_cos[pl.ds(i, 1), :], cols)
        sine[place, :] = column_of(angle_sin[pl.ds(i, 1), :], cols)

    for b in range(BLOCKS):
        tail_copy(b, band).start()

    for d in range(1, nband):
        came = lax.rem(band + nband - d, nband)
        to = {"band": lax.rem(band + d, nband)}
        remote(eig, lefts.at[:, came], sem_left.at[0, d], sem_left.at[1, d], to).wait_recv()
        remote(rank, rank_band.at[came], sem_rank.at[0, d], sem_rank.at[1, d], to).wait_recv()

    count = occ[0]

    @pl.when(leads)
    def _():
        row_mask = jnp.concatenate(
            [(rank_band[j] < count).astype(F32) for j in range(nband)], axis=1
        )
        for j in range(nband):
            next_rank(j).wait_recv()
            col_mask = column_of((rank_next[j] < count).astype(F32), cols)
            mask[j] = row_mask * jnp.concatenate([col_mask] * nband, axis=1)

    accs[band] = jnp.zeros(accs.shape[1:], F32)

    def lefts_of(p, place):
        return jnp.concatenate([lefts[p, j, place, :] for j in range(nband)], axis=1)

    @pl.loop(0, CHUNKS)
    def _(c):
        right_copy(c).wait_recv()
        place = chunk(c)
        real, imag = rights[0, place, :].astype(F32), rights[1, place, :].astype(F32)
        turn, lift = cosine[place, :], sine[place, :]
        new_real = (turn * real + lift * imag).astype(BF16)
        new_imag = (turn * imag - lift * real).astype(BF16)
        paired = jnp.concatenate(
            [
                jnp.concatenate([new_real, new_imag], axis=1),
                jnp.concatenate([new_imag, -new_real], axis=1),
            ],
            axis=0,
        )
        stacked = jnp.concatenate([lefts_of(p, place) for p in range(2)], axis=0)
        accs[band] += across(paired, stacked, ((0,), (0,)))

    def to_lead(j):
        return remote(
            accs.at[j], accs.at[j], sem_acc.at[0, j], sem_acc.at[1, j], {"band": lead}
        )

    def share(b, d):
        return remote(
            parts.at[:, 0, :, part_of(b)], parts.at[:, d, :, part_of(b)],
            sem_part.at[0, b, d], sem_part.at[1, b, d], {"orb": lax.rem(orb + d, norb)},
        )

    @pl.when(jnp.logical_not(leads))
    def _():
        to_lead(band).start()

    rest = pl.ds(body, depth)

    def absorb(b):
        for d in range(1, norb):
            share(b, d).wait_recv()
        for j in range(nband):
            for p in range(2):
                total = parts[j, 0, p, part_of(b), :].astype(F32)
                for d in range(1, norb):
                    total += parts[j, d, p, part_of(b), :].astype(F32)
                sums[p, pl.ds(j * cols + b * width, width), :] = total

    levels = levels_of(nka) if nka > 1 else 0
    height = bands // norb
    piece = height // PIECES
    scale = math.sqrt(bands)

    def rows_of(i):
        return pl.ds(i * piece, piece)

    def swap(i, j):
        return remote(
            given.at[j, rows_of(i)], taken.at[rows_of(i)],
            sem_swap.at[0, i, j], sem_swap.at[1, i, 0], {"band": j},
        )

    def push(level, t, i):
        here = pl.ds(pl.multiple_of(orb * height + i * piece, piece), piece)
        return remote(
            pfx.at[rows_of(i)] if level else cur.at[here], got.at[level, rows_of(i)],
            sem_pre.at[0, level, t, i], sem_pre.at[1, level, 0, i],
            {"ka": lax.rem(ka + t, nka)},
        )

    def each_push(level, i, act):
        for t in range(1, (1 << level) + 1):
            @pl.when(ka + t < nka)
            def _(t=t):
                act(push(level, t, i))

    def push_side(level, t):
        return remote(
            cur.at[pl.ds(0, bands)], sides.at[level],
            sem_side.at[0, level, t], sem_side.at[1, level, 0],
            {"ka": lax.rem(ka + t, nka)},
        )

    def side_sent(level):
        half = 1 << level
        sending = jnp.logical_and(ka >= 2 * half, lax.rem(ka, 2 * half) == half - 1)
        for t in range(1, half + 1):
            @pl.when(jnp.logical_and(sending, ka + t < nka))
            def _(t=t):
                push_side(level, t).wait_send()

    def set_cur(matrix):
        real, imag = matrix[:, :bands], matrix[:, bands:]
        cur[:bands, :bands] = real
        cur[:bands, bands:] = imag
        cur[bands:, :bands] = -imag
        cur[bands:, bands:] = real

    def hand_out(i, joined):
        for j in range(nband):
            for p in range(2):
                at = p * bands + j * cols
                given[j, rows_of(i), p * cols : (p + 1) * cols] = joined[:, at : at + cols] * scale
            if j != lead:
                swap(i, j).start()

    @pl.when(leads)
    def _():
        for j in range(lead):
            to_lead(j).wait_recv()
        whole = jnp.concatenate([lefts_of(p, rest) for p in range(2)], axis=0)
        for b in range(BLOCKS):
            quads = []
            for j in range(nband):
                tail_copy(b, j).wait_recv()
                real, imag = tail[j, 0, part_of(b), :], tail[j, 1, part_of(b), :]
                quads.append(jnp.concatenate([real, imag], axis=1))
                quads.append(jnp.concatenate([imag, -real], axis=1))
            term = across(jnp.concatenate(quads, axis=0), whole, ((1,), (0,)))
            for j in range(nband):
                for p in range(2):
                    at = (2 * j + p) * width
                    total = accs[j, pl.ds(p * cols + b * width, width), :] + term[at : at + width]
                    parts[j, 0, p, part_of(b), :] = (total * mask[j, part_of(b), :]).astype(BF16)
            for d in range(1, norb):
                share(b, d).start()
            if b >= BEHIND:
                absorb(b - BEHIND)
        for b in range(BLOCKS - BEHIND, BLOCKS):
            absorb(b)
        halves = [jnp.transpose(sums[p]) for p in range(2)]
        margins = jnp.concatenate(halves, axis=1)
        squares = jnp.sum(margins * margins, keepdims=True)
        iterate = margins * (ns_gain * lax.rsqrt(squares / count.astype(F32) + eps_mean))
        for _ in range(NS_STEPS):
            iterate = polar_step(iterate)
        rounded = iterate.astype(BF16)
        cur[:bands, :] = rounded

        @pl.when(ka == 0)
        def _():
            for i in range(PIECES):
                if levels:
                    each_push(0, i, lambda copy: copy.start())
            full[...] = iterate
            for i in range(PIECES):
                here = pl.ds(pl.multiple_of(orb * height + i * piece, piece), piece)
                hand_out(i, full[here, :])

        @pl.when(ka > 0)
        def _():
            cur[bands:, :bands] = -rounded[:, bands:]
            cur[bands:, bands:] = rounded[:, :bands]

        for level in range(levels):
            half = 1 << level
            later = ka >= 2 * half
            sending = jnp.logical_and(later, lax.rem(ka, 2 * half) == half - 1)
            taking = jnp.logical_and(later, lax.rem(ka // half, 2) == 1)
            if 2 * half < nka:
                if level:
                    side_sent(level - 1)
                for t in range(1, half + 1):
                    @pl.when(jnp.logical_and(sending, ka + t < nka))
                    def _(t=t):
                        push_side(level, t).start()

                @pl.when(taking)
                def _(level=level):
                    push_side(level, 1).wait_recv()
                    set_cur(across(sides[level], cur[...], ((1,), (0,))).astype(BF16))

            @pl.when(jnp.logical_and(ka >= half, ka < 2 * half))
            def _(level=level, half=half):
                for i in range(PIECES):
                    push(level, 1, i).wait_recv()
                    joined = across(got[level, rows_of(i), :], cur[...], ((1,), (0,)))
                    if level + 1 < levels:
                        pfx[rows_of(i), :] = joined.astype(BF16)

                        @pl.when(ka == 2 * half - 1)
                        def _(i=i):
                            each_push(level + 1, i, lambda copy: copy.start())
                    hand_out(i, joined)

        out[...] = given[lead]
        for i in range(PIECES):
            for j in range(lead):
                swap(i, j).wait_send()
        for level in range(levels):
            half = 1 << level

            @pl.when(ka == half - 1)
            def _(level=level):
                for i in range(PIECES):
                    each_push(level, i, lambda copy: copy.wait_send())

            if 2 * half < nka <= 4 * half:
                side_sent(level)

    @pl.when(jnp.logical_not(leads))
    def _():
        for i in range(PIECES):
            swap(i, band).wait_recv()
        out[...] = taken[...]

    for copy in band_sends + [next_rank(band)]:
        copy.wait_send()

    @pl.loop(0, CHUNKS)
    def _(c):
        right_copy(c).wait_send()

    for b in range(BLOCKS):
        tail_copy(b, band).wait_send()

    @pl.when(leads)
    def _():
        for b in range(BLOCKS):
            for d in range(1, norb):
                share(b, d).wait_send()

    @pl.when(jnp.logical_not(leads))
    def _():
        to_lead(band).wait_send()


def solution(mesh):
    nka, norb, nband = mesh.shape["ka"], mesh.shape["orb"], mesh.shape["band"]
    depth = levels_of(nka)

    def body(eigvecs, band_rank, occ_count, wrap_shift, orbital_site):
        rows, cols = eigvecs.shape[2], eigvecs.shape[3]
        bands = cols * nband
        share = bands // norb
        depth_of = rows // 4
        hbm = pl.BlockSpec(memory_space=pltpu.HBM)
        dma = pltpu.SemaphoreType.DMA
        result = pl.pallas_call(
            functools.partial(kernel, nka, norb, nband),
            out_shape=pltpu.VMEM((share, 2 * cols), F32),
            in_specs=[hbm] * 5,
            out_specs=pl.BlockSpec(memory_space=pltpu.VMEM),
            scratch_shapes=[
                pltpu.VMEM((2, nband, rows, cols), BF16),
                pltpu.VMEM((2, rows - depth_of, cols), BF16),
                pltpu.VMEM((2, cols, depth_of), BF16),
                pltpu.VMEM((nband, 2, cols, depth_of), BF16),
                pltpu.VMEM((rows - depth_of, cols), F32),
                pltpu.VMEM((rows - depth_of, cols), F32),
                pltpu.VMEM((rows // 128, 128), F32),
                pltpu.VMEM((rows // 128, 128), F32),
                pltpu.VMEM((rows // 128, 128), F32),
                pltpu.VMEM((rows // 128, 128), F32),
                pltpu.SMEM((1,), jnp.int32),
                pltpu.SMEM((1,), jnp.int32),
                pltpu.VMEM((rows // 128, 128), jnp.int32),
                pltpu.VMEM((nband, 1, cols), jnp.int32),
                pltpu.VMEM((nband, 1, cols), jnp.int32),
                pltpu.VMEM((nband, 2 * cols, bands), F32),
                pltpu.VMEM((nband, cols, bands), F32),
                pltpu.VMEM((nband, norb, 2, cols, bands), BF16),
                pltpu.VMEM((2, bands, bands), F32),
                pltpu.VMEM((bands, 2 * bands), F32),
                pltpu.VMEM((2 * bands, 2 * bands), BF16),
                pltpu.VMEM((share, 2 * bands), BF16),
                pltpu.VMEM((depth, share, 2 * bands), BF16),
                pltpu.VMEM((depth, bands, 2 * bands), BF16),
                pltpu.VMEM((nband, share, 2 * cols), F32),
                pltpu.VMEM((share, 2 * cols), F32),
                pltpu.SemaphoreType.REGULAR,
                dma,
                dma((4,)),
                dma((2, nband)),
                dma((2, nband)),
                dma((2, nband)),
                dma((2, CHUNKS)),
                dma((2, BLOCKS, nband)),
                dma((2, nband)),
                dma((2, BLOCKS, norb)),
                dma((2, depth, (1 << (depth - 1)) + 1, PIECES)),
                dma((2, depth, (1 << (depth - 1)) + 1)),
                dma((2, PIECES, nband)),
            ],
            compiler_params=pltpu.CompilerParams(
                collective_id=0, has_side_effects=True,
                vmem_limit_bytes=60000000
            ),
            name="wilson",
        )(
            eigvecs.reshape(2, rows, cols), band_rank, occ_count, wrap_shift,
            orbital_site.reshape(rows // 128, 128),
        )
        return result.reshape(1, share, 2, cols)

    return jax.shard_map(
        body,
        mesh=mesh,
        in_specs=(
            P(("grp", "ka"), None, "orb", "band"),
            P(("grp", "ka"), "band"),
            P("grp"),
            P("grp"),
            P(("grp", "orb")),
        ),
        out_specs=P(("grp", "ka"), "orb", None, "band"),
        check_vma=False,
    )
```

```python
import functools
import math

import jax
import jax.numpy as jnp
from jax import lax
from jax.experimental import pallas as pl
from jax.experimental.pallas import tpu as pltpu
from jax.sharding import PartitionSpec as P

NS_STEPS = 8
SITES = 64
CHUNKS = 6
BLOCKS = 8
PIECES = 2
BEHIND = 2

ns_gain = 0.7
eps_mean = 1e-06

MESH = pl.DeviceIdType.MESH
BF16 = jnp.bfloat16
F32 = jnp.float32


def levels_of(count):
    return max(1, (count - 1).bit_length())


def remote(src, dst, send_sem, recv_sem, device):
    return pltpu.make_async_remote_copy(
        src_ref=src,
        dst_ref=dst,
        send_sem=send_sem,
        recv_sem=recv_sem,
        device_id=device,
        device_id_type=MESH,
    )


def across(left, right, contract):
    return lax.dot_general(left, right, (contract, ((), ())), preferred_element_type=F32)


def column_of(row, width):
    return jnp.transpose(jnp.broadcast_to(row, (width, row.shape[1])))


def polar_step(iterate):
    rows, half = iterate.shape[0], iterate.shape[1] // 2
    rounded = iterate.astype(BF16)
    real, imag = rounded[:, :half], rounded[:, half:]
    turned = jnp.concatenate([imag, -real], axis=1)
    block = jnp.concatenate(
        [rounded, jnp.concatenate([-imag, real], axis=1)], axis=0
    )
    out = []
    part = rows // 2
    grams = []
    for i in range(2):
        here = slice(i * part, (i + 1) * part)
        tall = jnp.concatenate([rounded[here], turned[here]], axis=0)
        gram = across(tall, rounded, ((1,), (1,))).astype(BF16)
        grams.append(jnp.concatenate([gram[:part], gram[part:]], axis=1))
    for i in range(2):
        here = slice(i * part, (i + 1) * part)
        out.append(1.5 * iterate[here] - 0.5 * across(grams[i], block, ((1,), (0,))))
    return jnp.concatenate(out, axis=0)


def kernel(
    nka, norb, nband,
    eig, rank, occ_at, shift_at, site_at,
    out,
    lefts, rights, stage, tail, cosine, sine, angle_cos, angle_sin, tail_cos, tail_sin,
    occ, shift, site, rank_band, rank_next, accs, mask, parts, sums, full, cur, pfx, got, sides, given, taken,
    ready, known,
    sem_own, sem_arg, sem_left, sem_rank, sem_next, sem_right, sem_tail, sem_acc, sem_part, sem_pre, sem_side, sem_swap,
):
    ka, orb, band = lax.axis_index("ka"), lax.axis_index("orb"), lax.axis_index("band")
    rows, cols = eig.shape[1], eig.shape[2]
    bands = nband * cols
    depth = stage.shape[2]
    body = rows - depth
    step = body // CHUNKS
    width = cols // BLOCKS
    before = lax.rem(ka + nka - 1, nka)
    lead = nband - 1
    leads = band == lead
    lanes = site.shape[1]

    barrier = pltpu.get_barrier_semaphore()
    chip = [(0, e) for e in range(nband)]
    point = [(d, e) for d in range(norb) for e in range(nband)]

    def greet(semaphore, t, cores):
        for d, e in cores:
            to = {
                "ka": lax.rem(ka + nka + t, nka),
                "orb": lax.rem(orb + d, norb),
                "band": lax.rem(band + e, nband),
            }
            pl.semaphore_signal(semaphore, inc=1, device_id=to, device_id_type=MESH)

    for t in range(1, nka):
        @pl.when(ka + t < nka)
        def _(t=t):
            greet(barrier, t, point if t in (1, nka - 1) else chip)

    far = len(point) - nband if nka > 2 else 0

    @pl.when(jnp.logical_and(ka > 0, ka < nka - 1))
    def _():
        pl.semaphore_wait(barrier, len(point) + (ka - 1) * nband)

    @pl.when(ka == nka - 1)
    def _():
        pl.semaphore_wait(barrier, len(point) + (nka - 2) * nband + far)

    for t in range(nka - 1, 0, -1):
        @pl.when(ka >= t)
        def _(t=t):
            greet(ready, -t, point if t in (1, nka - 1) else chip)

    def chunk(c):
        return pl.ds(pl.multiple_of(c * step, step), step)

    def right_copy(c):
        return remote(
            eig.at[:, chunk(c)], rights.at[:, chunk(c)],
            sem_right.at[0, c], sem_right.at[1, c], {"ka": before},
        )

    def part_of(b):
        return pl.ds(b * width, width)

    def tail_copy(b, j):
        return remote(
            stage.at[:, part_of(b)], tail.at[j, :, part_of(b)],
            sem_tail.at[0, b, j], sem_tail.at[1, b, j], {"ka": before, "band": lead},
        )

    def next_rank(j):
        return remote(
            rank, rank_next.at[j], sem_next.at[0, j], sem_next.at[1, j],
            {"ka": before, "band": lead},
        )

    def start_right():
        next_rank(band).start()
        for c in range(CHUNKS):
            right_copy(c).start()

    @pl.when(ka > 0)
    def _():
        start_right()

    own = pltpu.make_async_copy(eig, lefts.at[:, band], sem_own)
    own.start()
    arguments = [
        pltpu.make_async_copy(src, dst, sem_arg.at[i])
        for i, (src, dst) in enumerate(
            ((occ_at, occ), (shift_at, shift), (site_at, site), (rank, rank_band.at[band]))
        )
    ]
    for copy in arguments:
        copy.start()

    @pl.when(ka == 0)
    def _():
        pl.semaphore_wait(ready, len(point) + (nka - 2) * nband + far)
        start_right()
        greet(known, -1, [(0, 0)])

    @pl.when(jnp.logical_and(ka > 0, ka < nka - 1))
    def _():
        pl.semaphore_wait(ready, len(point) + (nka - 2 - ka) * nband)

    @pl.when(ka == nka - 1)
    def _():
        pl.semaphore_wait(known, 1)

    band_sends = []
    for d in range(1, nband):
        to = {"band": lax.rem(band + d, nband)}
        copy = remote(eig, lefts.at[:, band], sem_left.at[0, d], sem_left.at[1, d], to)
        copy.start()
        band_sends.append(copy)
        copy = remote(rank, rank_band.at[band], sem_rank.at[0, d], sem_rank.at[1, d], to)
        copy.start()
        band_sends.append(copy)

    for copy in arguments:
        copy.wait()

    at_end, at_start = ka == nka - 1, ka == 0
    angle = ((shift[0] * site[...]) & (SITES - 1)).astype(F32) * (2.0 * math.pi / SITES)
    turned, lifted = jnp.cos(angle), jnp.sin(angle)
    angle_cos[...] = jnp.where(at_end, turned, 1.0)
    angle_sin[...] = jnp.where(at_end, lifted, 0.0)
    tail_cos[...] = jnp.where(at_start, turned, 1.0)
    tail_sin[...] = jnp.where(at_start, lifted, 0.0)

    own.wait()

    @pl.loop(0, depth // lanes)
    def _(i):
        from_rows = pl.ds(pl.multiple_of(body + i * lanes, lanes), lanes)
        to_lanes = pl.ds(pl.multiple_of(i * lanes, lanes), lanes)
        real = jnp.transpose(lefts[0, band, from_rows, :].astype(F32))
        imag = jnp.transpose(lefts[1, band, from_rows, :].astype(F32))
        turn = tail_cos[pl.ds(body // lanes + i, 1), :]
        lift = tail_sin[pl.ds(body // lanes + i, 1), :]
        stage[0, :, to_lanes] = (turn * real + lift * imag).astype(BF16)
        stage[1, :, to_lanes] = (turn * imag - lift * real).astype(BF16)

    @pl.loop(0, body // lanes)
    def _(i):
        place = pl.ds(pl.multiple_of(i * lanes, lanes), lanes)
        cosine[place, :] = column_of(angle_cos[pl.ds(i, 1), :], cols)
        sine[place, :] = column_of(angle_sin[pl.ds(i, 1), :], cols)

    for b in range(BLOCKS):
        tail_copy(b, band).start()

    for d in range(1, nband):
        came = lax.rem(band + nband - d, nband)
        to = {"band": lax.rem(band + d, nband)}
        remote(eig, lefts.at[:, came], sem_left.at[0, d], sem_left.at[1, d], to).wait_recv()
        remote(rank, rank_band.at[came], sem_rank.at[0, d], sem_rank.at[1, d], to).wait_recv()

    count = occ[0]

    @pl.when(leads)
    def _():
        row_mask = jnp.concatenate(
            [(rank_band[j] < count).astype(F32) for j in range(nband)], axis=1
        )
        for j in range(nband):
            next_rank(j).wait_recv()
            col_mask = column_of((rank_next[j] < count).astype(F32), cols)
            mask[j] = row_mask * jnp.concatenate([col_mask] * nband, axis=1)

    accs[band] = jnp.zeros(accs.shape[1:], F32)

    def lefts_of(p, place):
        return jnp.concatenate([lefts[p, j, place, :] for j in range(nband)], axis=1)

    @pl.loop(0, CHUNKS)
    def _(c):
        right_copy(c).wait_recv()
        place = chunk(c)
        real, imag = rights[0, place, :].astype(F32), rights[1, place, :].astype(F32)
        turn, lift = cosine[place, :], sine[place, :]
        new_real = (turn * real + lift * imag).astype(BF16)
        new_imag = (turn * imag - lift * real).astype(BF16)
        paired = jnp.concatenate(
            [
                jnp.concatenate([new_real, new_imag], axis=1),
                jnp.concatenate([new_imag, -new_real], axis=1),
            ],
            axis=0,
        )
        stacked = jnp.concatenate([lefts_of(p, place) for p in range(2)], axis=0)
        accs[band] += across(paired, stacked, ((0,), (0,)))

    def to_lead(j):
        return remote(
            accs.at[j], accs.at[j], sem_acc.at[0, j], sem_acc.at[1, j], {"band": lead}
        )

    def share(b, d):
        return remote(
            parts.at[:, 0, :, part_of(b)], parts.at[:, d, :, part_of(b)],
            sem_part.at[0, b, d], sem_part.at[1, b, d], {"orb": lax.rem(orb + d, norb)},
        )

    @pl.when(jnp.logical_not(leads))
    def _():
        to_lead(band).start()

    rest = pl.ds(body, depth)

    def absorb(b):
        for d in range(1, norb):
            share(b, d).wait_recv()
        for j in range(nband):
            for p in range(2):
                total = parts[j, 0, p, part_of(b), :].astype(F32)
                for d in range(1, norb):
                    total += parts[j, d, p, part_of(b), :].astype(F32)
                sums[p, pl.ds(j * cols + b * width, width), :] = total

    levels = levels_of(nka) if nka > 1 else 0
    height = bands // norb
    piece = height // PIECES
    scale = math.sqrt(bands)

    def rows_of(i):
        return pl.ds(i * piece, piece)

    def swap(i, j):
        return remote(
            given.at[j, rows_of(i)], taken.at[rows_of(i)],
            sem_swap.at[0, i, j], sem_swap.at[1, i, 0], {"band": j},
        )

    def push(level, t, i):
        here = pl.ds(pl.multiple_of(orb * height + i * piece, piece), piece)
        return remote(
            pfx.at[rows_of(i)] if level else cur.at[here], got.at[level, rows_of(i)],
            sem_pre.at[0, level, t, i], sem_pre.at[1, level, 0, i],
            {"ka": lax.rem(ka + t, nka)},
        )

    def each_push(level, i, act):
        for t in range(1, (1 << level) + 1):
            @pl.when(ka + t < nka)
            def _(t=t):
                act(push(level, t, i))

    def push_side(level, t):
        return remote(
            cur.at[pl.ds(0, bands)], sides.at[level],
            sem_side.at[0, level, t], sem_side.at[1, level, 0],
            {"ka": lax.rem(ka + t, nka)},
        )

    def side_sent(level):
        half = 1 << level
        sending = jnp.logical_and(ka >= 2 * half, lax.rem(ka, 2 * half) == half - 1)
        for t in range(1, half + 1):
            @pl.when(jnp.logical_and(sending, ka + t < nka))
            def _(t=t):
                push_side(level, t).wait_send()

    def set_cur(matrix):
        real, imag = matrix[:, :bands], matrix[:, bands:]
        cur[:bands, :bands] = real
        cur[:bands, bands:] = imag
        cur[bands:, :bands] = -imag
        cur[bands:, bands:] = real

    def hand_out(i, joined):
        for j in range(nband):
            for p in range(2):
                at = p * bands + j * cols
                given[j, rows_of(i), p * cols : (p + 1) * cols] = joined[:, at : at + cols] * scale
            if j != lead:
                swap(i, j).start()

    @pl.when(leads)
    def _():
        for j in range(lead):
            to_lead(j).wait_recv()
        whole = jnp.concatenate([lefts_of(p, rest) for p in range(2)], axis=0)
        for b in range(BLOCKS):
            quads = []
            for j in range(nband):
                tail_copy(b, j).wait_recv()
                real, imag = tail[j, 0, part_of(b), :], tail[j, 1, part_of(b), :]
                quads.append(jnp.concatenate([real, imag], axis=1))
                quads.append(jnp.concatenate([imag, -real], axis=1))
            term = across(jnp.concatenate(quads, axis=0), whole, ((1,), (0,)))
            for j in range(nband):
                for p in range(2):
                    at = (2 * j + p) * width
                    total = accs[j, pl.ds(p * cols + b * width, width), :] + term[at : at + width]
                    parts[j, 0, p, part_of(b), :] = (total * mask[j, part_of(b), :]).astype(BF16)
            for d in range(1, norb):
                share(b, d).start()
            if b >= BEHIND:
                absorb(b - BEHIND)
        for b in range(BLOCKS - BEHIND, BLOCKS):
            absorb(b)
        halves = [jnp.transpose(sums[p]) for p in range(2)]
        margins = jnp.concatenate(halves, axis=1)
        squares = jnp.sum(margins * margins, keepdims=True)
        iterate = margins * (ns_gain * lax.rsqrt(squares / count.astype(F32) + eps_mean))
        for _ in range(NS_STEPS):
            iterate = polar_step(iterate)
        rounded = iterate.astype(BF16)
        cur[:bands, :] = rounded

        @pl.when(ka == 0)
        def _():
            for i in range(PIECES):
                if levels:
                    each_push(0, i, lambda copy: copy.start())
            full[...] = iterate
            for i in range(PIECES):
                here = pl.ds(pl.multiple_of(orb * height + i * piece, piece), piece)
                hand_out(i, full[here, :])

        @pl.when(ka > 0)
        def _():
            cur[bands:, :bands] = -rounded[:, bands:]
            cur[bands:, bands:] = rounded[:, :bands]

        for level in range(levels):
            half = 1 << level
            later = ka >= 2 * half
            sending = jnp.logical_and(later, lax.rem(ka, 2 * half) == half - 1)
            taking = jnp.logical_and(later, lax.rem(ka // half, 2) == 1)
            if 2 * half < nka:
                if level:
                    side_sent(level - 1)
                for t in range(1, half + 1):
                    @pl.when(jnp.logical_and(sending, ka + t < nka))
                    def _(t=t):
                        push_side(level, t).start()

                @pl.when(taking)
                def _(level=level):
                    push_side(level, 1).wait_recv()
                    set_cur(across(sides[level], cur[...], ((1,), (0,))).astype(BF16))

            @pl.when(jnp.logical_and(ka >= half, ka < 2 * half))
            def _(level=level, half=half):
                for i in range(PIECES):
                    push(level, 1, i).wait_recv()
                    joined = across(got[level, rows_of(i), :], cur[...], ((1,), (0,)))
                    if level + 1 < levels:
                        pfx[rows_of(i), :] = joined.astype(BF16)

                        @pl.when(ka == 2 * half - 1)
                        def _(i=i):
                            each_push(level + 1, i, lambda copy: copy.start())
                    hand_out(i, joined)

        out[...] = given[lead]
        for i in range(PIECES):
            for j in range(lead):
                swap(i, j).wait_send()
        for level in range(levels):
            half = 1 << level

            @pl.when(ka == half - 1)
            def _(level=level):
                for i in range(PIECES):
                    each_push(level, i, lambda copy: copy.wait_send())

            if 2 * half < nka <= 4 * half:
                side_sent(level)

    @pl.when(jnp.logical_not(leads))
    def _():
        for i in range(PIECES):
            swap(i, band).wait_recv()
        out[...] = taken[...]

    for copy in band_sends + [next_rank(band)]:
        copy.wait_send()

    @pl.loop(0, CHUNKS)
    def _(c):
        right_copy(c).wait_send()

    for b in range(BLOCKS):
        tail_copy(b, band).wait_send()

    @pl.when(leads)
    def _():
        for b in range(BLOCKS):
            for d in range(1, norb):
                share(b, d).wait_send()

    @pl.when(jnp.logical_not(leads))
    def _():
        to_lead(band).wait_send()


def solution(mesh):
    nka, norb, nband = mesh.shape["ka"], mesh.shape["orb"], mesh.shape["band"]
    depth = levels_of(nka)

    def body(eigvecs, band_rank, occ_count, wrap_shift, orbital_site):
        rows, cols = eigvecs.shape[2], eigvecs.shape[3]
        bands = cols * nband
        share = bands // norb
        depth_of = rows // 4
        hbm = pl.BlockSpec(memory_space=pltpu.HBM)
        dma = pltpu.SemaphoreType.DMA
        result = pl.pallas_call(
            functools.partial(kernel, nka, norb, nband),
            out_shape=pltpu.VMEM((share, 2 * cols), F32),
            in_specs=[hbm] * 5,
            out_specs=pl.BlockSpec(memory_space=pltpu.VMEM),
            scratch_shapes=[
                pltpu.VMEM((2, nband, rows, cols), BF16),
                pltpu.VMEM((2, rows - depth_of, cols), BF16),
                pltpu.VMEM((2, cols, depth_of), BF16),
                pltpu.VMEM((nband, 2, cols, depth_of), BF16),
                pltpu.VMEM((rows - depth_of, cols), F32),
                pltpu.VMEM((rows - depth_of, cols), F32),
                pltpu.VMEM((rows // 128, 128), F32),
                pltpu.VMEM((rows // 128, 128), F32),
                pltpu.VMEM((rows // 128, 128), F32),
                pltpu.VMEM((rows // 128, 128), F32),
                pltpu.SMEM((1,), jnp.int32),
                pltpu.SMEM((1,), jnp.int32),
                pltpu.VMEM((rows // 128, 128), jnp.int32),
                pltpu.VMEM((nband, 1, cols), jnp.int32),
                pltpu.VMEM((nband, 1, cols), jnp.int32),
                pltpu.VMEM((nband, 2 * cols, bands), F32),
                pltpu.VMEM((nband, cols, bands), F32),
                pltpu.VMEM((nband, norb, 2, cols, bands), BF16),
                pltpu.VMEM((2, bands, bands), F32),
                pltpu.VMEM((bands, 2 * bands), F32),
                pltpu.VMEM((2 * bands, 2 * bands), BF16),
                pltpu.VMEM((share, 2 * bands), BF16),
                pltpu.VMEM((depth, share, 2 * bands), BF16),
                pltpu.VMEM((depth, bands, 2 * bands), BF16),
                pltpu.VMEM((nband, share, 2 * cols), F32),
                pltpu.VMEM((share, 2 * cols), F32),
                pltpu.SemaphoreType.REGULAR,
                pltpu.SemaphoreType.REGULAR,
                dma,
                dma((4,)),
                dma((2, nband)),
                dma((2, nband)),
                dma((2, nband)),
                dma((2, CHUNKS)),
                dma((2, BLOCKS, nband)),
                dma((2, nband)),
                dma((2, BLOCKS, norb)),
                dma((2, depth, (1 << (depth - 1)) + 1, PIECES)),
                dma((2, depth, (1 << (depth - 1)) + 1)),
                dma((2, PIECES, nband)),
            ],
            compiler_params=pltpu.CompilerParams(
                collective_id=0, has_side_effects=True,
                vmem_limit_bytes=60000000
            ),
            name="wilson",
        )(
            eigvecs.reshape(2, rows, cols), band_rank, occ_count, wrap_shift,
            orbital_site.reshape(rows // 128, 128),
        )
        return result.reshape(1, share, 2, cols)

    return jax.shard_map(
        body,
        mesh=mesh,
        in_specs=(
            P(("grp", "ka"), None, "orb", "band"),
            P(("grp", "ka"), "band"),
            P("grp"),
            P("grp"),
            P(("grp", "orb")),
        ),
        out_specs=P(("grp", "ka"), "orb", None, "band"),
        check_vma=False,
    )
```

```python
import functools
import math

import jax
import jax.numpy as jnp
from jax import lax
from jax.experimental import pallas as pl
from jax.experimental.pallas import tpu as pltpu
from jax.sharding import PartitionSpec as P

NS_STEPS = 8
SITES = 64
CHUNKS = 7
BLOCKS = 8
PIECES = 2
BEHIND = 6

ns_gain = 0.7
eps_mean = 1e-06

MESH = pl.DeviceIdType.MESH
BF16 = jnp.bfloat16
F32 = jnp.float32


def levels_of(count):
    return max(1, (count - 1).bit_length())


def remote(src, dst, send_sem, recv_sem, device):
    return pltpu.make_async_remote_copy(
        src_ref=src,
        dst_ref=dst,
        send_sem=send_sem,
        recv_sem=recv_sem,
        device_id=device,
        device_id_type=MESH,
    )


def across(left, right, contract):
    return lax.dot_general(left, right, (contract, ((), ())), preferred_element_type=F32)


def column_of(row, width):
    return jnp.transpose(jnp.broadcast_to(row, (width, row.shape[1])))


def polar_step(iterate):
    half = iterate.shape[1] // 2
    rounded = iterate.astype(BF16)
    real, imag = rounded[:, :half], rounded[:, half:]
    turned = jnp.concatenate([imag, -real], axis=1)
    block = jnp.concatenate(
        [rounded, jnp.concatenate([-imag, real], axis=1)], axis=0
    )
    gram_real = across(rounded, rounded, ((1,), (1,))).astype(BF16)
    gram_imag = across(turned, rounded, ((1,), (1,))).astype(BF16)
    wide = jnp.concatenate([gram_real, gram_imag], axis=1)
    return 1.5 * iterate - 0.5 * across(wide, block, ((1,), (0,)))


def kernel(
    nka, norb, nband,
    eig, rank, occ_at, shift_at, site_at,
    out,
    lefts, rights, stage, tail, cosine, sine, angle_cos, angle_sin, tail_cos, tail_sin,
    occ, shift, site, rank_band, rank_next, accs, mask, parts, sums, full, cur, pfx, got, sides, given, taken,
    ready, known,
    sem_own, sem_arg, sem_left, sem_rank, sem_next, sem_right, sem_tail, sem_acc, sem_part, sem_pre, sem_side, sem_swap,
):
    ka, orb, band = lax.axis_index("ka"), lax.axis_index("orb"), lax.axis_index("band")
    rows, cols = eig.shape[1], eig.shape[2]
    bands = nband * cols
    depth = stage.shape[2]
    body = rows - depth
    step = body // CHUNKS
    width = cols // BLOCKS
    before = lax.rem(ka + nka - 1, nka)
    lead = nband - 1
    leads = band == lead
    lanes = site.shape[1]

    barrier = pltpu.get_barrier_semaphore()
    chip = [(0, e) for e in range(nband)]
    point = [(d, e) for d in range(norb) for e in range(nband)]

    def greet(semaphore, t, cores):
        for d, e in cores:
            to = {
                "ka": lax.rem(ka + nka + t, nka),
                "orb": lax.rem(orb + d, norb),
                "band": lax.rem(band + e, nband),
            }
            pl.semaphore_signal(semaphore, inc=1, device_id=to, device_id_type=MESH)

    for t in range(1, nka):
        @pl.when(ka + t < nka)
        def _(t=t):
            greet(barrier, t, point if t in (1, nka - 1) else chip)

    far = len(point) - nband if nka > 2 else 0

    @pl.when(jnp.logical_and(ka > 0, ka < nka - 1))
    def _():
        pl.semaphore_wait(barrier, len(point) + (ka - 1) * nband)

    @pl.when(ka == nka - 1)
    def _():
        pl.semaphore_wait(barrier, len(point) + (nka - 2) * nband + far)

    for t in range(nka - 1, 0, -1):
        @pl.when(ka >= t)
        def _(t=t):
            greet(ready, -t, point if t in (1, nka - 1) else chip)

    def chunk(c):
        return pl.ds(pl.multiple_of(c * step, step), step)

    def right_copy(c):
        return remote(
            eig.at[:, chunk(c)], rights.at[:, chunk(c)],
            sem_right.at[0, c], sem_right.at[1, c], {"ka": before},
        )

    def part_of(b):
        return pl.ds(b * width, width)

    def tail_copy(b, j):
        return remote(
            stage.at[:, part_of(b)], tail.at[j, :, part_of(b)],
            sem_tail.at[0, b, j], sem_tail.at[1, b, j], {"ka": before, "band": lead},
        )

    def next_rank(j):
        return remote(
            rank, rank_next.at[j], sem_next.at[0, j], sem_next.at[1, j],
            {"ka": before, "band": lead},
        )

    def start_right():
        next_rank(band).start()
        for c in range(CHUNKS):
            right_copy(c).start()

    @pl.when(ka > 0)
    def _():
        start_right()

    own = pltpu.make_async_copy(eig, lefts.at[:, band], sem_own)
    own.start()
    arguments = [
        pltpu.make_async_copy(src, dst, sem_arg.at[i])
        for i, (src, dst) in enumerate(
            ((occ_at, occ), (shift_at, shift), (site_at, site), (rank, rank_band.at[band]))
        )
    ]
    for copy in arguments:
        copy.start()

    @pl.when(ka == 0)
    def _():
        pl.semaphore_wait(ready, len(point) + (nka - 2) * nband + far)
        start_right()
        greet(known, -1, [(0, 0)])

    @pl.when(jnp.logical_and(ka > 0, ka < nka - 1))
    def _():
        pl.semaphore_wait(ready, len(point) + (nka - 2 - ka) * nband)

    @pl.when(ka == nka - 1)
    def _():
        pl.semaphore_wait(known, 1)

    band_sends = []
    for d in range(1, nband):
        to = {"band": lax.rem(band + d, nband)}
        copy = remote(eig, lefts.at[:, band], sem_left.at[0, d], sem_left.at[1, d], to)
        copy.start()
        band_sends.append(copy)
        copy = remote(rank, rank_band.at[band], sem_rank.at[0, d], sem_rank.at[1, d], to)
        copy.start()
        band_sends.append(copy)

    for copy in arguments:
        copy.wait()

    at_end, at_start = ka == nka - 1, ka == 0
    angle = ((shift[0] * site[...]) & (SITES - 1)).astype(F32) * (2.0 * math.pi / SITES)
    turned, lifted = jnp.cos(angle), jnp.sin(angle)
    angle_cos[...] = jnp.where(at_end, turned, 1.0)
    angle_sin[...] = jnp.where(at_end, lifted, 0.0)
    tail_cos[...] = jnp.where(at_start, turned, 1.0)
    tail_sin[...] = jnp.where(at_start, lifted, 0.0)

    own.wait()

    @pl.loop(0, depth // lanes)
    def _(i):
        from_rows = pl.ds(pl.multiple_of(body + i * lanes, lanes), lanes)
        to_lanes = pl.ds(pl.multiple_of(i * lanes, lanes), lanes)
        real = jnp.transpose(lefts[0, band, from_rows, :].astype(F32))
        imag = jnp.transpose(lefts[1, band, from_rows, :].astype(F32))
        turn = tail_cos[pl.ds(body // lanes + i, 1), :]
        lift = tail_sin[pl.ds(body // lanes + i, 1), :]
        stage[0, :, to_lanes] = (turn * real + lift * imag).astype(BF16)
        stage[1, :, to_lanes] = (turn * imag - lift * real).astype(BF16)

    @pl.loop(0, body // lanes)
    def _(i):
        place = pl.ds(pl.multiple_of(i * lanes, lanes), lanes)
        cosine[place, :] = column_of(angle_cos[pl.ds(i, 1), :], cols)
        sine[place, :] = column_of(angle_sin[pl.ds(i, 1), :], cols)

    for b in range(BLOCKS):
        tail_copy(b, band).start()

    for d in range(1, nband):
        came = lax.rem(band + nband - d, nband)
        to = {"band": lax.rem(band + d, nband)}
        remote(eig, lefts.at[:, came], sem_left.at[0, d], sem_left.at[1, d], to).wait_recv()
        remote(rank, rank_band.at[came], sem_rank.at[0, d], sem_rank.at[1, d], to).wait_recv()

    count = occ[0]

    @pl.when(leads)
    def _():
        row_mask = jnp.concatenate(
            [(rank_band[j] < count).astype(F32) for j in range(nband)], axis=1
        )
        for j in range(nband):
            next_rank(j).wait_recv()
            col_mask = column_of((rank_next[j] < count).astype(F32), cols)
            mask[j] = row_mask * jnp.concatenate([col_mask] * nband, axis=1)

    accs[band] = jnp.zeros(accs.shape[1:], F32)

    def lefts_of(p, place):
        return jnp.concatenate([lefts[p, j, place, :] for j in range(nband)], axis=1)

    @pl.loop(0, CHUNKS)
    def _(c):
        right_copy(c).wait_recv()
        place = chunk(c)
        real, imag = rights[0, place, :].astype(F32), rights[1, place, :].astype(F32)
        turn, lift = cosine[place, :], sine[place, :]
        new_real = (turn * real + lift * imag).astype(BF16)
        new_imag = (turn * imag - lift * real).astype(BF16)
        paired = jnp.concatenate(
            [
                jnp.concatenate([new_real, new_imag], axis=1),
                jnp.concatenate([new_imag, -new_real], axis=1),
            ],
            axis=0,
        )
        stacked = jnp.concatenate([lefts_of(p, place) for p in range(2)], axis=0)
        accs[band] += across(paired, stacked, ((0,), (0,)))

    def to_lead(j):
        return remote(
            accs.at[j], accs.at[j], sem_acc.at[0, j], sem_acc.at[1, j], {"band": lead}
        )

    def share(b, d):
        return remote(
            parts.at[:, 0, :, part_of(b)], parts.at[:, d, :, part_of(b)],
            sem_part.at[0, b, d], sem_part.at[1, b, d], {"orb": lax.rem(orb + d, norb)},
        )

    @pl.when(jnp.logical_not(leads))
    def _():
        to_lead(band).start()

    rest = pl.ds(body, depth)

    def absorb(b):
        for d in range(1, norb):
            share(b, d).wait_recv()
        for j in range(nband):
            for p in range(2):
                total = parts[j, 0, p, part_of(b), :].astype(F32)
                for d in range(1, norb):
                    total += parts[j, d, p, part_of(b), :].astype(F32)
                sums[p, pl.ds(j * cols + b * width, width), :] = total

    levels = levels_of(nka) if nka > 1 else 0
    height = bands // norb
    piece = height // PIECES
    scale = math.sqrt(bands)

    def rows_of(i):
        return pl.ds(i * piece, piece)

    def swap(i, j):
        return remote(
            given.at[j, rows_of(i)], taken.at[rows_of(i)],
            sem_swap.at[0, i, j], sem_swap.at[1, i, 0], {"band": j},
        )

    def push(level, t, i):
        here = pl.ds(pl.multiple_of(orb * height + i * piece, piece), piece)
        return remote(
            pfx.at[rows_of(i)] if level else cur.at[here], got.at[level, rows_of(i)],
            sem_pre.at[0, level, t, i], sem_pre.at[1, level, 0, i],
            {"ka": lax.rem(ka + t, nka)},
        )

    def each_push(level, i, act):
        for t in range(1, (1 << level) + 1):
            @pl.when(ka + t < nka)
            def _(t=t):
                act(push(level, t, i))

    def push_side(level, t):
        return remote(
            cur.at[pl.ds(0, bands)], sides.at[level],
            sem_side.at[0, level, t], sem_side.at[1, level, 0],
            {"ka": lax.rem(ka + t, nka)},
        )

    def side_sent(level):
        half = 1 << level
        sending = jnp.logical_and(ka >= 2 * half, lax.rem(ka, 2 * half) == half - 1)
        for t in range(1, half + 1):
            @pl.when(jnp.logical_and(sending, ka + t < nka))
            def _(t=t):
                push_side(level, t).wait_send()

    def set_cur(matrix):
        real, imag = matrix[:, :bands], matrix[:, bands:]
        cur[:bands, :bands] = real
        cur[:bands, bands:] = imag
        cur[bands:, :bands] = -imag
        cur[bands:, bands:] = real

    def hand_out(i, joined):
        for j in range(nband):
            for p in range(2):
                at = p * bands + j * cols
                given[j, rows_of(i), p * cols : (p + 1) * cols] = joined[:, at : at + cols] * scale
            if j != lead:
                swap(i, j).start()

    @pl.when(leads)
    def _():
        for j in range(lead):
            to_lead(j).wait_recv()
        whole = jnp.concatenate([lefts_of(p, rest) for p in range(2)], axis=0)
        for b in range(BLOCKS):
            quads = []
            for j in range(nband):
                tail_copy(b, j).wait_recv()
                real, imag = tail[j, 0, part_of(b), :], tail[j, 1, part_of(b), :]
                quads.append(jnp.concatenate([real, imag], axis=1))
                quads.append(jnp.concatenate([imag, -real], axis=1))
            term = across(jnp.concatenate(quads, axis=0), whole, ((1,), (0,)))
            for j in range(nband):
                for p in range(2):
                    at = (2 * j + p) * width
                    total = accs[j, pl.ds(p * cols + b * width, width), :] + term[at : at + width]
                    parts[j, 0, p, part_of(b), :] = (total * mask[j, part_of(b), :]).astype(BF16)
            for d in range(1, norb):
                share(b, d).start()
            if b >= BEHIND:
                absorb(b - BEHIND)
        for b in range(BLOCKS - BEHIND, BLOCKS):
            absorb(b)
        halves = [jnp.transpose(sums[p]) for p in range(2)]
        margins = jnp.concatenate(halves, axis=1)
        squares = jnp.sum(margins * margins, keepdims=True)
        iterate = margins * (ns_gain * lax.rsqrt(squares / count.astype(F32) + eps_mean))
        for _ in range(NS_STEPS):
            iterate = polar_step(iterate)
        rounded = iterate.astype(BF16)
        cur[:bands, :] = rounded

        @pl.when(ka == 0)
        def _():
            for i in range(PIECES):
                if levels:
                    each_push(0, i, lambda copy: copy.start())
            full[...] = iterate
            for i in range(PIECES):
                here = pl.ds(pl.multiple_of(orb * height + i * piece, piece), piece)
                hand_out(i, full[here, :])

        if nka > 2:
            @pl.when(jnp.logical_and(ka >= 2, lax.rem(ka, 2) == 0))
            def _():
                @pl.when(ka + 1 < nka)
                def _():
                    push_side(0, 1).start()

        @pl.when(ka > 0)
        def _():
            cur[bands:, :bands] = -rounded[:, bands:]
            cur[bands:, bands:] = rounded[:, :bands]

        for level in range(levels):
            half = 1 << level
            later = ka >= 2 * half
            sending = jnp.logical_and(later, lax.rem(ka, 2 * half) == half - 1)
            taking = jnp.logical_and(later, lax.rem(ka // half, 2) == 1)
            if 2 * half < nka:
                if level:
                    side_sent(level - 1)
                for t in range(1, half + 1 if level else 1):
                    @pl.when(jnp.logical_and(sending, ka + t < nka))
                    def _(t=t):
                        push_side(level, t).start()

                @pl.when(taking)
                def _(level=level):
                    push_side(level, 1).wait_recv()
                    set_cur(across(sides[level], cur[...], ((1,), (0,))).astype(BF16))

            @pl.when(jnp.logical_and(ka >= half, ka < 2 * half))
            def _(level=level, half=half):
                for i in range(PIECES):
                    push(level, 1, i).wait_recv()
                    if level + 1 == levels:
                        for j in range(nband):
                            spans = [slice(p * bands + j * cols, p * bands + (j + 1) * cols) for p in range(2)]
                            factor = jnp.concatenate([cur[:, span] for span in spans], axis=1)
                            term = across(got[level, rows_of(i), :], factor, ((1,), (0,)))
                            given[j, rows_of(i), :] = term * scale
                            if j != lead:
                                swap(i, j).start()
                        continue
                    joined = across(got[level, rows_of(i), :], cur[...], ((1,), (0,)))
                    if level + 1 < levels:
                        pfx[rows_of(i), :] = joined.astype(BF16)

                        @pl.when(ka == 2 * half - 1)
                        def _(i=i):
                            each_push(level + 1, i, lambda copy: copy.start())
                    hand_out(i, joined)

        out[...] = given[lead]
        for i in range(PIECES):
            for j in range(lead):
                swap(i, j).wait_send()
        for level in range(levels):
            half = 1 << level

            @pl.when(ka == half - 1)
            def _(level=level):
                for i in range(PIECES):
                    each_push(level, i, lambda copy: copy.wait_send())

            if 2 * half < nka <= 4 * half:
                side_sent(level)

    @pl.when(jnp.logical_not(leads))
    def _():
        for i in range(PIECES):
            swap(i, band).wait_recv()
        out[...] = taken[...]

    for copy in band_sends + [next_rank(band)]:
        copy.wait_send()

    @pl.loop(0, CHUNKS)
    def _(c):
        right_copy(c).wait_send()

    for b in range(BLOCKS):
        tail_copy(b, band).wait_send()

    @pl.when(leads)
    def _():
        for b in range(BLOCKS):
            for d in range(1, norb):
                share(b, d).wait_send()

    @pl.when(jnp.logical_not(leads))
    def _():
        to_lead(band).wait_send()


def solution(mesh):
    nka, norb, nband = mesh.shape["ka"], mesh.shape["orb"], mesh.shape["band"]
    depth = levels_of(nka)

    def body(eigvecs, band_rank, occ_count, wrap_shift, orbital_site):
        rows, cols = eigvecs.shape[2], eigvecs.shape[3]
        bands = cols * nband
        share = bands // norb
        depth_of = rows // 8
        hbm = pl.BlockSpec(memory_space=pltpu.HBM)
        dma = pltpu.SemaphoreType.DMA
        result = pl.pallas_call(
            functools.partial(kernel, nka, norb, nband),
            out_shape=pltpu.VMEM((share, 2 * cols), F32),
            in_specs=[hbm] * 5,
            out_specs=pl.BlockSpec(memory_space=pltpu.VMEM),
            scratch_shapes=[
                pltpu.VMEM((2, nband, rows, cols), BF16),
                pltpu.VMEM((2, rows - depth_of, cols), BF16),
                pltpu.VMEM((2, cols, depth_of), BF16),
                pltpu.VMEM((nband, 2, cols, depth_of), BF16),
                pltpu.VMEM((rows - depth_of, cols), F32),
                pltpu.VMEM((rows - depth_of, cols), F32),
                pltpu.VMEM((rows // 128, 128), F32),
                pltpu.VMEM((rows // 128, 128), F32),
                pltpu.VMEM((rows // 128, 128), F32),
                pltpu.VMEM((rows // 128, 128), F32),
                pltpu.SMEM((1,), jnp.int32),
                pltpu.SMEM((1,), jnp.int32),
                pltpu.VMEM((rows // 128, 128), jnp.int32),
                pltpu.VMEM((nband, 1, cols), jnp.int32),
                pltpu.VMEM((nband, 1, cols), jnp.int32),
                pltpu.VMEM((nband, 2 * cols, bands), F32),
                pltpu.VMEM((nband, cols, bands), F32),
                pltpu.VMEM((nband, norb, 2, cols, bands), BF16),
                pltpu.VMEM((2, bands, bands), F32),
                pltpu.VMEM((bands, 2 * bands), F32),
                pltpu.VMEM((2 * bands, 2 * bands), BF16),
                pltpu.VMEM((share, 2 * bands), BF16),
                pltpu.VMEM((depth, share, 2 * bands), BF16),
                pltpu.VMEM((depth, bands, 2 * bands), BF16),
                pltpu.VMEM((nband, share, 2 * cols), F32),
                pltpu.VMEM((share, 2 * cols), F32),
                pltpu.SemaphoreType.REGULAR,
                pltpu.SemaphoreType.REGULAR,
                dma,
                dma((4,)),
                dma((2, nband)),
                dma((2, nband)),
                dma((2, nband)),
                dma((2, CHUNKS)),
                dma((2, BLOCKS, nband)),
                dma((2, nband)),
                dma((2, BLOCKS, norb)),
                dma((2, depth, (1 << (depth - 1)) + 1, PIECES)),
                dma((2, depth, (1 << (depth - 1)) + 1)),
                dma((2, PIECES, nband)),
            ],
            compiler_params=pltpu.CompilerParams(
                collective_id=0, has_side_effects=True,
                vmem_limit_bytes=60000000
            ),
            name="wilson",
        )(
            eigvecs.reshape(2, rows, cols), band_rank, occ_count, wrap_shift,
            orbital_site.reshape(rows // 128, 128),
        )
        return result.reshape(1, share, 2, cols)

    return jax.shard_map(
        body,
        mesh=mesh,
        in_specs=(
            P(("grp", "ka"), None, "orb", "band"),
            P(("grp", "ka"), "band"),
            P("grp"),
            P("grp"),
            P(("grp", "orb")),
        ),
        out_specs=P(("grp", "ka"), "orb", None, "band"),
        check_vma=False,
    )
```

```python
import functools
import math

import jax
import jax.numpy as jnp
from jax import lax
from jax.experimental import pallas as pl
from jax.experimental.pallas import tpu as pltpu
from jax.sharding import PartitionSpec as P

NS_STEPS = 8
SITES = 64
CHUNKS = 7
BLOCKS = 8
PIECES = 2
BEHIND = 6

ns_gain = 0.7
eps_mean = 1e-06

MESH = pl.DeviceIdType.MESH
BF16 = jnp.bfloat16
F32 = jnp.float32


def levels_of(count):
    return max(1, (count - 1).bit_length())


def remote(src, dst, send_sem, recv_sem, device):
    return pltpu.make_async_remote_copy(
        src_ref=src,
        dst_ref=dst,
        send_sem=send_sem,
        recv_sem=recv_sem,
        device_id=device,
        device_id_type=MESH,
    )


def across(left, right, contract):
    return lax.dot_general(left, right, (contract, ((), ())), preferred_element_type=F32)


def column_of(row, width):
    return jnp.transpose(jnp.broadcast_to(row, (width, row.shape[1])))


def polar_step(iterate):
    half = iterate.shape[1] // 2
    rounded = iterate.astype(BF16)
    real, imag = rounded[:, :half], rounded[:, half:]
    turned = jnp.concatenate([imag, -real], axis=1)
    block = jnp.concatenate(
        [rounded, jnp.concatenate([-imag, real], axis=1)], axis=0
    )
    gram_real = across(rounded, rounded, ((1,), (1,))).astype(BF16)
    gram_imag = across(turned, rounded, ((1,), (1,))).astype(BF16)
    wide = jnp.concatenate([gram_real, gram_imag], axis=1)
    return 1.5 * iterate - 0.5 * across(wide, block, ((1,), (0,)))


def kernel(
    nka, norb, nband,
    eig, rank, occ_at, shift_at, site_at,
    out,
    lefts, rights, stage, tail, cosine, sine, angle_cos, angle_sin, tail_cos, tail_sin,
    occ, shift, site, rank_band, rank_next, accs, mask, parts, sums, full, cur, pfx, got, sides, given, taken,
    ready, known,
    sem_own, sem_arg, sem_left, sem_rank, sem_next, sem_right, sem_tail, sem_acc, sem_part, sem_pre, sem_side, sem_swap,
):
    ka, orb, band = lax.axis_index("ka"), lax.axis_index("orb"), lax.axis_index("band")
    rows, cols = eig.shape[1], eig.shape[2]
    bands = nband * cols
    depth = stage.shape[2]
    body = rows - depth
    step = body // CHUNKS
    width = cols // BLOCKS
    before = lax.rem(ka + nka - 1, nka)
    lead = nband - 1
    leads = band == lead
    lanes = site.shape[1]

    barrier = pltpu.get_barrier_semaphore()
    chip = [(0, e) for e in range(nband)]
    point = [(d, e) for d in range(norb) for e in range(nband)]

    def greet(semaphore, t, cores):
        for d, e in cores:
            to = {
                "ka": lax.rem(ka + nka + t, nka),
                "orb": lax.rem(orb + d, norb),
                "band": lax.rem(band + e, nband),
            }
            pl.semaphore_signal(semaphore, inc=1, device_id=to, device_id_type=MESH)

    for t in range(1, nka):
        @pl.when(ka + t < nka)
        def _(t=t):
            greet(barrier, t, point if t in (1, nka - 1) else chip)

    far = len(point) - nband if nka > 2 else 0

    @pl.when(jnp.logical_and(ka > 0, ka < nka - 1))
    def _():
        pl.semaphore_wait(barrier, len(point) + (ka - 1) * nband)

    @pl.when(ka == nka - 1)
    def _():
        pl.semaphore_wait(barrier, len(point) + (nka - 2) * nband + far)

    for t in range(nka - 1, 0, -1):
        @pl.when(ka >= t)
        def _(t=t):
            greet(ready, -t, point if t in (1, nka - 1) else chip)

    def chunk(c):
        return pl.ds(pl.multiple_of(c * step, step), step)

    def right_copy(c):
        return remote(
            eig.at[:, chunk(c)], rights.at[:, chunk(c)],
            sem_right.at[0, c], sem_right.at[1, c], {"ka": before},
        )

    def part_of(b):
        return pl.ds(b * width, width)

    def tail_copy(b, j):
        return remote(
            stage.at[:, part_of(b)], tail.at[j, :, part_of(b)],
            sem_tail.at[0, b, j], sem_tail.at[1, b, j], {"ka": before, "band": lead},
        )

    def next_rank(j):
        return remote(
            rank, rank_next.at[j], sem_next.at[0, j], sem_next.at[1, j],
            {"ka": before, "band": lead},
        )

    def start_right():
        next_rank(band).start()
        for c in range(CHUNKS):
            right_copy(c).start()

    @pl.when(ka > 0)
    def _():
        start_right()

    own = pltpu.make_async_copy(eig, lefts.at[:, band], sem_own)
    own.start()
    arguments = [
        pltpu.make_async_copy(src, dst, sem_arg.at[i])
        for i, (src, dst) in enumerate(
            ((occ_at, occ), (shift_at, shift), (site_at, site), (rank, rank_band.at[band]))
        )
    ]
    for copy in arguments:
        copy.start()

    @pl.when(ka == 0)
    def _():
        pl.semaphore_wait(ready, len(point) + (nka - 2) * nband + far)
        start_right()
        greet(known, -1, [(0, 0)])

    @pl.when(jnp.logical_and(ka > 0, ka < nka - 1))
    def _():
        pl.semaphore_wait(ready, len(point) + (nka - 2 - ka) * nband)

    @pl.when(ka == nka - 1)
    def _():
        pl.semaphore_wait(known, 1)

    band_sends = []
    for d in range(1, nband):
        to = {"band": lax.rem(band + d, nband)}
        copy = remote(eig, lefts.at[:, band], sem_left.at[0, d], sem_left.at[1, d], to)
        copy.start()
        band_sends.append(copy)
        copy = remote(rank, rank_band.at[band], sem_rank.at[0, d], sem_rank.at[1, d], to)
        copy.start()
        band_sends.append(copy)

    for copy in arguments:
        copy.wait()

    at_end, at_start = ka == nka - 1, ka == 0
    angle = ((shift[0] * site[...]) & (SITES - 1)).astype(F32) * (2.0 * math.pi / SITES)
    turned, lifted = jnp.cos(angle), jnp.sin(angle)
    angle_cos[...] = jnp.where(at_end, turned, 1.0)
    angle_sin[...] = jnp.where(at_end, lifted, 0.0)
    tail_cos[...] = jnp.where(at_start, turned, 1.0)
    tail_sin[...] = jnp.where(at_start, lifted, 0.0)

    own.wait()

    @pl.loop(0, depth // lanes)
    def _(i):
        from_rows = pl.ds(pl.multiple_of(body + i * lanes, lanes), lanes)
        to_lanes = pl.ds(pl.multiple_of(i * lanes, lanes), lanes)
        real = jnp.transpose(lefts[0, band, from_rows, :].astype(F32))
        imag = jnp.transpose(lefts[1, band, from_rows, :].astype(F32))
        turn = tail_cos[pl.ds(body // lanes + i, 1), :]
        lift = tail_sin[pl.ds(body // lanes + i, 1), :]
        stage[0, :, to_lanes] = (turn * real + lift * imag).astype(BF16)
        stage[1, :, to_lanes] = (turn * imag - lift * real).astype(BF16)

    @pl.loop(0, body // lanes)
    def _(i):
        place = pl.ds(pl.multiple_of(i * lanes, lanes), lanes)
        cosine[place, :] = column_of(angle_cos[pl.ds(i, 1), :], cols)
        sine[place, :] = column_of(angle_sin[pl.ds(i, 1), :], cols)

    for b in range(BLOCKS):
        tail_copy(b, band).start()

    for d in range(1, nband):
        came = lax.rem(band + nband - d, nband)
        to = {"band": lax.rem(band + d, nband)}
        remote(eig, lefts.at[:, came], sem_left.at[0, d], sem_left.at[1, d], to).wait_recv()
        remote(rank, rank_band.at[came], sem_rank.at[0, d], sem_rank.at[1, d], to).wait_recv()

    count = occ[0]

    @pl.when(leads)
    def _():
        row_mask = jnp.concatenate(
            [(rank_band[j] < count).astype(F32) for j in range(nband)], axis=1
        )
        for j in range(nband):
            next_rank(j).wait_recv()
            col_mask = column_of((rank_next[j] < count).astype(F32), cols)
            mask[j] = row_mask * jnp.concatenate([col_mask] * nband, axis=1)

    accs[band] = jnp.zeros(accs.shape[1:], F32)

    def lefts_of(p, place):
        return jnp.concatenate([lefts[p, j, place, :] for j in range(nband)], axis=1)

    @pl.loop(0, CHUNKS)
    def _(c):
        right_copy(c).wait_recv()
        place = chunk(c)
        real, imag = rights[0, place, :].astype(F32), rights[1, place, :].astype(F32)
        turn, lift = cosine[place, :], sine[place, :]
        new_real = (turn * real + lift * imag).astype(BF16)
        new_imag = (turn * imag - lift * real).astype(BF16)
        paired = jnp.concatenate(
            [
                jnp.concatenate([new_real, new_imag], axis=1),
                jnp.concatenate([new_imag, -new_real], axis=1),
            ],
            axis=0,
        )
        stacked = jnp.concatenate([lefts_of(p, place) for p in range(2)], axis=0)
        accs[band] += across(paired, stacked, ((0,), (0,)))

    def to_lead(j):
        return remote(
            accs.at[j], accs.at[j], sem_acc.at[0, j], sem_acc.at[1, j], {"band": lead}
        )

    def share(b, d):
        return remote(
            parts.at[:, 0, :, part_of(b)], parts.at[:, d, :, part_of(b)],
            sem_part.at[0, b, d], sem_part.at[1, b, d], {"orb": lax.rem(orb + d, norb)},
        )

    @pl.when(jnp.logical_not(leads))
    def _():
        to_lead(band).start()

    rest = pl.ds(body, depth)

    def absorb(b):
        for d in range(1, norb):
            share(b, d).wait_recv()
        for j in range(nband):
            for p in range(2):
                total = parts[j, 0, p, part_of(b), :].astype(F32)
                for d in range(1, norb):
                    total += parts[j, d, p, part_of(b), :].astype(F32)
                sums[p, pl.ds(j * cols + b * width, width), :] = total

    levels = levels_of(nka) if nka > 1 else 0
    height = bands // norb
    piece = height // PIECES
    scale = math.sqrt(bands)

    def rows_of(i):
        return pl.ds(i * piece, piece)

    def swap(i, j):
        return remote(
            given.at[j, rows_of(i)], taken.at[rows_of(i)],
            sem_swap.at[0, i, j], sem_swap.at[1, i, 0], {"band": j},
        )

    def push(level, t, i):
        here = pl.ds(pl.multiple_of(orb * height + i * piece, piece), piece)
        return remote(
            pfx.at[rows_of(i)] if level else cur.at[here], got.at[level, rows_of(i)],
            sem_pre.at[0, level, t, i], sem_pre.at[1, level, 0, i],
            {"ka": lax.rem(ka + t, nka)},
        )

    def each_push(level, i, act):
        for t in range(1, (1 << level) + 1):
            @pl.when(ka + t < nka)
            def _(t=t):
                act(push(level, t, i))

    def push_side(level, t):
        return remote(
            cur.at[pl.ds(0, bands)], sides.at[level],
            sem_side.at[0, level, t], sem_side.at[1, level, 0],
            {"ka": lax.rem(ka + t, nka)},
        )

    def side_sent(level):
        half = 1 << level
        sending = jnp.logical_and(ka >= 2 * half, lax.rem(ka, 2 * half) == half - 1)
        for t in range(1, half + 1):
            @pl.when(jnp.logical_and(sending, ka + t < nka))
            def _(t=t):
                push_side(level, t).wait_send()

    def set_cur(matrix):
        real, imag = matrix[:, :bands], matrix[:, bands:]
        cur[:bands, :bands] = real
        cur[:bands, bands:] = imag
        cur[bands:, :bands] = -imag
        cur[bands:, bands:] = real

    def hand_out(i, joined):
        for j in range(nband):
            for p in range(2):
                at = p * bands + j * cols
                given[j, rows_of(i), p * cols : (p + 1) * cols] = joined[:, at : at + cols] * scale
            if j != lead:
                swap(i, j).start()

    @pl.when(leads)
    def _():
        for j in range(lead):
            to_lead(j).wait_recv()
        whole = jnp.concatenate([lefts_of(p, rest) for p in range(2)], axis=0)
        for b in range(BLOCKS):
            quads = []
            for j in range(nband):
                tail_copy(b, j).wait_recv()
                real, imag = tail[j, 0, part_of(b), :], tail[j, 1, part_of(b), :]
                quads.append(jnp.concatenate([real, imag], axis=1))
                quads.append(jnp.concatenate([imag, -real], axis=1))
            term = across(jnp.concatenate(quads, axis=0), whole, ((1,), (0,)))
            for j in range(nband):
                for p in range(2):
                    at = (2 * j + p) * width
                    total = accs[j, pl.ds(p * cols + b * width, width), :] + term[at : at + width]
                    parts[j, 0, p, part_of(b), :] = (total * mask[j, part_of(b), :]).astype(BF16)
            for d in range(1, norb):
                share(b, d).start()
            if b >= BEHIND:
                absorb(b - BEHIND)
        for b in range(BLOCKS - BEHIND, BLOCKS):
            absorb(b)
        halves = [jnp.transpose(sums[p]) for p in range(2)]
        margins = jnp.concatenate(halves, axis=1)
        squares = jnp.sum(sums[0] * sums[0] + sums[1] * sums[1], keepdims=True)
        iterate = margins * (ns_gain * lax.rsqrt(squares / count.astype(F32) + eps_mean))
        for _ in range(NS_STEPS):
            iterate = polar_step(iterate)
        rounded = iterate.astype(BF16)
        cur[:bands, :] = rounded

        @pl.when(ka == 0)
        def _():
            for i in range(PIECES):
                if levels:
                    each_push(0, i, lambda copy: copy.start())
            full[...] = iterate
            for i in range(PIECES):
                here = pl.ds(pl.multiple_of(orb * height + i * piece, piece), piece)
                hand_out(i, full[here, :])

        if nka > 2:
            @pl.when(jnp.logical_and(ka >= 2, lax.rem(ka, 2) == 0))
            def _():
                @pl.when(ka + 1 < nka)
                def _():
                    push_side(0, 1).start()

        @pl.when(ka > 0)
        def _():
            cur[bands:, :bands] = -rounded[:, bands:]
            cur[bands:, bands:] = rounded[:, :bands]

        for level in range(levels):
            half = 1 << level
            later = ka >= 2 * half
            sending = jnp.logical_and(later, lax.rem(ka, 2 * half) == half - 1)
            taking = jnp.logical_and(later, lax.rem(ka // half, 2) == 1)
            if 2 * half < nka:
                if level:
                    side_sent(level - 1)
                for t in range(1, half + 1 if level else 1):
                    @pl.when(jnp.logical_and(sending, ka + t < nka))
                    def _(t=t):
                        push_side(level, t).start()

                @pl.when(taking)
                def _(level=level):
                    push_side(level, 1).wait_recv()
                    set_cur(across(sides[level], cur[...], ((1,), (0,))).astype(BF16))

            @pl.when(jnp.logical_and(ka >= half, ka < 2 * half))
            def _(level=level, half=half):
                for i in range(PIECES):
                    push(level, 1, i).wait_recv()
                    if level + 1 == levels:
                        for j in range(nband):
                            spans = [slice(p * bands + j * cols, p * bands + (j + 1) * cols) for p in range(2)]
                            factor = jnp.concatenate([cur[:, span] for span in spans], axis=1)
                            term = across(got[level, rows_of(i), :], factor, ((1,), (0,)))
                            given[j, rows_of(i), :] = term * scale
                            if j != lead:
                                swap(i, j).start()
                        continue
                    joined = across(got[level, rows_of(i), :], cur[...], ((1,), (0,)))
                    if level + 1 < levels:
                        pfx[rows_of(i), :] = joined.astype(BF16)

                        @pl.when(ka == 2 * half - 1)
                        def _(i=i):
                            each_push(level + 1, i, lambda copy: copy.start())
                    hand_out(i, joined)

        out[...] = given[lead]
        for i in range(PIECES):
            for j in range(lead):
                swap(i, j).wait_send()
        for level in range(levels):
            half = 1 << level

            @pl.when(ka == half - 1)
            def _(level=level):
                for i in range(PIECES):
                    each_push(level, i, lambda copy: copy.wait_send())

            if 2 * half < nka <= 4 * half:
                side_sent(level)

    @pl.when(jnp.logical_not(leads))
    def _():
        for i in range(PIECES):
            swap(i, band).wait_recv()
        out[...] = taken[...]

    for copy in band_sends + [next_rank(band)]:
        copy.wait_send()

    @pl.loop(0, CHUNKS)
    def _(c):
        right_copy(c).wait_send()

    for b in range(BLOCKS):
        tail_copy(b, band).wait_send()

    @pl.when(leads)
    def _():
        for b in range(BLOCKS):
            for d in range(1, norb):
                share(b, d).wait_send()

    @pl.when(jnp.logical_not(leads))
    def _():
        to_lead(band).wait_send()


def solution(mesh):
    nka, norb, nband = mesh.shape["ka"], mesh.shape["orb"], mesh.shape["band"]
    depth = levels_of(nka)

    def body(eigvecs, band_rank, occ_count, wrap_shift, orbital_site):
        rows, cols = eigvecs.shape[2], eigvecs.shape[3]
        bands = cols * nband
        share = bands // norb
        depth_of = rows // 8
        hbm = pl.BlockSpec(memory_space=pltpu.HBM)
        dma = pltpu.SemaphoreType.DMA
        result = pl.pallas_call(
            functools.partial(kernel, nka, norb, nband),
            out_shape=pltpu.VMEM((share, 2 * cols), F32),
            in_specs=[hbm] * 5,
            out_specs=pl.BlockSpec(memory_space=pltpu.VMEM),
            scratch_shapes=[
                pltpu.VMEM((2, nband, rows, cols), BF16),
                pltpu.VMEM((2, rows - depth_of, cols), BF16),
                pltpu.VMEM((2, cols, depth_of), BF16),
                pltpu.VMEM((nband, 2, cols, depth_of), BF16),
                pltpu.VMEM((rows - depth_of, cols), F32),
                pltpu.VMEM((rows - depth_of, cols), F32),
                pltpu.VMEM((rows // 128, 128), F32),
                pltpu.VMEM((rows // 128, 128), F32),
                pltpu.VMEM((rows // 128, 128), F32),
                pltpu.VMEM((rows // 128, 128), F32),
                pltpu.SMEM((1,), jnp.int32),
                pltpu.SMEM((1,), jnp.int32),
                pltpu.VMEM((rows // 128, 128), jnp.int32),
                pltpu.VMEM((nband, 1, cols), jnp.int32),
                pltpu.VMEM((nband, 1, cols), jnp.int32),
                pltpu.VMEM((nband, 2 * cols, bands), F32),
                pltpu.VMEM((nband, cols, bands), F32),
                pltpu.VMEM((nband, norb, 2, cols, bands), BF16),
                pltpu.VMEM((2, bands, bands), F32),
                pltpu.VMEM((bands, 2 * bands), F32),
                pltpu.VMEM((2 * bands, 2 * bands), BF16),
                pltpu.VMEM((share, 2 * bands), BF16),
                pltpu.VMEM((depth, share, 2 * bands), BF16),
                pltpu.VMEM((depth, bands, 2 * bands), BF16),
                pltpu.VMEM((nband, share, 2 * cols), F32),
                pltpu.VMEM((share, 2 * cols), F32),
                pltpu.SemaphoreType.REGULAR,
                pltpu.SemaphoreType.REGULAR,
                dma,
                dma((4,)),
                dma((2, nband)),
                dma((2, nband)),
                dma((2, nband)),
                dma((2, CHUNKS)),
                dma((2, BLOCKS, nband)),
                dma((2, nband)),
                dma((2, BLOCKS, norb)),
                dma((2, depth, (1 << (depth - 1)) + 1, PIECES)),
                dma((2, depth, (1 << (depth - 1)) + 1)),
                dma((2, PIECES, nband)),
            ],
            compiler_params=pltpu.CompilerParams(
                collective_id=0, has_side_effects=True,
                vmem_limit_bytes=60000000
            ),
            name="wilson",
        )(
            eigvecs.reshape(2, rows, cols), band_rank, occ_count, wrap_shift,
            orbital_site.reshape(rows // 128, 128),
        )
        return result.reshape(1, share, 2, cols)

    return jax.shard_map(
        body,
        mesh=mesh,
        in_specs=(
            P(("grp", "ka"), None, "orb", "band"),
            P(("grp", "ka"), "band"),
            P("grp"),
            P("grp"),
            P(("grp", "orb")),
        ),
        out_specs=P(("grp", "ka"), "orb", None, "band"),
        check_vma=False,
    )
```

```python
import functools
import math

import jax
import jax.numpy as jnp
from jax import lax
from jax.experimental import pallas as pl
from jax.experimental.pallas import tpu as pltpu
from jax.sharding import PartitionSpec as P

NS_STEPS = 8
SITES = 64
CHUNKS = 7
BLOCKS = 8
PIECES = 2
BEHIND = 6

ns_gain = 0.7
eps_mean = 1e-06

MESH = pl.DeviceIdType.MESH
BF16 = jnp.bfloat16
F32 = jnp.float32


def levels_of(count):
    return max(1, (count - 1).bit_length())


def remote(src, dst, send_sem, recv_sem, device):
    return pltpu.make_async_remote_copy(
        src_ref=src,
        dst_ref=dst,
        send_sem=send_sem,
        recv_sem=recv_sem,
        device_id=device,
        device_id_type=MESH,
    )


def across(left, right, contract):
    return lax.dot_general(left, right, (contract, ((), ())), preferred_element_type=F32)


def column_of(row, width):
    return jnp.transpose(jnp.broadcast_to(row, (width, row.shape[1])))


def polar_rows(iterate, rounded):
    half = rounded.shape[1] // 2
    real, imag = rounded[:, :half], rounded[:, half:]
    block = jnp.concatenate(
        [rounded, jnp.concatenate([-imag, real], axis=1)], axis=0
    )
    mine = iterate.astype(BF16)
    turned = jnp.concatenate([mine[:, half:], -mine[:, :half]], axis=1)
    gram_real = across(mine, rounded, ((1,), (1,))).astype(BF16)
    gram_imag = across(turned, rounded, ((1,), (1,))).astype(BF16)
    wide = jnp.concatenate([gram_real, gram_imag], axis=1)
    return 1.5 * iterate - 0.5 * across(wide, block, ((1,), (0,)))


def polar_step(iterate):
    return polar_rows(iterate, iterate.astype(BF16))


def kernel(
    nka, norb, nband,
    eig, rank, occ_at, shift_at, site_at,
    out,
    lefts, rights, stage, tail, cosine, sine, angle_cos, angle_sin, tail_cos, tail_sin,
    occ, shift, site, rank_band, rank_next, accs, mask, parts, sums, full, cur, pfx, got, sides, given, taken,
    ready, known,
    sem_own, sem_arg, sem_left, sem_rank, sem_next, sem_right, sem_tail, sem_acc, sem_part, sem_pre, sem_side, sem_swap,
):
    ka, orb, band = lax.axis_index("ka"), lax.axis_index("orb"), lax.axis_index("band")
    rows, cols = eig.shape[1], eig.shape[2]
    bands = nband * cols
    depth = stage.shape[2]
    body = rows - depth
    step = body // CHUNKS
    width = cols // BLOCKS
    before = lax.rem(ka + nka - 1, nka)
    lead = nband - 1
    leads = band == lead
    lanes = site.shape[1]

    barrier = pltpu.get_barrier_semaphore()
    chip = [(0, e) for e in range(nband)]
    point = [(d, e) for d in range(norb) for e in range(nband)]

    def greet(semaphore, t, cores):
        for d, e in cores:
            to = {
                "ka": lax.rem(ka + nka + t, nka),
                "orb": lax.rem(orb + d, norb),
                "band": lax.rem(band + e, nband),
            }
            pl.semaphore_signal(semaphore, inc=1, device_id=to, device_id_type=MESH)

    for t in range(1, nka):
        @pl.when(ka + t < nka)
        def _(t=t):
            greet(barrier, t, point if t in (1, nka - 1) else chip)

    far = len(point) - nband if nka > 2 else 0

    @pl.when(jnp.logical_and(ka > 0, ka < nka - 1))
    def _():
        pl.semaphore_wait(barrier, len(point) + (ka - 1) * nband)

    @pl.when(ka == nka - 1)
    def _():
        pl.semaphore_wait(barrier, len(point) + (nka - 2) * nband + far)

    for t in range(nka - 1, 0, -1):
        @pl.when(ka >= t)
        def _(t=t):
            greet(ready, -t, point if t in (1, nka - 1) else chip)

    def chunk(c):
        return pl.ds(pl.multiple_of(c * step, step), step)

    def right_copy(c):
        return remote(
            eig.at[:, chunk(c)], rights.at[:, chunk(c)],
            sem_right.at[0, c], sem_right.at[1, c], {"ka": before},
        )

    def part_of(b):
        return pl.ds(b * width, width)

    def tail_copy(b, j):
        return remote(
            stage.at[:, part_of(b)], tail.at[j, :, part_of(b)],
            sem_tail.at[0, b, j], sem_tail.at[1, b, j], {"ka": before, "band": lead},
        )

    def next_rank(j):
        return remote(
            rank, rank_next.at[j], sem_next.at[0, j], sem_next.at[1, j],
            {"ka": before, "band": lead},
        )

    def start_right():
        next_rank(band).start()
        for c in range(CHUNKS):
            right_copy(c).start()

    @pl.when(ka > 0)
    def _():
        start_right()

    own = pltpu.make_async_copy(eig, lefts.at[:, band], sem_own)
    own.start()
    arguments = [
        pltpu.make_async_copy(src, dst, sem_arg.at[i])
        for i, (src, dst) in enumerate(
            ((occ_at, occ), (shift_at, shift), (site_at, site), (rank, rank_band.at[band]))
        )
    ]
    for copy in arguments:
        copy.start()

    @pl.when(ka == 0)
    def _():
        pl.semaphore_wait(ready, len(point) + (nka - 2) * nband + far)
        start_right()
        greet(known, -1, [(0, 0)])

    @pl.when(jnp.logical_and(ka > 0, ka < nka - 1))
    def _():
        pl.semaphore_wait(ready, len(point) + (nka - 2 - ka) * nband)

    @pl.when(ka == nka - 1)
    def _():
        pl.semaphore_wait(known, 1)

    band_sends = []
    for d in range(1, nband):
        to = {"band": lax.rem(band + d, nband)}
        copy = remote(eig, lefts.at[:, band], sem_left.at[0, d], sem_left.at[1, d], to)
        copy.start()
        band_sends.append(copy)
        copy = remote(rank, rank_band.at[band], sem_rank.at[0, d], sem_rank.at[1, d], to)
        copy.start()
        band_sends.append(copy)

    for copy in arguments:
        copy.wait()

    at_end, at_start = ka == nka - 1, ka == 0
    angle = ((shift[0] * site[...]) & (SITES - 1)).astype(F32) * (2.0 * math.pi / SITES)
    turned, lifted = jnp.cos(angle), jnp.sin(angle)
    angle_cos[...] = jnp.where(at_end, turned, 1.0)
    angle_sin[...] = jnp.where(at_end, lifted, 0.0)
    tail_cos[...] = jnp.where(at_start, turned, 1.0)
    tail_sin[...] = jnp.where(at_start, lifted, 0.0)

    own.wait()

    @pl.loop(0, depth // lanes)
    def _(i):
        from_rows = pl.ds(pl.multiple_of(body + i * lanes, lanes), lanes)
        to_lanes = pl.ds(pl.multiple_of(i * lanes, lanes), lanes)
        real = jnp.transpose(lefts[0, band, from_rows, :].astype(F32))
        imag = jnp.transpose(lefts[1, band, from_rows, :].astype(F32))
        turn = tail_cos[pl.ds(body // lanes + i, 1), :]
        lift = tail_sin[pl.ds(body // lanes + i, 1), :]
        stage[0, :, to_lanes] = (turn * real + lift * imag).astype(BF16)
        stage[1, :, to_lanes] = (turn * imag - lift * real).astype(BF16)

    @pl.loop(0, body // lanes)
    def _(i):
        place = pl.ds(pl.multiple_of(i * lanes, lanes), lanes)
        cosine[place, :] = column_of(angle_cos[pl.ds(i, 1), :], cols)
        sine[place, :] = column_of(angle_sin[pl.ds(i, 1), :], cols)

    for b in range(BLOCKS):
        tail_copy(b, band).start()

    for d in range(1, nband):
        came = lax.rem(band + nband - d, nband)
        to = {"band": lax.rem(band + d, nband)}
        remote(eig, lefts.at[:, came], sem_left.at[0, d], sem_left.at[1, d], to).wait_recv()
        remote(rank, rank_band.at[came], sem_rank.at[0, d], sem_rank.at[1, d], to).wait_recv()

    count = occ[0]

    @pl.when(leads)
    def _():
        row_mask = jnp.concatenate(
            [(rank_band[j] < count).astype(F32) for j in range(nband)], axis=1
        )
        for j in range(nband):
            next_rank(j).wait_recv()
            col_mask = column_of((rank_next[j] < count).astype(F32), cols)
            mask[j] = row_mask * jnp.concatenate([col_mask] * nband, axis=1)

    accs[band] = jnp.zeros(accs.shape[1:], F32)

    def lefts_of(p, place):
        return jnp.concatenate([lefts[p, j, place, :] for j in range(nband)], axis=1)

    @pl.loop(0, CHUNKS)
    def _(c):
        right_copy(c).wait_recv()
        place = chunk(c)
        real, imag = rights[0, place, :].astype(F32), rights[1, place, :].astype(F32)
        turn, lift = cosine[place, :], sine[place, :]
        new_real = (turn * real + lift * imag).astype(BF16)
        new_imag = (turn * imag - lift * real).astype(BF16)
        paired = jnp.concatenate(
            [
                jnp.concatenate([new_real, new_imag], axis=1),
                jnp.concatenate([new_imag, -new_real], axis=1),
            ],
            axis=0,
        )
        stacked = jnp.concatenate([lefts_of(p, place) for p in range(2)], axis=0)
        accs[band] += across(paired, stacked, ((0,), (0,)))

    def to_lead(j):
        return remote(
            accs.at[j], accs.at[j], sem_acc.at[0, j], sem_acc.at[1, j], {"band": lead}
        )

    def share(b, d):
        return remote(
            parts.at[:, 0, :, part_of(b)], parts.at[:, d, :, part_of(b)],
            sem_part.at[0, b, d], sem_part.at[1, b, d], {"orb": lax.rem(orb + d, norb)},
        )

    @pl.when(jnp.logical_not(leads))
    def _():
        to_lead(band).start()

    rest = pl.ds(body, depth)

    def absorb(b):
        for d in range(1, norb):
            share(b, d).wait_recv()
        for j in range(nband):
            for p in range(2):
                total = parts[j, 0, p, part_of(b), :].astype(F32)
                for d in range(1, norb):
                    total += parts[j, d, p, part_of(b), :].astype(F32)
                sums[p, pl.ds(j * cols + b * width, width), :] = total

    levels = levels_of(nka) if nka > 1 else 0
    height = bands // norb
    piece = height // PIECES
    scale = math.sqrt(bands)

    def rows_of(i):
        return pl.ds(i * piece, piece)

    def swap(i, j):
        return remote(
            given.at[j, rows_of(i)], taken.at[rows_of(i)],
            sem_swap.at[0, i, j], sem_swap.at[1, i, 0], {"band": j},
        )

    def push(level, t, i):
        return remote(
            pfx.at[rows_of(i)], got.at[level, rows_of(i)],
            sem_pre.at[0, level, t, i], sem_pre.at[1, level, 0, i],
            {"ka": lax.rem(ka + t, nka)},
        )

    def each_push(level, i, act):
        for t in range(1, (1 << level) + 1):
            @pl.when(ka + t < nka)
            def _(t=t):
                act(push(level, t, i))

    def push_side(level, t):
        return remote(
            cur.at[pl.ds(0, bands)], sides.at[level],
            sem_side.at[0, level, t], sem_side.at[1, level, 0],
            {"ka": lax.rem(ka + t, nka)},
        )

    def side_sent(level):
        half = 1 << level
        sending = jnp.logical_and(ka >= 2 * half, lax.rem(ka, 2 * half) == half - 1)
        for t in range(1, half + 1):
            @pl.when(jnp.logical_and(sending, ka + t < nka))
            def _(t=t):
                push_side(level, t).wait_send()

    def set_cur(matrix):
        real, imag = matrix[:, :bands], matrix[:, bands:]
        cur[:bands, :bands] = real
        cur[:bands, bands:] = imag
        cur[bands:, :bands] = -imag
        cur[bands:, bands:] = real

    def hand_out(i, joined):
        for j in range(nband):
            for p in range(2):
                at = p * bands + j * cols
                given[j, rows_of(i), p * cols : (p + 1) * cols] = joined[:, at : at + cols] * scale
            if j != lead:
                swap(i, j).start()

    @pl.when(leads)
    def _():
        for j in range(lead):
            to_lead(j).wait_recv()
        whole = jnp.concatenate([lefts_of(p, rest) for p in range(2)], axis=0)
        for b in range(BLOCKS):
            quads = []
            for j in range(nband):
                tail_copy(b, j).wait_recv()
                real, imag = tail[j, 0, part_of(b), :], tail[j, 1, part_of(b), :]
                quads.append(jnp.concatenate([real, imag], axis=1))
                quads.append(jnp.concatenate([imag, -real], axis=1))
            term = across(jnp.concatenate(quads, axis=0), whole, ((1,), (0,)))
            for j in range(nband):
                for p in range(2):
                    at = (2 * j + p) * width
                    total = accs[j, pl.ds(p * cols + b * width, width), :] + term[at : at + width]
                    parts[j, 0, p, part_of(b), :] = (total * mask[j, part_of(b), :]).astype(BF16)
            for d in range(1, norb):
                share(b, d).start()
            if b >= BEHIND:
                absorb(b - BEHIND)
        for b in range(BLOCKS - BEHIND, BLOCKS):
            absorb(b)
        halves = [jnp.transpose(sums[p]) for p in range(2)]
        margins = jnp.concatenate(halves, axis=1)
        squares = jnp.sum(sums[0] * sums[0] + sums[1] * sums[1], keepdims=True)
        iterate = margins * (ns_gain * lax.rsqrt(squares / count.astype(F32) + eps_mean))
        for _ in range(NS_STEPS - 1):
            iterate = polar_step(iterate)

        @pl.when(ka == 0)
        def _():
            full[...] = iterate
            here = pl.ds(pl.multiple_of(orb * height, height), height)
            mine = polar_rows(full[here, :], iterate.astype(BF16))
            pfx[...] = mine.astype(BF16)
            for i in range(PIECES):
                if levels:
                    each_push(0, i, lambda copy: copy.start())
            for i in range(PIECES):
                hand_out(i, mine[i * piece : (i + 1) * piece])

        @pl.when(ka > 0)
        def _():
            cur[:bands, :] = polar_step(iterate).astype(BF16)

        if nka > 2:
            @pl.when(jnp.logical_and(ka >= 2, lax.rem(ka, 2) == 0))
            def _():
                @pl.when(ka + 1 < nka)
                def _():
                    push_side(0, 1).start()

        @pl.when(ka > 0)
        def _():
            cur[bands:, :bands] = -cur[:bands, bands:]
            cur[bands:, bands:] = cur[:bands, :bands]

        for level in range(levels):
            half = 1 << level
            later = ka >= 2 * half
            sending = jnp.logical_and(later, lax.rem(ka, 2 * half) == half - 1)
            taking = jnp.logical_and(later, lax.rem(ka // half, 2) == 1)
            if 2 * half < nka:
                if level:
                    side_sent(level - 1)
                for t in range(1, half + 1 if level else 1):
                    @pl.when(jnp.logical_and(sending, ka + t < nka))
                    def _(t=t):
                        push_side(level, t).start()

                @pl.when(taking)
                def _(level=level):
                    push_side(level, 1).wait_recv()
                    set_cur(across(sides[level], cur[...], ((1,), (0,))).astype(BF16))

            @pl.when(jnp.logical_and(ka >= half, ka < 2 * half))
            def _(level=level, half=half):
                for i in range(PIECES):
                    push(level, 1, i).wait_recv()
                    if level + 1 == levels:
                        for j in range(nband):
                            spans = [slice(p * bands + j * cols, p * bands + (j + 1) * cols) for p in range(2)]
                            factor = jnp.concatenate([cur[:, span] for span in spans], axis=1)
                            term = across(got[level, rows_of(i), :], factor, ((1,), (0,)))
                            given[j, rows_of(i), :] = term * scale
                            if j != lead:
                                swap(i, j).start()
                        continue
                    joined = across(got[level, rows_of(i), :], cur[...], ((1,), (0,)))
                    if level + 1 < levels:
                        pfx[rows_of(i), :] = joined.astype(BF16)

                        @pl.when(ka == 2 * half - 1)
                        def _(i=i):
                            each_push(level + 1, i, lambda copy: copy.start())
                    hand_out(i, joined)

        out[...] = given[lead]
        for i in range(PIECES):
            for j in range(lead):
                swap(i, j).wait_send()
        for level in range(levels):
            half = 1 << level

            @pl.when(ka == half - 1)
            def _(level=level):
                for i in range(PIECES):
                    each_push(level, i, lambda copy: copy.wait_send())

            if 2 * half < nka <= 4 * half:
                side_sent(level)

    @pl.when(jnp.logical_not(leads))
    def _():
        for i in range(PIECES):
            swap(i, band).wait_recv()
        out[...] = taken[...]

    for copy in band_sends + [next_rank(band)]:
        copy.wait_send()

    @pl.loop(0, CHUNKS)
    def _(c):
        right_copy(c).wait_send()

    for b in range(BLOCKS):
        tail_copy(b, band).wait_send()

    @pl.when(leads)
    def _():
        for b in range(BLOCKS):
            for d in range(1, norb):
                share(b, d).wait_send()

    @pl.when(jnp.logical_not(leads))
    def _():
        to_lead(band).wait_send()


def solution(mesh):
    nka, norb, nband = mesh.shape["ka"], mesh.shape["orb"], mesh.shape["band"]
    depth = levels_of(nka)

    def body(eigvecs, band_rank, occ_count, wrap_shift, orbital_site):
        rows, cols = eigvecs.shape[2], eigvecs.shape[3]
        bands = cols * nband
        share = bands // norb
        depth_of = rows // 8
        hbm = pl.BlockSpec(memory_space=pltpu.HBM)
        dma = pltpu.SemaphoreType.DMA
        result = pl.pallas_call(
            functools.partial(kernel, nka, norb, nband),
            out_shape=pltpu.VMEM((share, 2 * cols), F32),
            in_specs=[hbm] * 5,
            out_specs=pl.BlockSpec(memory_space=pltpu.VMEM),
            scratch_shapes=[
                pltpu.VMEM((2, nband, rows, cols), BF16),
                pltpu.VMEM((2, rows - depth_of, cols), BF16),
                pltpu.VMEM((2, cols, depth_of), BF16),
                pltpu.VMEM((nband, 2, cols, depth_of), BF16),
                pltpu.VMEM((rows - depth_of, cols), F32),
                pltpu.VMEM((rows - depth_of, cols), F32),
                pltpu.VMEM((rows // 128, 128), F32),
                pltpu.VMEM((rows // 128, 128), F32),
                pltpu.VMEM((rows // 128, 128), F32),
                pltpu.VMEM((rows // 128, 128), F32),
                pltpu.SMEM((1,), jnp.int32),
                pltpu.SMEM((1,), jnp.int32),
                pltpu.VMEM((rows // 128, 128), jnp.int32),
                pltpu.VMEM((nband, 1, cols), jnp.int32),
                pltpu.VMEM((nband, 1, cols), jnp.int32),
                pltpu.VMEM((nband, 2 * cols, bands), F32),
                pltpu.VMEM((nband, cols, bands), F32),
                pltpu.VMEM((nband, norb, 2, cols, bands), BF16),
                pltpu.VMEM((2, bands, bands), F32),
                pltpu.VMEM((bands, 2 * bands), F32),
                pltpu.VMEM((2 * bands, 2 * bands), BF16),
                pltpu.VMEM((share, 2 * bands), BF16),
                pltpu.VMEM((depth, share, 2 * bands), BF16),
                pltpu.VMEM((depth, bands, 2 * bands), BF16),
                pltpu.VMEM((nband, share, 2 * cols), F32),
                pltpu.VMEM((share, 2 * cols), F32),
                pltpu.SemaphoreType.REGULAR,
                pltpu.SemaphoreType.REGULAR,
                dma,
                dma((4,)),
                dma((2, nband)),
                dma((2, nband)),
                dma((2, nband)),
                dma((2, CHUNKS)),
                dma((2, BLOCKS, nband)),
                dma((2, nband)),
                dma((2, BLOCKS, norb)),
                dma((2, depth, (1 << (depth - 1)) + 1, PIECES)),
                dma((2, depth, (1 << (depth - 1)) + 1)),
                dma((2, PIECES, nband)),
            ],
            compiler_params=pltpu.CompilerParams(
                collective_id=0, has_side_effects=True,
                vmem_limit_bytes=60000000
            ),
            name="wilson",
        )(
            eigvecs.reshape(2, rows, cols), band_rank, occ_count, wrap_shift,
            orbital_site.reshape(rows // 128, 128),
        )
        return result.reshape(1, share, 2, cols)

    return jax.shard_map(
        body,
        mesh=mesh,
        in_specs=(
            P(("grp", "ka"), None, "orb", "band"),
            P(("grp", "ka"), "band"),
            P("grp"),
            P("grp"),
            P(("grp", "orb")),
        ),
        out_specs=P(("grp", "ka"), "orb", None, "band"),
        check_vma=False,
    )
```

```python
import functools
import math

import jax
import jax.numpy as jnp
from jax import lax
from jax.experimental import pallas as pl
from jax.experimental.pallas import tpu as pltpu
from jax.sharding import PartitionSpec as P

NS_STEPS = 8
SITES = 64
CHUNKS = 7
BLOCKS = 8
PIECES = 2
BEHIND = 6

ns_gain = 0.7
eps_mean = 1e-06

MESH = pl.DeviceIdType.MESH
BF16 = jnp.bfloat16
F32 = jnp.float32


def levels_of(count):
    return max(1, (count - 1).bit_length())


def remote(src, dst, send_sem, recv_sem, device):
    return pltpu.make_async_remote_copy(
        src_ref=src,
        dst_ref=dst,
        send_sem=send_sem,
        recv_sem=recv_sem,
        device_id=device,
        device_id_type=MESH,
    )


def across(left, right, contract):
    return lax.dot_general(left, right, (contract, ((), ())), preferred_element_type=F32)


def column_of(row, width):
    return jnp.transpose(jnp.broadcast_to(row, (width, row.shape[1])))


def polar_rows(iterate, rounded):
    half = rounded.shape[1] // 2
    real, imag = rounded[:, :half], rounded[:, half:]
    block = jnp.concatenate(
        [rounded, jnp.concatenate([-imag, real], axis=1)], axis=0
    )
    mine = iterate.astype(BF16)
    turned = jnp.concatenate([mine[:, half:], -mine[:, :half]], axis=1)
    gram_real = across(mine, rounded, ((1,), (1,))).astype(BF16)
    gram_imag = across(turned, rounded, ((1,), (1,))).astype(BF16)
    wide = jnp.concatenate([gram_real, gram_imag], axis=1)
    return 1.5 * iterate - 0.5 * across(wide, block, ((1,), (0,)))


def polar_step(iterate):
    return polar_rows(iterate, iterate.astype(BF16))


def kernel(
    nka, norb, nband,
    eig, rank, occ_at, shift_at, site_at,
    out,
    lefts, rights, stage, tail, cosine, sine, angle_cos, angle_sin, tail_cos, tail_sin,
    occ, shift, site, rank_band, rank_next, accs, mask, parts, sums, full, cur, pfx, got, sides, given, taken,
    ready, known,
    sem_own, sem_arg, sem_left, sem_rank, sem_next, sem_right, sem_tail, sem_acc, sem_part, sem_pre, sem_side, sem_swap,
):
    ka, orb, band = lax.axis_index("ka"), lax.axis_index("orb"), lax.axis_index("band")
    rows, cols = eig.shape[1], eig.shape[2]
    bands = nband * cols
    depth = stage.shape[2]
    body = rows - depth
    step = body // CHUNKS
    width = cols // BLOCKS
    before = lax.rem(ka + nka - 1, nka)
    lead = nband - 1
    leads = band == lead
    lanes = site.shape[1]

    barrier = pltpu.get_barrier_semaphore()
    chip = [(0, e) for e in range(nband)]
    point = [(d, e) for d in range(norb) for e in range(nband)]

    def greet(semaphore, t, cores):
        for d, e in cores:
            to = {
                "ka": lax.rem(ka + nka + t, nka),
                "orb": lax.rem(orb + d, norb),
                "band": lax.rem(band + e, nband),
            }
            pl.semaphore_signal(semaphore, inc=1, device_id=to, device_id_type=MESH)

    for t in range(1, nka):
        @pl.when(ka + t < nka)
        def _(t=t):
            greet(barrier, t, point if t in (1, nka - 1) else chip)

    far = len(point) - nband if nka > 2 else 0

    @pl.when(jnp.logical_and(ka > 0, ka < nka - 1))
    def _():
        pl.semaphore_wait(barrier, len(point) + (ka - 1) * nband)

    @pl.when(ka == nka - 1)
    def _():
        pl.semaphore_wait(barrier, len(point) + (nka - 2) * nband + far)

    for t in range(nka - 1, 0, -1):
        @pl.when(ka >= t)
        def _(t=t):
            greet(ready, -t, point if t in (1, nka - 1) else chip)

    def chunk(c):
        return pl.ds(pl.multiple_of(c * step, step), step)

    def right_copy(c):
        return remote(
            eig.at[:, chunk(c)], rights.at[:, chunk(c)],
            sem_right.at[0, c], sem_right.at[1, c], {"ka": before},
        )

    def part_of(b):
        return pl.ds(b * width, width)

    def tail_copy(b, j):
        return remote(
            stage.at[:, part_of(b)], tail.at[j, :, part_of(b)],
            sem_tail.at[0, b, j], sem_tail.at[1, b, j], {"ka": before, "band": lead},
        )

    def next_rank(j):
        return remote(
            rank, rank_next.at[j], sem_next.at[0, j], sem_next.at[1, j],
            {"ka": before, "band": lead},
        )

    def start_right():
        next_rank(band).start()
        for c in range(CHUNKS):
            right_copy(c).start()

    @pl.when(ka > 0)
    def _():
        start_right()

    own = pltpu.make_async_copy(eig, lefts.at[:, band], sem_own)
    own.start()
    arguments = [
        pltpu.make_async_copy(src, dst, sem_arg.at[i])
        for i, (src, dst) in enumerate(
            ((occ_at, occ), (shift_at, shift), (site_at, site), (rank, rank_band.at[band]))
        )
    ]
    for copy in arguments:
        copy.start()

    @pl.when(ka == 0)
    def _():
        pl.semaphore_wait(ready, len(point) + (nka - 2) * nband + far)
        start_right()
        greet(known, -1, [(0, 0)])

    @pl.when(jnp.logical_and(ka > 0, ka < nka - 1))
    def _():
        pl.semaphore_wait(ready, len(point) + (nka - 2 - ka) * nband)

    @pl.when(ka == nka - 1)
    def _():
        pl.semaphore_wait(known, 1)

    band_sends = []
    for d in range(1, nband):
        to = {"band": lax.rem(band + d, nband)}
        copy = remote(eig, lefts.at[:, band], sem_left.at[0, d], sem_left.at[1, d], to)
        copy.start()
        band_sends.append(copy)
        copy = remote(rank, rank_band.at[band], sem_rank.at[0, d], sem_rank.at[1, d], to)
        copy.start()
        band_sends.append(copy)

    for copy in arguments:
        copy.wait()

    at_end, at_start = ka == nka - 1, ka == 0
    angle = ((shift[0] * site[...]) & (SITES - 1)).astype(F32) * (2.0 * math.pi / SITES)
    turned, lifted = jnp.cos(angle), jnp.sin(angle)
    angle_cos[...] = jnp.where(at_end, turned, 1.0)
    angle_sin[...] = jnp.where(at_end, lifted, 0.0)
    tail_cos[...] = jnp.where(at_start, turned, 1.0)
    tail_sin[...] = jnp.where(at_start, lifted, 0.0)

    own.wait()

    @pl.loop(0, depth // lanes)
    def _(i):
        from_rows = pl.ds(pl.multiple_of(body + i * lanes, lanes), lanes)
        to_lanes = pl.ds(pl.multiple_of(i * lanes, lanes), lanes)
        real = jnp.transpose(lefts[0, band, from_rows, :].astype(F32))
        imag = jnp.transpose(lefts[1, band, from_rows, :].astype(F32))
        turn = tail_cos[pl.ds(body // lanes + i, 1), :]
        lift = tail_sin[pl.ds(body // lanes + i, 1), :]
        stage[0, :, to_lanes] = (turn * real + lift * imag).astype(BF16)
        stage[1, :, to_lanes] = (turn * imag - lift * real).astype(BF16)

    @pl.loop(0, body // lanes)
    def _(i):
        place = pl.ds(pl.multiple_of(i * lanes, lanes), lanes)
        cosine[place, :] = column_of(angle_cos[pl.ds(i, 1), :], cols)
        sine[place, :] = column_of(angle_sin[pl.ds(i, 1), :], cols)

    for b in range(BLOCKS):
        tail_copy(b, band).start()

    for d in range(1, nband):
        came = lax.rem(band + nband - d, nband)
        to = {"band": lax.rem(band + d, nband)}
        remote(eig, lefts.at[:, came], sem_left.at[0, d], sem_left.at[1, d], to).wait_recv()
        remote(rank, rank_band.at[came], sem_rank.at[0, d], sem_rank.at[1, d], to).wait_recv()

    count = occ[0]

    @pl.when(leads)
    def _():
        row_mask = jnp.concatenate(
            [(rank_band[j] < count).astype(F32) for j in range(nband)], axis=1
        )
        for j in range(nband):
            next_rank(j).wait_recv()
            col_mask = column_of((rank_next[j] < count).astype(F32), cols)
            mask[j] = row_mask * jnp.concatenate([col_mask] * nband, axis=1)

    accs[band] = jnp.zeros(accs.shape[1:], F32)

    def lefts_of(p, place):
        return jnp.concatenate([lefts[p, j, place, :] for j in range(nband)], axis=1)

    @pl.loop(0, CHUNKS)
    def _(c):
        right_copy(c).wait_recv()
        place = chunk(c)
        real, imag = rights[0, place, :].astype(F32), rights[1, place, :].astype(F32)
        turn, lift = cosine[place, :], sine[place, :]
        new_real = (turn * real + lift * imag).astype(BF16)
        new_imag = (turn * imag - lift * real).astype(BF16)
        paired = jnp.concatenate(
            [
                jnp.concatenate([new_real, new_imag], axis=1),
                jnp.concatenate([new_imag, -new_real], axis=1),
            ],
            axis=0,
        )
        stacked = jnp.concatenate([lefts_of(p, place) for p in range(2)], axis=0)
        accs[band] += across(paired, stacked, ((0,), (0,)))

    def to_lead(j):
        return remote(
            accs.at[j], accs.at[j], sem_acc.at[0, j], sem_acc.at[1, j], {"band": lead}
        )

    def share(b, d):
        return remote(
            parts.at[:, 0, :, part_of(b)], parts.at[:, d, :, part_of(b)],
            sem_part.at[0, b, d], sem_part.at[1, b, d], {"orb": lax.rem(orb + d, norb)},
        )

    @pl.when(jnp.logical_not(leads))
    def _():
        to_lead(band).start()

    rest = pl.ds(body, depth)

    def absorb(b):
        for d in range(1, norb):
            share(b, d).wait_recv()
        for j in range(nband):
            for p in range(2):
                total = parts[j, 0, p, part_of(b), :].astype(F32)
                for d in range(1, norb):
                    total += parts[j, d, p, part_of(b), :].astype(F32)
                sums[p, pl.ds(j * cols + b * width, width), :] = total

    levels = levels_of(nka) if nka > 1 else 0
    height = bands // norb
    piece = height // PIECES
    scale = math.sqrt(bands)

    def rows_of(i):
        return pl.ds(i * piece, piece)

    def swap(i, j):
        return remote(
            given.at[j, rows_of(i)], taken.at[rows_of(i)],
            sem_swap.at[0, i, j], sem_swap.at[1, i, 0], {"band": j},
        )

    def push(level, t, i):
        return remote(
            pfx.at[rows_of(i)], got.at[level, rows_of(i)],
            sem_pre.at[0, level, t, i], sem_pre.at[1, level, 0, i],
            {"ka": lax.rem(ka + t, nka)},
        )

    def each_push(level, i, act):
        for t in range(1, (1 << level) + 1):
            @pl.when(ka + t < nka)
            def _(t=t):
                act(push(level, t, i))

    def push_side(level, t, h):
        here = pl.ds(h * (bands // 2), bands // 2)
        return remote(
            cur.at[here], sides.at[level, here],
            sem_side.at[0, level, t, h], sem_side.at[1, level, 0, h],
            {"ka": lax.rem(ka + t, nka)},
        )

    def side_sent(level):
        half = 1 << level
        sending = jnp.logical_and(ka >= 2 * half, lax.rem(ka, 2 * half) == half - 1)
        for t in range(1, half + 1):
            @pl.when(jnp.logical_and(sending, ka + t < nka))
            def _(t=t):
                for h in range(2):
                    push_side(level, t, h).wait_send()

    def set_cur(matrix):
        real, imag = matrix[:, :bands], matrix[:, bands:]
        cur[:bands, :bands] = real
        cur[:bands, bands:] = imag
        cur[bands:, :bands] = -imag
        cur[bands:, bands:] = real

    def hand_out(i, joined):
        for j in range(nband):
            for p in range(2):
                at = p * bands + j * cols
                given[j, rows_of(i), p * cols : (p + 1) * cols] = joined[:, at : at + cols] * scale
            if j != lead:
                swap(i, j).start()

    @pl.when(leads)
    def _():
        for j in range(lead):
            to_lead(j).wait_recv()
        whole = jnp.concatenate([lefts_of(p, rest) for p in range(2)], axis=0)
        for b in range(BLOCKS):
            quads = []
            for j in range(nband):
                tail_copy(b, j).wait_recv()
                real, imag = tail[j, 0, part_of(b), :], tail[j, 1, part_of(b), :]
                quads.append(jnp.concatenate([real, imag], axis=1))
                quads.append(jnp.concatenate([imag, -real], axis=1))
            term = across(jnp.concatenate(quads, axis=0), whole, ((1,), (0,)))
            for j in range(nband):
                for p in range(2):
                    at = (2 * j + p) * width
                    total = accs[j, pl.ds(p * cols + b * width, width), :] + term[at : at + width]
                    parts[j, 0, p, part_of(b), :] = (total * mask[j, part_of(b), :]).astype(BF16)
            for d in range(1, norb):
                share(b, d).start()
            if b >= BEHIND:
                absorb(b - BEHIND)
        for b in range(BLOCKS - BEHIND, BLOCKS):
            absorb(b)
        halves = [jnp.transpose(sums[p]) for p in range(2)]
        margins = jnp.concatenate(halves, axis=1)
        squares = jnp.sum(sums[0] * sums[0] + sums[1] * sums[1], keepdims=True)
        iterate = margins * (ns_gain * lax.rsqrt(squares / count.astype(F32) + eps_mean))
        for _ in range(NS_STEPS - 1):
            iterate = polar_step(iterate)

        @pl.when(ka == 0)
        def _():
            full[...] = iterate
            here = pl.ds(pl.multiple_of(orb * height, height), height)
            mine = polar_rows(full[here, :], iterate.astype(BF16))
            pfx[...] = mine.astype(BF16)
            for i in range(PIECES):
                if levels:
                    each_push(0, i, lambda copy: copy.start())
            for i in range(PIECES):
                hand_out(i, mine[i * piece : (i + 1) * piece])

        @pl.when(ka > 0)
        def _():
            cur[:bands, :] = polar_step(iterate).astype(BF16)

        if nka > 2:
            @pl.when(jnp.logical_and(ka >= 2, lax.rem(ka, 2) == 0))
            def _():
                @pl.when(ka + 1 < nka)
                def _():
                    for h in range(2):
                        push_side(0, 1, h).start()

        @pl.when(ka > 0)
        def _():
            cur[bands:, :bands] = -cur[:bands, bands:]
            cur[bands:, bands:] = cur[:bands, :bands]

        for level in range(levels):
            half = 1 << level
            later = ka >= 2 * half
            sending = jnp.logical_and(later, lax.rem(ka, 2 * half) == half - 1)
            taking = jnp.logical_and(later, lax.rem(ka // half, 2) == 1)
            if 2 * half < nka:
                if level:
                    side_sent(level - 1)
                for t in range(1, half + 1 if level else 1):
                    @pl.when(jnp.logical_and(sending, ka + t < nka))
                    def _(t=t):
                        for h in range(2):
                            push_side(level, t, h).start()

                @pl.when(taking)
                def _(level=level):
                    rows_in = []
                    for h in range(2):
                        here = pl.ds(h * (bands // 2), bands // 2)
                        push_side(level, 1, h).wait_recv()
                        rows_in.append(
                            across(sides[level, here, :], cur[...], ((1,), (0,))).astype(BF16)
                        )
                    set_cur(jnp.concatenate(rows_in, axis=0))

            @pl.when(jnp.logical_and(ka >= half, ka < 2 * half))
            def _(level=level, half=half):
                for i in range(PIECES):
                    push(level, 1, i).wait_recv()
                    if level + 1 == levels:
                        for j in range(nband):
                            spans = [slice(p * bands + j * cols, p * bands + (j + 1) * cols) for p in range(2)]
                            factor = jnp.concatenate([cur[:, span] for span in spans], axis=1)
                            term = across(got[level, rows_of(i), :], factor, ((1,), (0,)))
                            given[j, rows_of(i), :] = term * scale
                            if j != lead:
                                swap(i, j).start()
                        continue
                    joined = across(got[level, rows_of(i), :], cur[...], ((1,), (0,)))
                    if level + 1 < levels:
                        pfx[rows_of(i), :] = joined.astype(BF16)

                        @pl.when(ka == 2 * half - 1)
                        def _(i=i):
                            each_push(level + 1, i, lambda copy: copy.start())
                    hand_out(i, joined)

        out[...] = given[lead]
        for i in range(PIECES):
            for j in range(lead):
                swap(i, j).wait_send()
        for level in range(levels):
            half = 1 << level

            @pl.when(ka == half - 1)
            def _(level=level):
                for i in range(PIECES):
                    each_push(level, i, lambda copy: copy.wait_send())

            if 2 * half < nka <= 4 * half:
                side_sent(level)

    @pl.when(jnp.logical_not(leads))
    def _():
        for i in range(PIECES):
            swap(i, band).wait_recv()
        out[...] = taken[...]

    for copy in band_sends + [next_rank(band)]:
        copy.wait_send()

    @pl.loop(0, CHUNKS)
    def _(c):
        right_copy(c).wait_send()

    for b in range(BLOCKS):
        tail_copy(b, band).wait_send()

    @pl.when(leads)
    def _():
        for b in range(BLOCKS):
            for d in range(1, norb):
                share(b, d).wait_send()

    @pl.when(jnp.logical_not(leads))
    def _():
        to_lead(band).wait_send()


def solution(mesh):
    nka, norb, nband = mesh.shape["ka"], mesh.shape["orb"], mesh.shape["band"]
    depth = levels_of(nka)

    def body(eigvecs, band_rank, occ_count, wrap_shift, orbital_site):
        rows, cols = eigvecs.shape[2], eigvecs.shape[3]
        bands = cols * nband
        share = bands // norb
        depth_of = rows // 8
        hbm = pl.BlockSpec(memory_space=pltpu.HBM)
        dma = pltpu.SemaphoreType.DMA
        result = pl.pallas_call(
            functools.partial(kernel, nka, norb, nband),
            out_shape=pltpu.VMEM((share, 2 * cols), F32),
            in_specs=[hbm] * 5,
            out_specs=pl.BlockSpec(memory_space=pltpu.VMEM),
            scratch_shapes=[
                pltpu.VMEM((2, nband, rows, cols), BF16),
                pltpu.VMEM((2, rows - depth_of, cols), BF16),
                pltpu.VMEM((2, cols, depth_of), BF16),
                pltpu.VMEM((nband, 2, cols, depth_of), BF16),
                pltpu.VMEM((rows - depth_of, cols), F32),
                pltpu.VMEM((rows - depth_of, cols), F32),
                pltpu.VMEM((rows // 128, 128), F32),
                pltpu.VMEM((rows // 128, 128), F32),
                pltpu.VMEM((rows // 128, 128), F32),
                pltpu.VMEM((rows // 128, 128), F32),
                pltpu.SMEM((1,), jnp.int32),
                pltpu.SMEM((1,), jnp.int32),
                pltpu.VMEM((rows // 128, 128), jnp.int32),
                pltpu.VMEM((nband, 1, cols), jnp.int32),
                pltpu.VMEM((nband, 1, cols), jnp.int32),
                pltpu.VMEM((nband, 2 * cols, bands), F32),
                pltpu.VMEM((nband, cols, bands), F32),
                pltpu.VMEM((nband, norb, 2, cols, bands), BF16),
                pltpu.VMEM((2, bands, bands), F32),
                pltpu.VMEM((bands, 2 * bands), F32),
                pltpu.VMEM((2 * bands, 2 * bands), BF16),
                pltpu.VMEM((share, 2 * bands), BF16),
                pltpu.VMEM((depth, share, 2 * bands), BF16),
                pltpu.VMEM((depth, bands, 2 * bands), BF16),
                pltpu.VMEM((nband, share, 2 * cols), F32),
                pltpu.VMEM((share, 2 * cols), F32),
                pltpu.SemaphoreType.REGULAR,
                pltpu.SemaphoreType.REGULAR,
                dma,
                dma((4,)),
                dma((2, nband)),
                dma((2, nband)),
                dma((2, nband)),
                dma((2, CHUNKS)),
                dma((2, BLOCKS, nband)),
                dma((2, nband)),
                dma((2, BLOCKS, norb)),
                dma((2, depth, (1 << (depth - 1)) + 1, PIECES)),
                dma((2, depth, (1 << (depth - 1)) + 1, 2)),
                dma((2, PIECES, nband)),
            ],
            compiler_params=pltpu.CompilerParams(
                collective_id=0, has_side_effects=True,
                vmem_limit_bytes=60000000
            ),
            name="wilson",
        )(
            eigvecs.reshape(2, rows, cols), band_rank, occ_count, wrap_shift,
            orbital_site.reshape(rows // 128, 128),
        )
        return result.reshape(1, share, 2, cols)

    return jax.shard_map(
        body,
        mesh=mesh,
        in_specs=(
            P(("grp", "ka"), None, "orb", "band"),
            P(("grp", "ka"), "band"),
            P("grp"),
            P("grp"),
            P(("grp", "orb")),
        ),
        out_specs=P(("grp", "ka"), "orb", None, "band"),
        check_vma=False,
    )
```
